256 devices in a mesh: section: 2 (over core), dp: 16 (over z, x_lo), tensor: 8 (over y, x_hi).
Axes of the slice: x: 4 (x_hi: 2, x_lo: 2; x = x_hi * 2 + x_lo), y: 4, z: 8, core: 2. Of those that a mesh axis runs over, the one named last changes fastest.
Arguments:
- tokens: bfloat16 [2048, 4096], P('dp', 'tensor'), may hold values from -6 to 6
- gain: bfloat16 [2, 4096], P('section', 'tensor'), may hold values from 0.099609375 to 1.8984375
- w_up: bfloat16 [2, 4096, 5120], P('section', 'dp', 'tensor'), may hold values from -0.09375 to 0.09375
- w_down: bfloat16 [2, 5120, 4096], P('section', 'tensor', 'dp'), may hold values from -0.078125 to 0.078125
- cotangent: bfloat16 [2, 2048, 4096], P('section', 'dp'), may hold values from -6 to 6
Outputs:
- states: bfloat16 [2, 2048, 4096], P('section', 'dp', 'tensor')
- grad_down: bfloat16 [2, 5120, 4096], P('section', 'tensor', 'dp')
The draws below stay inside these ranges and needn't reach their ends.
All inputs are finite; a program needn't handle non-finite values.
Results may differ from the reference program's by a relative error of at most 0.02.
Values may be sent and summed in bfloat16 or wider, within the bound.
A program may use at most 64 MiB of HBM per device.

```python
import jax
import jax.numpy as jnp
from jax import lax

WIDTH = 4096
HIDDEN_SIZE = 5120
TOK_DEV = 128
TOKENS = 2048
LAYERS = 2
N_SECTION = 2
N_DP = 16
N_TENSOR = 8


def block_levels(own_key, dims, pieces, low, high):
    level = 1.0
    for dim, blocks in pieces:
        steps = jax.random.uniform(jax.random.fold_in(jax.random.fold_in(own_key, 6), dim), (blocks,), jnp.float32, low / len(pieces), high / len(pieces))
        level = level * jnp.repeat(jnp.exp(steps), dims[dim] // blocks).reshape((-1,) + (1,) * (len(dims) - 1 - dim))
    return level


def normal_values(key, extent, deviation, bound, cuts=(), dtype=jnp.bfloat16):
    drawn = deviation * jax.random.normal(key, extent, jnp.float32)
    if cuts:
        drawn = drawn * block_levels(key, extent, cuts, -0.22, 0.18)
    return jnp.clip(drawn, -bound, bound).astype(dtype)


def setup_inputs(seed: int = 0) -> dict:
    arg_keys = jax.random.split(jax.random.key(seed), 6)
    return {
        "tokens": normal_values(arg_keys[0], (TOKENS, WIDTH), 1.0, 6.0, ((0, 16), (1, 8))),
        "gain": jnp.clip(1.0 + 0.18 * jax.random.normal(arg_keys[1], (LAYERS, WIDTH), jnp.float32), 0.099609375, 1.8984375).astype(jnp.bfloat16),
        "w_up": normal_values(arg_keys[2], (LAYERS, WIDTH, HIDDEN_SIZE), WIDTH ** -0.5, 0.09375, ((0, 2), (1, 16), (2, 8))),
        "w_down": normal_values(arg_keys[3], (LAYERS, HIDDEN_SIZE, WIDTH), HIDDEN_SIZE ** -0.5, 0.078125, ((0, 2), (1, 8), (2, 16))),
        "cotangent": normal_values(arg_keys[4], (LAYERS, TOKENS, WIDTH), 1.0, 6.0, ((0, 2), (1, 16))),
    }


EPS = 1e-06

def layer_ref(acts, gain_row, up_mat, down_mat):
    acts_f = acts.astype(jnp.float32)
    mean_sq = lax.optimization_barrier(jnp.mean(acts_f * acts_f, axis=1, keepdims=True))
    normed = (acts_f * lax.rsqrt(mean_sq + EPS) * gain_row.astype(jnp.float32)).astype(jnp.bfloat16)
    pre_act = jnp.dot(normed, up_mat, preferred_element_type=jnp.float32)
    hidden = jax.nn.gelu(pre_act, approximate=True).astype(jnp.bfloat16)
    group_width = HIDDEN_SIZE // N_TENSOR
    summed = jnp.zeros(acts.shape, jnp.float32)
    for group_id in range(N_TENSOR):
        lower = group_id * group_width
        partial_value = jnp.dot(hidden[:, lower:lower + group_width], down_mat[lower:lower + group_width, :], preferred_element_type=jnp.float32).astype(jnp.bfloat16)
        summed = summed + lax.optimization_barrier(partial_value).astype(jnp.float32)
    return ((acts_f + summed).astype(jnp.bfloat16), hidden)

def reference(tokens, gain, w_up, w_down, cotangent):
    acts = tokens
    states = []
    grads = []
    for layer_id in range(N_SECTION):
        acts, hidden = layer_ref(acts, gain[layer_id], w_up[layer_id], w_down[layer_id])
        states.append(acts)
        grad_sum = jnp.zeros((HIDDEN_SIZE, WIDTH), jnp.float32)
        for peer_id in range(N_DP):
            lower = peer_id * TOK_DEV
            partial_value = lax.dot_general(hidden[lower:lower + TOK_DEV], cotangent[layer_id][lower:lower + TOK_DEV], (((0,), (0,)), ((), ())), preferred_element_type=jnp.float32).astype(jnp.bfloat16)
            grad_sum = grad_sum + lax.optimization_barrier(partial_value).astype(jnp.float32)
        grads.append(grad_sum.astype(jnp.bfloat16))
    return (jnp.stack(states), jnp.stack(grads))
```

```python
import jax
import jax.numpy as jnp
from jax import lax
from jax.experimental import pallas as pl
from jax.experimental.pallas import tpu as pltpu
from jax.sharding import Mesh
from jax.sharding import PartitionSpec as P

EPS = 1e-06
MESH = pl.DeviceIdType.MESH
NZ, NY, NX = 8, 4, 2
NT = NY * NX
F32, BF16 = jnp.float32, jnp.bfloat16


def ring_offset(i):
    return ((i + 1) // 2) * (1 - 2 * ((i + 1) % 2))


def kernel(
    width,
    tok_ref, gain_ref, up_ref, down_ref, cot_ref,
    state_ref, grad_ref,
    x_all, c_all, gain_z, up_pair, down_pair,
    part_out, part_in, sq_out, sq_in, acc, hid_all, y_out, y_in, x_next,
    grad_own, grad_out, grad_in,
    xin_s, xin_r, gain_s, gain_r, cotp_s, cotp_r, up_s, up_r, down_s, down_r, core_s,
    ag_s, ag_r, cg_s, cg_r, rz_s, rz_r, sq_s, sq_r, az_s, az_r, rt_s, rt_r,
    gr_s, gr_r, out_s, out_r,
):
    section = lax.axis_index("section")
    z = lax.axis_index("z")
    xl = lax.axis_index("xl")
    y = lax.axis_index("y")
    xh = lax.axis_index("xh")
    t = y * NX + xh
    half = up_ref.shape[1]
    feats = tok_ref.shape[1]
    pair = {"xl": 1 - xl}
    core = {"section": 1 - section}
    mirror = {"z": t, "y": z // NX, "xh": z % NX}
    off_diag = z != t

    def to_tensor(k):
        return {"y": k // NX, "xh": k % NX}

    def tensor_at(i):
        k = i % NY
        step = k + (k // 2) * (1 - 2 * (k % 2))
        return ((y + step) % NY) * NX + (xh + i // NY) % NX

    def z_at(i):
        return (z + ring_offset(i) + NZ) % NZ

    def rdma(src, dst, ssem, rsem, dev):
        return pltpu.make_async_remote_copy(
            src_ref=src, dst_ref=dst, send_sem=ssem, recv_sem=rsem,
            device_id=dev, device_id_type=MESH,
        )

    barrier = pltpu.get_barrier_semaphore()

    @pl.loop(1, NZ)
    def _(i):
        pl.semaphore_signal(barrier, inc=1, device_id={"z": z_at(i)}, device_id_type=MESH)

    @pl.loop(1, NT)
    def _(i):
        pl.semaphore_signal(barrier, inc=1, device_id=to_tensor(tensor_at(i)), device_id_type=MESH)

    pl.semaphore_signal(barrier, inc=1, device_id=pair, device_id_type=MESH)
    pl.semaphore_signal(barrier, inc=1, device_id=core, device_id_type=MESH)

    @pl.when(off_diag)
    def _():
        pl.semaphore_signal(barrier, inc=1, device_id=mirror, device_id_type=MESH)
        pl.semaphore_wait(barrier, NZ + NT + 1)

    @pl.when(z == t)
    def _():
        pl.semaphore_wait(barrier, NZ + NT)

    tok_send = rdma(tok_ref, x_all.at[z], xin_s, xin_r, mirror)
    tok_here = pltpu.make_async_copy(tok_ref, x_all.at[t], xin_r)
    x_in = rdma(x_all.at[t], x_all.at[t], xin_s, xin_r, mirror)
    gain_send = rdma(gain_ref, gain_z, gain_s, gain_r, mirror)
    gain_here = pltpu.make_async_copy(gain_ref, gain_z, gain_r)
    cot_part = cot_ref.at[0, :, pl.ds(pl.multiple_of(t * feats, 128), feats)]
    cot_send = rdma(cot_part, c_all.at[z], cotp_s, cotp_r, mirror)
    cot_here = pltpu.make_async_copy(cot_part, c_all.at[t], cotp_r)
    cot_in = rdma(c_all.at[t], c_all.at[t], cotp_s, cotp_r, mirror)

    @pl.when(off_diag & (section == 0))
    def _():
        tok_send.start()

    @pl.when((z == t) & (section == 0))
    def _():
        tok_here.start()

    @pl.when(off_diag)
    def _():
        gain_send.start()

    @pl.when(z == t)
    def _():
        gain_here.start()

    mine = pl.ds(pl.multiple_of(xl * half, 128), half)
    up_send = rdma(up_ref.at[0], up_pair.at[mine], up_s, up_r, pair)
    up_send.start()

    @pl.when(off_diag)
    def _():
        cot_send.start()

    @pl.when(z == t)
    def _():
        cot_here.start()

    down_send = rdma(down_ref.at[0], down_pair.at[xl], down_s, down_r, pair)
    down_send.start()
    up_pair[mine, :] = up_ref[0]
    down_pair[xl] = down_ref[0]

    gain_send.wait_recv()
    x_in.wait_recv()

    def spread(i):
        return rdma(x_all.at[t], x_all.at[t], ag_s.at[i], ag_r.at[t], to_tensor(tensor_at(i)))

    @pl.loop(1, NT)
    def _(i):
        spread(i).start()

    up_send.wait_recv()
    gain_f = gain_z[...].astype(F32)
    up_all = up_pair

    def part_copy(k):
        return rdma(part_out.at[k], part_in.at[z], rz_s.at[k], rz_r.at[z], {"z": k})

    def sq_copy(k):
        return rdma(sq_out.at[k], sq_in.at[z], sq_s.at[k], sq_r.at[z], {"z": k})

    @pl.loop(0, NT)
    def _(i):
        k = tensor_at(i)

        @pl.when(i > 0)
        def _():
            rdma(x_all.at[k], x_all.at[k], ag_s.at[i], ag_r.at[k], to_tensor(k)).wait_recv()

        x_f = x_all[k].astype(F32)
        sq = x_f * x_f
        sq_hi = sq.astype(BF16)
        sq_lo = (sq - sq_hi.astype(F32)).astype(BF16)
        ones = jnp.ones((8, feats), BF16)
        row_dims = (((1,), (1,)), ((), ()))
        sq_row = lax.dot_general(ones, sq_hi, row_dims, preferred_element_type=F32)
        sq_row = sq_row + lax.dot_general(ones, sq_lo, row_dims, preferred_element_type=F32)
        scaled = (x_f * gain_f).astype(BF16)
        part = jnp.dot(scaled, up_all[...], preferred_element_type=F32).astype(BF16)

        @pl.when(k == z)
        def _():
            part_in[k] = part
            sq_in[k] = sq_row

        @pl.when(k != z)
        def _():
            part_out[k] = part
            sq_out[k] = sq_row
            part_copy(k).start()
            sq_copy(k).start()

    cot_in.wait_recv()

    def cot_spread(i):
        return rdma(c_all.at[t], c_all.at[t], cg_s.at[i], cg_r.at[t], to_tensor(tensor_at(i)))

    @pl.loop(1, NT)
    def _(i):
        cot_spread(i).start()

    acc[...] = part_in[z].astype(F32)

    def add_square(i, total):
        k = z_at(i)
        rdma(part_out.at[k], part_in.at[k], rz_s.at[k], rz_r.at[k], {"z": k}).wait_recv()
        rdma(sq_out.at[k], sq_in.at[k], sq_s.at[k], sq_r.at[k], {"z": k}).wait_recv()
        acc[...] += part_in[k].astype(F32)
        return total + sq_in[k]

    sq_sum = lax.fori_loop(1, NZ, add_square, sq_in[z])
    tokens = acc.shape[0]
    mean_col = jnp.transpose(jnp.broadcast_to(sq_sum[0:1, :], (tokens, tokens)))[:, 0:1] / width
    pre_act = acc[...] * lax.rsqrt(mean_col + EPS)
    hid_all[z] = jax.nn.gelu(pre_act, approximate=True).astype(BF16)

    def hid_spread(i):
        return rdma(hid_all.at[z], hid_all.at[z], az_s.at[i], az_r.at[z], {"z": z_at(i)})

    @pl.loop(1, NZ)
    def _(i):
        hid_spread(i).start()

    down_send.wait_recv()

    def y_copy(k):
        return rdma(y_out.at[k], y_in.at[t], rt_s.at[k], rt_r.at[t], to_tensor(k))

    @pl.loop(0, NZ)
    def _(i):
        k = z_at(i)

        @pl.when(i > 0)
        def _():
            rdma(hid_all.at[k], hid_all.at[k], az_s.at[i], az_r.at[k], {"z": k}).wait_recv()

        hid = hid_all[k]
        y_lo = jnp.dot(hid, down_pair[0], preferred_element_type=F32).astype(BF16)
        y_hi = jnp.dot(hid, down_pair[1], preferred_element_type=F32).astype(BF16)

        @pl.when(k == t)
        def _():
            y_in[k, :, 0:half] = y_lo
            y_in[k, :, half:] = y_hi

        @pl.when(k != t)
        def _():
            y_out[k, :, 0:half] = y_lo
            y_out[k, :, half:] = y_hi
            y_copy(k).start()

    @pl.loop(1, NT)
    def _(i):
        k = tensor_at(i)
        rdma(c_all.at[k], c_all.at[k], cg_s.at[i], cg_r.at[k], to_tensor(k)).wait_recv()

    hid_t = hid_all[...].reshape(NZ * tokens, hid_all.shape[2])

    def grad_half(which):
        cols = pl.ds(pl.multiple_of(which * half, 128), half)
        cot = c_all[:, :, cols].reshape(NZ * tokens, half)
        return lax.dot_general(hid_t, cot, (((0,), (0,)), ((), ())), preferred_element_type=F32)

    grad_out[...] = grad_half(1 - xl).astype(BF16)
    grad_send = rdma(grad_out, grad_in, gr_s, gr_r, pair)
    grad_send.start()
    grad_own[...] = grad_half(xl)

    acc_y = x_all[t].astype(F32) + y_in[t].astype(F32)

    def add_y(i, total):
        k = tensor_at(i)
        rdma(y_out.at[k], y_in.at[k], rt_s.at[k], rt_r.at[k], to_tensor(k)).wait_recv()
        return total + y_in[k].astype(F32)

    x_next[...] = lax.fori_loop(1, NT, add_y, acc_y).astype(BF16)

    core_send = rdma(x_next, x_all.at[t], core_s, xin_r, core)
    state_send = rdma(x_next, state_ref.at[0], out_s, out_r, mirror)
    state_here = pltpu.make_async_copy(x_next, state_ref.at[0], out_r)

    @pl.when(section == 0)
    def _():
        core_send.start()

    @pl.when(off_diag)
    def _():
        state_send.start()

    @pl.when(z == t)
    def _():
        state_here.start()

    grad_send.wait_recv()
    grad_ref[0] = (grad_own[...] + grad_in[...].astype(F32)).astype(BF16)

    @pl.when(section == 0)
    def _():
        core_send.wait_send()

    @pl.when(off_diag & (section == 0))
    def _():
        tok_send.wait_send()

    @pl.when(off_diag)
    def _():
        gain_send.wait_send()
        cot_send.wait_send()
        state_send.wait_send()

    up_send.wait_send()
    down_send.wait_send()
    grad_send.wait_send()

    @pl.loop(1, NT)
    def _(i):
        spread(i).wait_send()
        cot_spread(i).wait_send()
        y_copy(tensor_at(i)).wait_send()

    @pl.loop(1, NZ)
    def _(i):
        part_copy(z_at(i)).wait_send()
        sq_copy(z_at(i)).wait_send()
        hid_spread(i).wait_send()

    state_send.wait_recv()


def body(tokens, gain, w_up, w_down, cotangent):
    rows, feats = tokens.shape
    half, hidden = w_up.shape[1:]
    width = cotangent.shape[2]
    dma = pltpu.SemaphoreType.DMA
    vmem = pl.BlockSpec(memory_space=pltpu.VMEM)

    def run(*refs):
        kernel(width, *refs)

    one = dma(())
    states, grads = pl.pallas_call(
        run,
        out_shape=(
            jax.ShapeDtypeStruct((1, rows, feats), BF16),
            jax.ShapeDtypeStruct((1, hidden, half), BF16),
        ),
        in_specs=[vmem] * 5,
        out_specs=(vmem, vmem),
        scratch_shapes=[
            pltpu.VMEM((NT, rows, feats), BF16),
            pltpu.VMEM((NT, rows, feats), BF16),
            pltpu.VMEM((1, feats), BF16),
            pltpu.VMEM((2 * half, hidden), BF16),
            pltpu.VMEM((2, hidden, half), BF16),
            pltpu.VMEM((NZ, rows, hidden), BF16),
            pltpu.VMEM((NZ, rows, hidden), BF16),
            pltpu.VMEM((NZ, 8, rows), F32),
            pltpu.VMEM((NZ, 8, rows), F32),
            pltpu.VMEM((rows, hidden), F32),
            pltpu.VMEM((NZ, rows, hidden), BF16),
            pltpu.VMEM((NT, rows, feats), BF16),
            pltpu.VMEM((NT, rows, feats), BF16),
            pltpu.VMEM((rows, feats), BF16),
            pltpu.VMEM((hidden, half), F32),
            pltpu.VMEM((hidden, half), BF16),
            pltpu.VMEM((hidden, half), BF16),
        ]
        + [one] * 11
        + [dma((8,))] * 12
        + [one] * 4,
        compiler_params=pltpu.CompilerParams(
            collective_id=0, has_side_effects=True, vmem_limit_bytes=48 * 1024 * 1024
        ),
    )(tokens, gain, w_up, w_down, cotangent)
    return states, grads


def solution(mesh):
    torus = Mesh(
        mesh.devices.reshape(mesh.shape["section"], NZ, 2, NY, NX),
        ("section", "z", "xl", "y", "xh"),
    )
    dp, tensor = ("z", "xl"), ("y", "xh")
    in_specs = (
        P(dp, tensor),
        P("section", tensor),
        P("section", dp, tensor),
        P("section", tensor, dp),
        P("section", dp, None),
    )
    out_specs = (P("section", dp, tensor), P("section", tensor, dp))
    return jax.shard_map(body, mesh=torus, in_specs=in_specs, out_specs=out_specs, check_vma=False)
```

```python
import jax
import jax.numpy as jnp
from jax import lax
from jax.experimental import pallas as pl
from jax.experimental.pallas import tpu as pltpu
from jax.sharding import Mesh
from jax.sharding import PartitionSpec as P

EPS = 1e-06
MESH = pl.DeviceIdType.MESH
NZ, NY, NX = 8, 4, 2
NT = NY * NX
PARTS = 2
F32, BF16 = jnp.float32, jnp.bfloat16


def ring_offset(i):
    return ((i + 1) // 2) * (1 - 2 * ((i + 1) % 2))


def kernel(
    width,
    tok_ref, gain_ref, up_ref, down_ref, cot_ref,
    state_ref, grad_ref,
    x_all, c_all, gain_z, up_pair, down_pair,
    part_out, part_in, sq_out, sq_in, acc, hid_all, y_out, y_in, x_next,
    grad_own, grad_out, grad_in, grad_done,
    gain_s, gain_r, cotp_s, cotp_r, up_s, up_r, down_s, down_r, upl, downl,
    gr_s, gr_r, gd_s, cg_s, cg_r,
    xin_s, xin_r, core_s, out_s, out_r,
    ag_s, ag_r, rz_s, rz_r, sq_s, sq_r, az_s, az_r, rt_s, rt_r,
    go,
):
    section = lax.axis_index("section")
    z = lax.axis_index("z")
    xl = lax.axis_index("xl")
    y = lax.axis_index("y")
    xh = lax.axis_index("xh")
    t = y * NX + xh
    half = up_ref.shape[1]
    feats = tok_ref.shape[1]
    tokens = tok_ref.shape[0]
    rows = tokens // PARTS
    hidden = up_ref.shape[2]
    pair = {"xl": 1 - xl}
    core = {"section": 1 - section}
    mirror = {"z": t, "y": z // NX, "xh": z % NX}
    off_diag = z != t

    def to_tensor(k):
        return {"y": k // NX, "xh": k % NX}

    def tensor_at(i):
        k = i % NY
        step = k + (k // 2) * (1 - 2 * (k % 2))
        return ((y + step) % NY) * NX + (xh + i // NY) % NX

    def z_at(i):
        return (z + ring_offset(i) + NZ) % NZ

    def part(m):
        return pl.ds(m * rows, rows)

    def rdma(src, dst, ssem, rsem, dev):
        return pltpu.make_async_remote_copy(
            src_ref=src, dst_ref=dst, send_sem=ssem, recv_sem=rsem,
            device_id=dev, device_id_type=MESH,
        )

    with jax.named_scope("barrier"):
        mine = pl.ds(pl.multiple_of(xl * half, 128), half)
        up_here = pltpu.make_async_copy(up_ref.at[0], up_pair.at[mine], upl)
        down_here = pltpu.make_async_copy(down_ref.at[0], down_pair.at[xl], downl)
        up_here.start()
        down_here.start()
        barrier = pltpu.get_barrier_semaphore()

        @pl.loop(1, NZ)
        def _(i):
            pl.semaphore_signal(barrier, inc=1, device_id={"z": z_at(i)}, device_id_type=MESH)

        @pl.loop(1, NT)
        def _(i):
            pl.semaphore_signal(
                barrier, inc=1, device_id=to_tensor(tensor_at(i)), device_id_type=MESH
            )

        pl.semaphore_signal(barrier, inc=1, device_id=pair, device_id_type=MESH)
        pl.semaphore_signal(barrier, inc=1, device_id=core, device_id_type=MESH)

        @pl.when(off_diag)
        def _():
            pl.semaphore_signal(barrier, inc=1, device_id=mirror, device_id_type=MESH)
            pl.semaphore_wait(barrier, NZ + NT + 1)

        @pl.when(z == t)
        def _():
            pl.semaphore_wait(barrier, NZ + NT)

    def tok_send(m):
        return rdma(tok_ref.at[part(m)], x_all.at[z, part(m)], xin_s.at[m], xin_r.at[m], mirror)

    def tok_here(m):
        return pltpu.make_async_copy(tok_ref.at[part(m)], x_all.at[t, part(m)], xin_r.at[m])

    def x_in(m):
        return rdma(x_all.at[t, part(m)], x_all.at[t, part(m)], xin_s.at[m], xin_r.at[m], mirror)

    gain_send = rdma(gain_ref, gain_z, gain_s, gain_r, mirror)
    gain_here = pltpu.make_async_copy(gain_ref, gain_z, gain_r)
    cot_part = cot_ref.at[0, :, pl.ds(pl.multiple_of(t * feats, 128), feats)]
    cot_send = rdma(cot_part, c_all.at[z], cotp_s, cotp_r, mirror)
    cot_here = pltpu.make_async_copy(cot_part, c_all.at[t], cotp_r)
    cot_in = rdma(c_all.at[t], c_all.at[t], cotp_s, cotp_r, mirror)
    up_send = rdma(up_ref.at[0], up_pair.at[mine], up_s, up_r, pair)
    down_send = rdma(down_ref.at[0], down_pair.at[xl], down_s, down_r, pair)

    def start_cot():
        @pl.when(off_diag)
        def _():
            cot_send.start()

        @pl.when(z == t)
        def _():
            cot_here.start()

    def go_on():
        pl.semaphore_signal(go, inc=1, device_id=core, device_id_type=MESH)

    with jax.named_scope("send0"):
        @pl.when(off_diag & (section == 0))
        def _():
            for m in range(PARTS):
                tok_send(m).start()

        @pl.when((z == t) & (section == 0))
        def _():
            for m in range(PARTS):
                tok_here(m).start()

        @pl.when(off_diag)
        def _():
            gain_send.start()

        @pl.when(z == t)
        def _():
            gain_here.start()

    with jax.named_scope("background"):
        @pl.when(section == 0)
        def _():
            up_send.start()

        @pl.when(section == 1)
        def _():
            pl.semaphore_wait(go, 1)
            start_cot()
            pl.semaphore_wait(go, 1)
            up_send.start()
            down_send.start()

    def spread(m, i):
        return rdma(
            x_all.at[t, part(m)], x_all.at[t, part(m)],
            ag_s.at[m * NT + i], ag_r.at[m * NT + t], to_tensor(tensor_at(i)),
        )

    def take_x(m):
        x_in(m).wait_recv()

        @pl.loop(1, NT)
        def _(i):
            spread(m, i).start()

    with jax.named_scope("waitx"):
        take_x(0)

        @pl.when(section == 0)
        def _():
            for m in range(1, PARTS):
                take_x(m)
            go_on()
            start_cot()

    with jax.named_scope("waitup"):
        gain_send.wait_recv()
        up_here.wait()
        up_send.wait_recv()

    def part_copy(m, k):
        return rdma(
            part_out.at[k, part(m)], part_in.at[z, part(m)],
            rz_s.at[m * NZ + k], rz_r.at[m * NZ + z], {"z": k},
        )

    def sq_copy(m, k):
        return rdma(
            sq_out.at[m, k], sq_in.at[m, z], sq_s.at[m * NZ + k], sq_r.at[m * NZ + z], {"z": k}
        )

    def up_stage(m):
        gain_f = gain_z[...].astype(F32)

        @pl.loop(0, NT)
        def _(i):
            k = tensor_at(i)

            @pl.when(i > 0)
            def _():
                rdma(
                    x_all.at[k, part(m)], x_all.at[k, part(m)],
                    ag_s.at[m * NT + i], ag_r.at[m * NT + k], to_tensor(k),
                ).wait_recv()

            x_f = x_all[k, m * rows:(m + 1) * rows].astype(F32)
            sq = jnp.concatenate([x_f * x_f] * PARTS, axis=0)
            sq_hi = sq.astype(BF16)
            sq_lo = (sq - sq_hi.astype(F32)).astype(BF16)
            ones = jnp.ones((8, feats), BF16)
            row_dims = (((1,), (1,)), ((), ()))
            sq_row = lax.dot_general(ones, sq_hi, row_dims, preferred_element_type=F32)
            sq_row = sq_row + lax.dot_general(ones, sq_lo, row_dims, preferred_element_type=F32)
            scaled = (x_f * gain_f).astype(BF16)
            value = jnp.dot(scaled, up_pair[...], preferred_element_type=F32).astype(BF16)

            @pl.when(k == z)
            def _():
                part_in[k, m * rows:(m + 1) * rows] = value
                sq_in[m, k] = sq_row

            @pl.when(k != z)
            def _():
                part_out[k, m * rows:(m + 1) * rows] = value
                sq_out[m, k] = sq_row
                part_copy(m, k).start()
                sq_copy(m, k).start()

    def hid_spread(m, i):
        return rdma(
            hid_all.at[z, part(m)], hid_all.at[z, part(m)],
            az_s.at[m * NZ + i], az_r.at[m * NZ + z], {"z": z_at(i)},
        )

    def hid_stage(m):
        acc[...] = part_in[z, m * rows:(m + 1) * rows].astype(F32)

        def add_square(i, total):
            k = z_at(i)
            rdma(
                part_out.at[k, part(m)], part_in.at[k, part(m)],
                rz_s.at[m * NZ + k], rz_r.at[m * NZ + k], {"z": k},
            ).wait_recv()
            rdma(
                sq_out.at[m, k], sq_in.at[m, k],
                sq_s.at[m * NZ + k], sq_r.at[m * NZ + k], {"z": k},
            ).wait_recv()
            acc[...] += part_in[k, m * rows:(m + 1) * rows].astype(F32)
            return total + sq_in[m, k]

        sq_sum = lax.fori_loop(1, NZ, add_square, sq_in[m, z])
        square = jnp.transpose(jnp.broadcast_to(sq_sum[0:1, :], (tokens, tokens)))
        mean_col = square[0:rows, 0:1] / width
        pre_act = acc[...] * lax.rsqrt(mean_col + EPS)
        hid_all[z, m * rows:(m + 1) * rows] = jax.nn.gelu(pre_act, approximate=True).astype(BF16)

        @pl.loop(1, NZ)
        def _(i):
            hid_spread(m, i).start()

    def y_copy(m, k):
        return rdma(
            y_out.at[k, part(m)], y_in.at[t, part(m)],
            rt_s.at[m * NT + k], rt_r.at[m * NT + t], to_tensor(k),
        )

    def down_stage(m):
        @pl.loop(0, NZ)
        def _(i):
            k = z_at(i)

            @pl.when(i > 0)
            def _():
                rdma(
                    hid_all.at[k, part(m)], hid_all.at[k, part(m)],
                    az_s.at[m * NZ + i], az_r.at[m * NZ + k], {"z": k},
                ).wait_recv()

            hid = hid_all[k, m * rows:(m + 1) * rows]
            y_lo = jnp.dot(hid, down_pair[0], preferred_element_type=F32).astype(BF16)
            y_hi = jnp.dot(hid, down_pair[1], preferred_element_type=F32).astype(BF16)

            @pl.when(k == t)
            def _():
                y_in[k, m * rows:(m + 1) * rows, 0:half] = y_lo
                y_in[k, m * rows:(m + 1) * rows, half:] = y_hi

            @pl.when(k != t)
            def _():
                y_out[k, m * rows:(m + 1) * rows, 0:half] = y_lo
                y_out[k, m * rows:(m + 1) * rows, half:] = y_hi
                y_copy(m, k).start()

    def core_send(m):
        return rdma(x_next.at[part(m)], x_all.at[t, part(m)], core_s.at[m], xin_r.at[m], core)

    def state_send(m):
        return rdma(x_next.at[part(m)], state_ref.at[0, part(m)], out_s.at[m], out_r.at[m], mirror)

    def state_here(m):
        return pltpu.make_async_copy(x_next.at[part(m)], state_ref.at[0, part(m)], out_r.at[m])

    def next_stage(m):
        def add_y(i, total):
            k = tensor_at(i)
            rdma(
                y_out.at[k, part(m)], y_in.at[k, part(m)],
                rt_s.at[m * NT + k], rt_r.at[m * NT + k], to_tensor(k),
            ).wait_recv()
            return total + y_in[k, m * rows:(m + 1) * rows].astype(F32)

        first = x_all[t, m * rows:(m + 1) * rows].astype(F32)
        first = first + y_in[t, m * rows:(m + 1) * rows].astype(F32)
        x_next[m * rows:(m + 1) * rows] = lax.fori_loop(1, NT, add_y, first).astype(BF16)

        @pl.when(section == 0)
        def _():
            core_send(m).start()

        @pl.when(off_diag)
        def _():
            state_send(m).start()

        @pl.when(z == t)
        def _():
            state_here(m).start()

    def cot_spread(i):
        return rdma(c_all.at[t], c_all.at[t], cg_s.at[i], cg_r.at[t], to_tensor(tensor_at(i)))

    for m in range(PARTS):
        if m > 0:
            with jax.named_scope("waitx%d" % m):
                @pl.when(section == 1)
                def _():
                    take_x(m)
        with jax.named_scope("up%d" % m):
            up_stage(m)

    with jax.named_scope("waitcot"):
        @pl.when(section == 0)
        def _():
            down_send.start()
            go_on()

        cot_in.wait_recv()

        @pl.loop(1, NT)
        def _(i):
            cot_spread(i).start()

    for m in range(PARTS):
        with jax.named_scope("hid%d" % m):
            hid_stage(m)

    with jax.named_scope("waitdown"):
        down_here.wait()
        down_send.wait_recv()

    for m in range(PARTS - 1):
        with jax.named_scope("down%d" % m):
            down_stage(m)
        with jax.named_scope("next%d" % m):
            next_stage(m)
    with jax.named_scope("down%d" % (PARTS - 1)):
        down_stage(PARTS - 1)

    with jax.named_scope("waitcg"):
        @pl.loop(1, NT)
        def _(i):
            k = tensor_at(i)
            rdma(c_all.at[k], c_all.at[k], cg_s.at[i], cg_r.at[k], to_tensor(k)).wait_recv()

    def grad_half(which):
        hid_t = hid_all[...].reshape(NZ * tokens, hidden)
        cols = pl.ds(pl.multiple_of(which * half, 128), half)
        cot = c_all[:, :, cols].reshape(NZ * tokens, half)
        return lax.dot_general(hid_t, cot, (((0,), (0,)), ((), ())), preferred_element_type=F32)

    grad_send = rdma(grad_out, grad_in, gr_s, gr_r, pair)

    def grad_stage():
        grad_out[...] = grad_half(1 - xl).astype(BF16)
        grad_send.start()
        grad_own[...] = grad_half(xl)

    with jax.named_scope("grad1"):
        @pl.when(section == 1)
        def _():
            grad_stage()

    with jax.named_scope("next%d" % (PARTS - 1)):
        next_stage(PARTS - 1)

    with jax.named_scope("grad0"):
        @pl.when(section == 0)
        def _():
            grad_stage()

    with jax.named_scope("waitgrad"):
        grad_send.wait_recv()
        grad_done[...] = (grad_own[...] + grad_in[...].astype(F32)).astype(BF16)
        grad_store = pltpu.make_async_copy(grad_done, grad_ref.at[0], gd_s)
        grad_store.start()

    with jax.named_scope("drain"):
        @pl.when(section == 0)
        def _():
            for m in range(PARTS):
                core_send(m).wait_send()

        @pl.when(off_diag & (section == 0))
        def _():
            for m in range(PARTS):
                tok_send(m).wait_send()

        @pl.when(off_diag)
        def _():
            gain_send.wait_send()
            cot_send.wait_send()
            for m in range(PARTS):
                state_send(m).wait_send()

        up_send.wait_send()
        down_send.wait_send()
        grad_send.wait_send()

        @pl.loop(1, NT)
        def _(i):
            cot_spread(i).wait_send()
            for m in range(PARTS):
                spread(m, i).wait_send()
                y_copy(m, tensor_at(i)).wait_send()

        @pl.loop(1, NZ)
        def _(i):
            for m in range(PARTS):
                part_copy(m, z_at(i)).wait_send()
                sq_copy(m, z_at(i)).wait_send()
                hid_spread(m, i).wait_send()

    with jax.named_scope("waitstate"):
        for m in range(PARTS):
            state_send(m).wait_recv()
        grad_store.wait()


def body(tokens, gain, w_up, w_down, cotangent):
    rows, feats = tokens.shape
    half, hidden = w_up.shape[1:]
    width = cotangent.shape[2]
    dma = pltpu.SemaphoreType.DMA
    vmem = pl.BlockSpec(memory_space=pltpu.VMEM)
    hbm = pl.BlockSpec(memory_space=pl.ANY)

    def run(*refs):
        kernel(width, *refs)

    one = dma(())
    states, grads = pl.pallas_call(
        run,
        out_shape=(
            jax.ShapeDtypeStruct((1, rows, feats), BF16),
            jax.ShapeDtypeStruct((1, hidden, half), BF16),
        ),
        in_specs=[hbm] * 5,
        out_specs=(hbm, hbm),
        scratch_shapes=[
            pltpu.VMEM((NT, rows, feats), BF16),
            pltpu.VMEM((NT, rows, feats), BF16),
            pltpu.VMEM((1, feats), BF16),
            pltpu.VMEM((2 * half, hidden), BF16),
            pltpu.VMEM((2, hidden, half), BF16),
            pltpu.VMEM((NZ, rows, hidden), BF16),
            pltpu.VMEM((NZ, rows, hidden), BF16),
            pltpu.VMEM((PARTS, NZ, 8, rows), F32),
            pltpu.VMEM((PARTS, NZ, 8, rows), F32),
            pltpu.VMEM((rows // PARTS, hidden), F32),
            pltpu.VMEM((NZ, rows, hidden), BF16),
            pltpu.VMEM((NT, rows, feats), BF16),
            pltpu.VMEM((NT, rows, feats), BF16),
            pltpu.VMEM((rows, feats), BF16),
            pltpu.VMEM((hidden, half), F32),
            pltpu.VMEM((hidden, half), BF16),
            pltpu.VMEM((hidden, half), BF16),
            pltpu.VMEM((hidden, half), BF16),
        ]
        + [one] * 13
        + [dma((8,))] * 2
        + [dma((PARTS,))] * 5
        + [dma((8 * PARTS,))] * 10
        + [pltpu.SemaphoreType.REGULAR],
        compiler_params=pltpu.CompilerParams(
            collective_id=0, has_side_effects=True, vmem_limit_bytes=60 * 1024 * 1024
        ),
    )(tokens, gain, w_up, w_down, cotangent)
    return states, grads


def solution(mesh):
    torus = Mesh(
        mesh.devices.reshape(mesh.shape["section"], NZ, 2, NY, NX),
        ("section", "z", "xl", "y", "xh"),
    )
    dp, tensor = ("z", "xl"), ("y", "xh")
    in_specs = (
        P(dp, tensor),
        P("section", tensor),
        P("section", dp, tensor),
        P("section", tensor, dp),
        P("section", dp, None),
    )
    out_specs = (P("section", dp, tensor), P("section", tensor, dp))
    return jax.shard_map(body, mesh=torus, in_specs=in_specs, out_specs=out_specs, check_vma=False)
```

```python
import jax
import jax.numpy as jnp
from jax import lax
from jax.experimental import pallas as pl
from jax.experimental.pallas import tpu as pltpu
from jax.sharding import Mesh
from jax.sharding import PartitionSpec as P

EPS = 1e-06
MESH = pl.DeviceIdType.MESH
NZ, NY, NX = 8, 4, 2
NT = NY * NX
PARTS = 2
F32, BF16 = jnp.float32, jnp.bfloat16


def ring_offset(i):
    return ((i + 1) // 2) * (1 - 2 * ((i + 1) % 2))


def kernel(
    width,
    tok_ref, gain_ref, up_ref, down_ref, cot_ref,
    state_ref, grad_ref,
    x_all, c_all, gain_z, up_pair, down_pair,
    part_out, part_in, sq_out, sq_in, acc, hid_all, y_out, y_in, x_next,
    grad_own, grad_out, grad_in, grad_done,
    gain_s, gain_r, cotp_s, cotp_r, up_s, up_r, down_s, down_r, upl, downl,
    gr_s, gr_r, gd_s, cotl, cg_s, cg_r,
    xin_s, xin_r, core_s, out_s, out_r,
    ag_s, ag_r, rz_s, rz_r, sq_s, sq_r, az_s, az_r, rt_s, rt_r,
    go,
):
    section = lax.axis_index("section")
    z = lax.axis_index("z")
    xl = lax.axis_index("xl")
    y = lax.axis_index("y")
    xh = lax.axis_index("xh")
    t = y * NX + xh
    half = up_ref.shape[1]
    feats = tok_ref.shape[1]
    tokens = tok_ref.shape[0]
    rows = tokens // PARTS
    hidden = up_ref.shape[2]
    pair = {"xl": 1 - xl}
    core = {"section": 1 - section}
    own = (t - z + NT) % NT
    ahead_t = (z + t) % NT
    ahead = {"z": t, "y": ahead_t // NX, "xh": ahead_t % NX}
    back = {"z": own, "y": z // NX, "xh": z % NX}
    moves = (z + t) > 0
    shares_cot = own != z

    def to_tensor(k):
        return {"y": k // NX, "xh": k % NX}

    def tensor_at(i):
        k = i % NY
        step = k + (k // 2) * (1 - 2 * (k % 2))
        return ((y + step) % NY) * NX + (xh + i // NY) % NX

    def block_at(i):
        return (tensor_at(i) - z + NT) % NT

    def z_at(i):
        return (z + ring_offset(i) + NZ) % NZ

    def part(m):
        return pl.ds(m * rows, rows)

    def rdma(src, dst, ssem, rsem, dev):
        return pltpu.make_async_remote_copy(
            src_ref=src, dst_ref=dst, send_sem=ssem, recv_sem=rsem,
            device_id=dev, device_id_type=MESH,
        )

    with jax.named_scope("barrier"):
        mine = pl.ds(pl.multiple_of(xl * half, 128), half)
        up_here = pltpu.make_async_copy(up_ref.at[0], up_pair.at[mine], upl)
        down_here = pltpu.make_async_copy(down_ref.at[0], down_pair.at[xl], downl)
        up_here.start()
        down_here.start()
        barrier = pltpu.get_barrier_semaphore()

        @pl.loop(1, NZ)
        def _(i):
            pl.semaphore_signal(barrier, inc=1, device_id={"z": z_at(i)}, device_id_type=MESH)

        @pl.loop(1, NT)
        def _(i):
            pl.semaphore_signal(
                barrier, inc=1, device_id=to_tensor(tensor_at(i)), device_id_type=MESH
            )

        pl.semaphore_signal(barrier, inc=1, device_id=pair, device_id_type=MESH)
        pl.semaphore_signal(barrier, inc=1, device_id=core, device_id_type=MESH)

        @pl.when(moves)
        def _():
            pl.semaphore_signal(barrier, inc=1, device_id=ahead, device_id_type=MESH)
            pl.semaphore_signal(barrier, inc=1, device_id=back, device_id_type=MESH)
            pl.semaphore_wait(barrier, NZ + NT + 2)

        @pl.when(z + t == 0)
        def _():
            pl.semaphore_wait(barrier, NZ + NT)

    def tok_send(m):
        return rdma(tok_ref.at[part(m)], x_all.at[z, part(m)], xin_s.at[m], xin_r.at[m], ahead)

    def tok_here(m):
        return pltpu.make_async_copy(tok_ref.at[part(m)], x_all.at[own, part(m)], xin_r.at[m])

    def x_in(m):
        return rdma(x_all.at[own, part(m)], x_all.at[own, part(m)], xin_s.at[m], xin_r.at[m], back)

    gain_send = rdma(gain_ref, gain_z, gain_s, gain_r, ahead)
    gain_here = pltpu.make_async_copy(gain_ref, gain_z, gain_r)

    def cot_cols(k):
        return cot_ref.at[0, :, pl.ds(pl.multiple_of(k * feats, 128), feats)]

    cot_send = rdma(cot_cols(own), c_all.at[z], cotp_s, cotp_r, {"z": own})
    cot_in = rdma(c_all.at[own], c_all.at[own], cotp_s, cotp_r, {"z": own})
    cot_here = pltpu.make_async_copy(cot_cols(z), c_all.at[z], cotl)
    up_send = rdma(up_ref.at[0], up_pair.at[mine], up_s, up_r, pair)
    down_send = rdma(down_ref.at[0], down_pair.at[xl], down_s, down_r, pair)

    def start_cot():
        @pl.when(shares_cot)
        def _():
            cot_send.start()

    def cot_spread(i):
        return rdma(
            c_all.at[own], c_all.at[own], cg_s.at[i], cg_r.at[own], to_tensor(tensor_at(i))
        )

    def spread_cot():
        @pl.when(shares_cot)
        def _():
            cot_in.wait_recv()

            @pl.loop(1, NT)
            def _(i):
                cot_spread(i).start()

    def go_on():
        pl.semaphore_signal(go, inc=1, device_id=core, device_id_type=MESH)

    with jax.named_scope("send0"):
        @pl.when(moves & (section == 0))
        def _():
            for m in range(PARTS):
                tok_send(m).start()

        @pl.when((z + t == 0) & (section == 0))
        def _():
            for m in range(PARTS):
                tok_here(m).start()

        @pl.when(moves)
        def _():
            gain_send.start()

        @pl.when(z + t == 0)
        def _():
            gain_here.start()

        cot_here.start()

    with jax.named_scope("background"):
        @pl.when(section == 0)
        def _():
            up_send.start()

        @pl.when(section == 1)
        def _():
            pl.semaphore_wait(go, 1)
            start_cot()
            pl.semaphore_wait(go, 1)
            up_send.start()
            down_send.start()
            spread_cot()

    def spread(m, i):
        return rdma(
            x_all.at[own, part(m)], x_all.at[own, part(m)],
            ag_s.at[m * NT + i], ag_r.at[m * NT + own], to_tensor(tensor_at(i)),
        )

    def take_x(m):
        x_in(m).wait_recv()

        @pl.loop(1, NT)
        def _(i):
            spread(m, i).start()

    with jax.named_scope("waitx"):
        take_x(0)

        @pl.when(section == 0)
        def _():
            for m in range(1, PARTS):
                take_x(m)
            start_cot()
            go_on()

    with jax.named_scope("waitup"):
        gain_send.wait_recv()
        up_here.wait()
        up_send.wait_recv()

    def part_copy(m, k):
        return rdma(
            part_out.at[k, part(m)], part_in.at[z, part(m)],
            rz_s.at[m * NZ + k], rz_r.at[m * NZ + z], {"z": k},
        )

    def sq_copy(m, k):
        return rdma(
            sq_out.at[m, k], sq_in.at[m, z], sq_s.at[m * NZ + k], sq_r.at[m * NZ + z], {"z": k}
        )

    def up_stage(m):
        gain_f = gain_z[...].astype(F32)

        @pl.loop(0, NT)
        def _(i):
            k = block_at(i)

            @pl.when(i > 0)
            def _():
                rdma(
                    x_all.at[k, part(m)], x_all.at[k, part(m)],
                    ag_s.at[m * NT + i], ag_r.at[m * NT + k], to_tensor(tensor_at(i)),
                ).wait_recv()

            x_f = x_all[k, m * rows:(m + 1) * rows].astype(F32)
            sq = jnp.concatenate([x_f * x_f] * PARTS, axis=0)
            sq_hi = sq.astype(BF16)
            sq_lo = (sq - sq_hi.astype(F32)).astype(BF16)
            ones = jnp.ones((8, feats), BF16)
            row_dims = (((1,), (1,)), ((), ()))
            sq_row = lax.dot_general(ones, sq_hi, row_dims, preferred_element_type=F32)
            sq_row = sq_row + lax.dot_general(ones, sq_lo, row_dims, preferred_element_type=F32)
            scaled = (x_f * gain_f).astype(BF16)
            value = jnp.dot(scaled, up_pair[...], preferred_element_type=F32).astype(BF16)

            @pl.when(k == z)
            def _():
                part_in[k, m * rows:(m + 1) * rows] = value
                sq_in[m, k] = sq_row

            @pl.when(k != z)
            def _():
                part_out[k, m * rows:(m + 1) * rows] = value
                sq_out[m, k] = sq_row
                part_copy(m, k).start()
                sq_copy(m, k).start()

    def hid_spread(m, i):
        return rdma(
            hid_all.at[z, part(m)], hid_all.at[z, part(m)],
            az_s.at[m * NZ + i], az_r.at[m * NZ + z], {"z": z_at(i)},
        )

    def hid_stage(m):
        acc[...] = part_in[z, m * rows:(m + 1) * rows].astype(F32)

        def add_square(i, total):
            k = z_at(i)
            rdma(
                part_out.at[k, part(m)], part_in.at[k, part(m)],
                rz_s.at[m * NZ + k], rz_r.at[m * NZ + k], {"z": k},
            ).wait_recv()
            rdma(
                sq_out.at[m, k], sq_in.at[m, k],
                sq_s.at[m * NZ + k], sq_r.at[m * NZ + k], {"z": k},
            ).wait_recv()
            acc[...] += part_in[k, m * rows:(m + 1) * rows].astype(F32)
            return total + sq_in[m, k]

        sq_sum = lax.fori_loop(1, NZ, add_square, sq_in[m, z])
        square = jnp.transpose(jnp.broadcast_to(sq_sum[0:1, :], (tokens, tokens)))
        mean_col = square[0:rows, 0:1] / width
        pre_act = acc[...] * lax.rsqrt(mean_col + EPS)
        hid_all[z, m * rows:(m + 1) * rows] = jax.nn.gelu(pre_act, approximate=True).astype(BF16)

        @pl.loop(1, NZ)
        def _(i):
            hid_spread(m, i).start()

    def y_copy(m, k):
        return rdma(
            y_out.at[k, part(m)], y_in.at[t, part(m)],
            rt_s.at[m * NT + k], rt_r.at[m * NT + t], to_tensor((k + z) % NT),
        )

    def down_stage(m, first, last):
        @pl.loop(first, last)
        def _(i):
            k = z_at(i)

            @pl.when(i > 0)
            def _():
                rdma(
                    hid_all.at[k, part(m)], hid_all.at[k, part(m)],
                    az_s.at[m * NZ + i], az_r.at[m * NZ + k], {"z": k},
                ).wait_recv()

            hid = hid_all[k, m * rows:(m + 1) * rows]
            y_lo = jnp.dot(hid, down_pair[0], preferred_element_type=F32).astype(BF16)
            y_hi = jnp.dot(hid, down_pair[1], preferred_element_type=F32).astype(BF16)

            @pl.when(k == own)
            def _():
                y_in[t, m * rows:(m + 1) * rows, 0:half] = y_lo
                y_in[t, m * rows:(m + 1) * rows, half:] = y_hi

            @pl.when(k != own)
            def _():
                y_out[k, m * rows:(m + 1) * rows, 0:half] = y_lo
                y_out[k, m * rows:(m + 1) * rows, half:] = y_hi
                y_copy(m, k).start()

    def core_send(m):
        return rdma(x_next.at[part(m)], x_all.at[own, part(m)], core_s.at[m], xin_r.at[m], core)

    def state_send(m):
        return rdma(x_next.at[part(m)], state_ref.at[0, part(m)], out_s.at[m], out_r.at[m], back)

    def state_here(m):
        return pltpu.make_async_copy(x_next.at[part(m)], state_ref.at[0, part(m)], out_r.at[m])

    def next_stage(m):
        def add_y(i, total):
            k = tensor_at(i)
            rdma(
                y_out.at[k, part(m)], y_in.at[k, part(m)],
                rt_s.at[m * NT + k], rt_r.at[m * NT + k], to_tensor(k),
            ).wait_recv()
            return total + y_in[k, m * rows:(m + 1) * rows].astype(F32)

        first = x_all[own, m * rows:(m + 1) * rows].astype(F32)
        first = first + y_in[t, m * rows:(m + 1) * rows].astype(F32)
        x_next[m * rows:(m + 1) * rows] = lax.fori_loop(1, NT, add_y, first).astype(BF16)

        @pl.when(section == 0)
        def _():
            core_send(m).start()

        @pl.when(section == 1)
        def _():
            store_state(m)

    def store_state(m):
        @pl.when(moves)
        def _():
            state_send(m).start()

        @pl.when(z + t == 0)
        def _():
            state_here(m).start()

    for m in range(PARTS):
        if m > 0:
            with jax.named_scope("waitx%d" % m):
                @pl.when(section == 1)
                def _():
                    take_x(m)
        with jax.named_scope("up%d" % m):
            up_stage(m)

    with jax.named_scope("after_up"):
        @pl.when(section == 0)
        def _():
            down_send.start()

        go_on()

    for m in range(PARTS):
        with jax.named_scope("hid%d" % m):
            hid_stage(m)

    with jax.named_scope("waitcot"):
        @pl.when(section == 0)
        def _():
            spread_cot()

    with jax.named_scope("waitdown"):
        down_here.wait()
        down_send.wait_recv()

    with jax.named_scope("down0"):
        down_stage(0, 0, NZ)
    with jax.named_scope("down1a"):
        down_stage(1, 0, NZ // 2 + 1)
    with jax.named_scope("next0"):
        next_stage(0)
    with jax.named_scope("down1b"):
        down_stage(1, NZ // 2 + 1, NZ)

    with jax.named_scope("waitcg"):
        @pl.loop(1, NT)
        def _(i):
            k = block_at(i)

            @pl.when(k != z)
            def _():
                rdma(
                    c_all.at[k], c_all.at[k], cg_s.at[i], cg_r.at[k], to_tensor(tensor_at(i))
                ).wait_recv()

        cot_here.wait()

    def grad_half(which):
        hid_t = hid_all[...].reshape(NZ * tokens, hidden)
        cols = pl.ds(pl.multiple_of(which * half, 128), half)
        cot = c_all[:, :, cols].reshape(NZ * tokens, half)
        return lax.dot_general(hid_t, cot, (((0,), (0,)), ((), ())), preferred_element_type=F32)

    grad_send = rdma(grad_out, grad_in, gr_s, gr_r, pair)

    with jax.named_scope("grad1"):
        @pl.when(section == 1)
        def _():
            grad_out[...] = grad_half(1 - xl).astype(BF16)
            grad_send.start()
            grad_own[...] = grad_half(xl)

    with jax.named_scope("next%d" % (PARTS - 1)):
        next_stage(PARTS - 1)

    with jax.named_scope("grad0"):
        @pl.when(section == 0)
        def _():
            grad_out[...] = grad_half(1 - xl).astype(BF16)
            grad_own[...] = grad_half(xl)
            pl.semaphore_wait(go, 1)
            grad_send.start()
            for m in range(PARTS):
                store_state(m)

    with jax.named_scope("waitgrad"):
        grad_send.wait_recv()
        grad_done[...] = (grad_own[...] + grad_in[...].astype(F32)).astype(BF16)
        grad_store = pltpu.make_async_copy(grad_done, grad_ref.at[0], gd_s)
        grad_store.start()

    with jax.named_scope("drain"):
        @pl.when(section == 0)
        def _():
            for m in range(PARTS):
                core_send(m).wait_send()

        @pl.when(moves & (section == 0))
        def _():
            for m in range(PARTS):
                tok_send(m).wait_send()

        @pl.when(shares_cot)
        def _():
            cot_send.wait_send()

            @pl.loop(1, NT)
            def _(i):
                cot_spread(i).wait_send()

        @pl.when(moves)
        def _():
            gain_send.wait_send()
            for m in range(PARTS):
                state_send(m).wait_send()

        up_send.wait_send()
        down_send.wait_send()
        grad_send.wait_send()

        @pl.loop(1, NT)
        def _(i):
            for m in range(PARTS):
                spread(m, i).wait_send()
                y_copy(m, block_at(i)).wait_send()

        @pl.loop(1, NZ)
        def _(i):
            for m in range(PARTS):
                part_copy(m, z_at(i)).wait_send()
                sq_copy(m, z_at(i)).wait_send()
                hid_spread(m, i).wait_send()

    with jax.named_scope("waitstate"):
        for m in range(PARTS):
            state_send(m).wait_recv()
        grad_store.wait()


def body(tokens, gain, w_up, w_down, cotangent):
    rows, feats = tokens.shape
    half, hidden = w_up.shape[1:]
    width = cotangent.shape[2]
    dma = pltpu.SemaphoreType.DMA
    vmem = pl.BlockSpec(memory_space=pltpu.VMEM)
    hbm = pl.BlockSpec(memory_space=pl.ANY)

    def run(*refs):
        kernel(width, *refs)

    one = dma(())
    states, grads = pl.pallas_call(
        run,
        out_shape=(
            jax.ShapeDtypeStruct((1, rows, feats), BF16),
            jax.ShapeDtypeStruct((1, hidden, half), BF16),
        ),
        in_specs=[hbm] * 5,
        out_specs=(hbm, hbm),
        scratch_shapes=[
            pltpu.VMEM((NT, rows, feats), BF16),
            pltpu.VMEM((NT, rows, feats), BF16),
            pltpu.VMEM((1, feats), BF16),
            pltpu.VMEM((2 * half, hidden), BF16),
            pltpu.VMEM((2, hidden, half), BF16),
            pltpu.VMEM((NZ, rows, hidden), BF16),
            pltpu.VMEM((NZ, rows, hidden), BF16),
            pltpu.VMEM((PARTS, NZ, 8, rows), F32),
            pltpu.VMEM((PARTS, NZ, 8, rows), F32),
            pltpu.VMEM((rows // PARTS, hidden), F32),
            pltpu.VMEM((NZ, rows, hidden), BF16),
            pltpu.VMEM((NT, rows, feats), BF16),
            pltpu.VMEM((NT, rows, feats), BF16),
            pltpu.VMEM((rows, feats), BF16),
            pltpu.VMEM((hidden, half), F32),
            pltpu.VMEM((hidden, half), BF16),
            pltpu.VMEM((hidden, half), BF16),
            pltpu.VMEM((hidden, half), BF16),
        ]
        + [one] * 14
        + [dma((8,))] * 2
        + [dma((PARTS,))] * 5
        + [dma((8 * PARTS,))] * 10
        + [pltpu.SemaphoreType.REGULAR],
        compiler_params=pltpu.CompilerParams(
            collective_id=0, has_side_effects=True, vmem_limit_bytes=60 * 1024 * 1024
        ),
    )(tokens, gain, w_up, w_down, cotangent)
    return states, grads


def solution(mesh):
    torus = Mesh(
        mesh.devices.reshape(mesh.shape["section"], NZ, 2, NY, NX),
        ("section", "z", "xl", "y", "xh"),
    )
    dp, tensor = ("z", "xl"), ("y", "xh")
    in_specs = (
        P(dp, tensor),
        P("section", tensor),
        P("section", dp, tensor),
        P("section", tensor, dp),
        P("section", dp, None),
    )
    out_specs = (P("section", dp, tensor), P("section", tensor, dp))
    return jax.shard_map(body, mesh=torus, in_specs=in_specs, out_specs=out_specs, check_vma=False)
```

```python
import jax
import jax.numpy as jnp
from jax import lax
from jax.experimental import pallas as pl
from jax.experimental.pallas import tpu as pltpu
from jax.sharding import Mesh
from jax.sharding import PartitionSpec as P

EPS = 1e-06
MESH = pl.DeviceIdType.MESH
NZ, NY, NX = 8, 4, 2
NT = NY * NX
PARTS = 2
UP_SPLIT = 5
F32, BF16 = jnp.float32, jnp.bfloat16


def ring_offset(i):
    return ((i + 1) // 2) * (1 - 2 * ((i + 1) % 2))


def kernel(
    width,
    tok_ref, gain_ref, up_ref, down_ref, cot_ref,
    state_ref, grad_ref,
    x_all, c_all, gain_z, up_pair, down_pair,
    part_out, part_own, part_in, sum_in, sum_out, relay, sq_out, sq_in, acc, hid_all,
    y_out, y_in, x_next,
    grad_own, grad_out, grad_in, grad_done,
    gain_s, gain_r, cotp_s, cotp_r, up_s, up_r, down_s, down_r, upl, downl,
    gr_s, gr_r, gd_s, cotl, cg_s, cg_r,
    xin_s, xin_r, core_s, out_s, out_r,
    ag_s, ag_r, sq_s, sq_r, rt_s, rt_r,
    rz_s, rz_r, sum_r, sum_s, az_s, az_r, rel_r, rel_s,
    go,
):
    section = lax.axis_index("section")
    z = lax.axis_index("z")
    xl = lax.axis_index("xl")
    y = lax.axis_index("y")
    xh = lax.axis_index("xh")
    t = y * NX + xh
    half = up_ref.shape[1]
    feats = tok_ref.shape[1]
    tokens = tok_ref.shape[0]
    rows = tokens // PARTS
    piece = rows // 2
    hidden = up_ref.shape[2]
    pair = {"xl": 1 - xl}
    core = {"section": 1 - section}
    own = (t - z + NT) % NT
    ahead_t = (z + t) % NT
    ahead = {"z": t, "y": ahead_t // NX, "xh": ahead_t % NX}
    back = {"z": own, "y": z // NX, "xh": z % NX}
    moves = (z + t) > 0
    shares_cot = own != z

    def to_tensor(k):
        return {"y": k // NX, "xh": k % NX}

    def tensor_at(i):
        k = i % NY
        step = k + (k // 2) * (1 - 2 * (k % 2))
        return ((y + step) % NY) * NX + (xh + i // NY) % NX

    def block_at(i):
        return (tensor_at(i) - z + NT) % NT

    def z_at(i):
        return (z + ring_offset(i) + NZ) % NZ

    def helper(step):
        return {"section": 1 - section, "z": (z + step + NZ) % NZ}

    def part(m):
        return pl.ds(m * rows, rows)

    def rdma(src, dst, ssem, rsem, dev):
        return pltpu.make_async_remote_copy(
            src_ref=src, dst_ref=dst, send_sem=ssem, recv_sem=rsem,
            device_id=dev, device_id_type=MESH,
        )

    with jax.named_scope("barrier"):
        mine = pl.ds(pl.multiple_of(xl * half, 128), half)
        up_here = pltpu.make_async_copy(up_ref.at[0], up_pair.at[mine], upl)
        down_here = pltpu.make_async_copy(down_ref.at[0], down_pair.at[xl], downl)
        up_here.start()
        down_here.start()
        barrier = pltpu.get_barrier_semaphore()

        @pl.loop(1, NZ)
        def _(i):
            pl.semaphore_signal(barrier, inc=1, device_id={"z": z_at(i)}, device_id_type=MESH)

        @pl.loop(1, NT)
        def _(i):
            pl.semaphore_signal(
                barrier, inc=1, device_id=to_tensor(tensor_at(i)), device_id_type=MESH
            )

        pl.semaphore_signal(barrier, inc=1, device_id=pair, device_id_type=MESH)
        pl.semaphore_signal(barrier, inc=1, device_id=core, device_id_type=MESH)
        for step in (1, -1, 2, -2):
            pl.semaphore_signal(
                barrier, inc=1, device_id=helper(step), device_id_type=MESH
            )

        @pl.when(moves)
        def _():
            pl.semaphore_signal(barrier, inc=1, device_id=ahead, device_id_type=MESH)
            pl.semaphore_signal(barrier, inc=1, device_id=back, device_id_type=MESH)
            pl.semaphore_wait(barrier, NZ + NT + 6)

        @pl.when(z + t == 0)
        def _():
            pl.semaphore_wait(barrier, NZ + NT + 4)

    def tok_send(m):
        return rdma(tok_ref.at[part(m)], x_all.at[z, part(m)], xin_s.at[m], xin_r.at[m], ahead)

    def tok_here(m):
        return pltpu.make_async_copy(tok_ref.at[part(m)], x_all.at[own, part(m)], xin_r.at[m])

    def x_in(m):
        return rdma(x_all.at[own, part(m)], x_all.at[own, part(m)], xin_s.at[m], xin_r.at[m], back)

    gain_send = rdma(gain_ref, gain_z, gain_s, gain_r, ahead)
    gain_here = pltpu.make_async_copy(gain_ref, gain_z, gain_r)

    def cot_cols(k):
        return cot_ref.at[0, :, pl.ds(pl.multiple_of(k * feats, 128), feats)]

    cot_send = rdma(cot_cols(own), c_all.at[z], cotp_s, cotp_r, {"z": own})
    cot_in = rdma(c_all.at[own], c_all.at[own], cotp_s, cotp_r, {"z": own})
    cot_here = pltpu.make_async_copy(cot_cols(z), c_all.at[z], cotl)
    up_send = rdma(up_ref.at[0], up_pair.at[mine], up_s, up_r, pair)
    down_send = rdma(down_ref.at[0], down_pair.at[xl], down_s, down_r, pair)

    def start_cot():
        @pl.when(shares_cot)
        def _():
            cot_send.start()

    beside = (y * NX + 1 - xh - z + NT) % NT

    def cot_spread(i):
        return rdma(
            c_all.at[own], c_all.at[own], cg_s.at[i - 1], cg_r.at[own], to_tensor(tensor_at(i))
        )

    def cot_pass(i):
        return rdma(
            c_all.at[beside], c_all.at[beside], cg_s.at[i + 3], cg_r.at[beside],
            to_tensor(tensor_at(i)),
        )

    def spread_cot():
        @pl.when(shares_cot)
        def _():
            cot_in.wait_recv()
            for i in (NY, 1, 2, 3):
                cot_spread(i).start()

    def pass_cot():
        @pl.when(beside != z)
        def _():
            ref = c_all.at[beside]
            rdma(ref, ref, cg_s.at[0], cg_r.at[beside], pair).wait_recv()
            for i in range(1, NY):
                cot_pass(i).start()

    def sum_wait(m, way, slot):
        span = pl.ds(way * piece, piece) if slot == 2 else pl.ds(0, rows)
        ref = sum_in.at[m, way, slot, span]
        rdma(ref, ref, sum_s.at[0], sum_r.at[m * 6 + way * 3 + slot], core).wait_recv()

    def sum_send(m, way):
        return rdma(
            sum_out.at[m, way], part_in.at[2 + way, part(m)],
            sum_s.at[m * 2 + way], rz_r.at[m * 4 + 2 + way], helper(2 - 4 * way),
        )

    def relay_sum(m):
        for way in range(2):
            for slot in range(3):
                sum_wait(m, way, slot)
            for quarter in range(2):
                span = slice(quarter * piece, (quarter + 1) * piece)
                total = sum_in[m, way, 0, span].astype(F32) + sum_in[m, way, 1, span].astype(F32)
                if quarter == way:
                    total = total + sum_in[m, way, 2, span].astype(F32)
                sum_out[m, way, span] = total.astype(BF16)
            sum_send(m, way).start()

    def relay_sends(m, way):
        sign = 1 - 2 * way
        block = (z - 2 * sign + NZ) % NZ
        slot = m * 6 + way * 3
        first = m * 8 + way * 4
        span = pl.ds(way * piece, piece)
        far = pl.ds(m * rows + way * piece, piece)
        return (
            rdma(
                relay.at[m, way, span], hid_all.at[block, far],
                rel_s.at[slot], az_r.at[first + 3], helper(2 * sign),
            ),
            rdma(
                relay.at[m, way], hid_all.at[block, part(m)],
                rel_s.at[slot + 1], az_r.at[first + 2], helper(sign),
            ),
            rdma(
                relay.at[m, way], hid_all.at[block, part(m)],
                rel_s.at[slot + 2], az_r.at[first + 1], core,
            ),
        )

    def relay_hid(m):
        for way in range(2):
            ref = relay.at[m, way]
            rdma(ref, ref, rel_s.at[0], rel_r.at[m * 2 + way], core).wait_recv()
            for copy in relay_sends(m, way):
                copy.start()

    def go_on():
        pl.semaphore_signal(go, inc=1, device_id=core, device_id_type=MESH)

    with jax.named_scope("send0"):
        @pl.when(moves & (section == 0))
        def _():
            for m in range(PARTS):
                tok_send(m).start()

        @pl.when((z + t == 0) & (section == 0))
        def _():
            for m in range(PARTS):
                tok_here(m).start()

        @pl.when(moves)
        def _():
            gain_send.start()

        @pl.when(z + t == 0)
        def _():
            gain_here.start()

        cot_here.start()

    with jax.named_scope("background"):
        @pl.when(section == 0)
        def _():
            up_send.start()

        @pl.when(section == 1)
        def _():
            pl.semaphore_wait(go, 1)
            start_cot()
            relay_sum(0)
            spread_cot()
            pl.semaphore_wait(go, 1)
            relay_sum(1)
            up_send.start()
            pass_cot()
            relay_hid(0)
            relay_hid(1)
            down_send.start()

    def spread(m, i):
        return rdma(
            x_all.at[own, part(m)], x_all.at[own, part(m)],
            ag_s.at[m * NT + i], ag_r.at[m * NT + own], to_tensor(tensor_at(i)),
        )

    def take_x(m):
        x_in(m).wait_recv()

        @pl.loop(1, NT)
        def _(i):
            spread(m, i).start()

    with jax.named_scope("waitx"):
        take_x(0)

        @pl.when(section == 0)
        def _():
            for m in range(1, PARTS):
                take_x(m)
            start_cot()
            go_on()

    with jax.named_scope("waitup"):
        gain_send.wait_recv()
        up_here.wait()
        up_send.wait_recv()

    def part_copies(m, k, way, dist):
        sign = 1 - 2 * way
        src = part_out.at[k, part(m)]
        slot = m * 8 + way
        if dist == 1:
            return (rdma(src, part_in.at[way, part(m)], rz_s.at[slot], rz_r.at[m * 4 + way], {"z": k}),)
        if dist == 2:
            return (
                rdma(src, sum_in.at[m, way, 0], rz_s.at[slot + 2], sum_r.at[m * 6 + way * 3], core),
            )
        if dist == 3:
            return (
                rdma(
                    src, sum_in.at[m, way, 1], rz_s.at[slot + 4],
                    sum_r.at[m * 6 + way * 3 + 1], helper(sign),
                ),
            )
        return tuple(
            rdma(
                part_out.at[k, pl.ds(m * rows + w * piece, piece)],
                sum_in.at[m, w, 2, pl.ds(w * piece, piece)],
                rz_s.at[m * 8 + 6 + w], sum_r.at[m * 6 + w * 3 + 2], helper(2 - 4 * w),
            )
            for w in range(2)
        )

    def sq_copy(m, k):
        return rdma(
            sq_out.at[m, k], sq_in.at[m, z], sq_s.at[m * NZ + k], sq_r.at[m * NZ + z], {"z": k}
        )

    def up_stage(m, first, last):
        gain_f = gain_z[...].astype(F32)

        @pl.loop(first, last)
        def _(i):
            k = block_at(i)

            @pl.when(i > 0)
            def _():
                rdma(
                    x_all.at[k, part(m)], x_all.at[k, part(m)],
                    ag_s.at[m * NT + i], ag_r.at[m * NT + k], to_tensor(tensor_at(i)),
                ).wait_recv()

            x_f = x_all[k, m * rows:(m + 1) * rows].astype(F32)
            sq = x_f * x_f
            sq = sum(sq[:, c:c + tokens] for c in range(0, feats, tokens))
            sq = jnp.concatenate([sq] * PARTS, axis=0)
            sq_hi = sq.astype(BF16)
            sq_lo = (sq - sq_hi.astype(F32)).astype(BF16)
            ones = jnp.ones((8, tokens), BF16)
            row_dims = (((1,), (1,)), ((), ()))
            sq_row = lax.dot_general(ones, sq_hi, row_dims, preferred_element_type=F32)
            sq_row = sq_row + lax.dot_general(ones, sq_lo, row_dims, preferred_element_type=F32)
            scaled = (x_f * gain_f).astype(BF16)
            value = jnp.dot(scaled, up_pair[...], preferred_element_type=F32).astype(BF16)

            delta = (k - z + NZ) % NZ
            way = delta // 5
            dist = delta + way * (NZ - 2 * delta)

            @pl.when(k == z)
            def _():
                part_own[m * rows:(m + 1) * rows] = value
                sq_in[m, k] = sq_row

            @pl.when(k != z)
            def _():
                part_out[k, m * rows:(m + 1) * rows] = value
                sq_out[m, k] = sq_row

            for far in range(1, 5):
                @pl.when(dist == far)
                def _():
                    for copy in part_copies(m, k, way, far):
                        copy.start()

            @pl.when(k != z)
            def _():
                sq_copy(m, k).start()

    def hid_sends(m):
        block = hid_all.at[z, part(m)]
        out = []
        for way in range(2):
            sign = 1 - 2 * way
            out.append(
                rdma(block, relay.at[m, way], az_s.at[m * 4 + 2 + way], rel_r.at[m * 2 + way], helper(2 * sign))
            )
            out.append(
                rdma(block, block, az_s.at[m * 4 + way], az_r.at[m * 8 + way * 4], {"z": (z + sign + NZ) % NZ})
            )
        return out

    def hid_stage(m):
        span = slice(m * rows, (m + 1) * rows)
        acc[...] = part_own[span].astype(F32)
        for slot in range(4):
            ref = part_in.at[slot, part(m)]
            rdma(ref, ref, rz_s.at[0], rz_r.at[m * 4 + slot], core).wait_recv()
            acc[...] += part_in[slot, span].astype(F32)

        def add_square(i, total):
            k = z_at(i)
            rdma(
                sq_out.at[m, k], sq_in.at[m, k],
                sq_s.at[m * NZ + k], sq_r.at[m * NZ + k], {"z": k},
            ).wait_recv()
            return total + sq_in[m, k]

        sq_sum = lax.fori_loop(1, NZ, add_square, sq_in[m, z])
        square = jnp.transpose(jnp.broadcast_to(sq_sum[0:1, :], (tokens, tokens)))
        mean_col = square[0:rows, 0:1] / width
        pre_act = acc[...] * lax.rsqrt(mean_col + EPS)
        hid_all[z, m * rows:(m + 1) * rows] = jax.nn.gelu(pre_act, approximate=True).astype(BF16)

        for copy in hid_sends(m):
            copy.start()

    def y_copy(m, k):
        return rdma(
            y_out.at[k, part(m)], y_in.at[t, part(m)],
            rt_s.at[m * NT + k], rt_r.at[m * NT + t], to_tensor((k + z) % NT),
        )

    def down_stage(m, first, last):
        @pl.loop(first, last)
        def _(i):
            k = z_at(i)

            @pl.when((i > 0) & (i < NZ - 1))
            def _():
                ref = hid_all.at[k, part(m)]
                slot = m * 8 + (i % 2) * 4 + (i + 1) // 2 - 1
                rdma(ref, ref, az_s.at[0], az_r.at[slot], core).wait_recv()

            @pl.when(i == NZ - 1)
            def _():
                for way in range(2):
                    ref = hid_all.at[k, pl.ds(m * rows + way * piece, piece)]
                    rdma(ref, ref, az_s.at[0], az_r.at[m * 8 + way * 4 + 3], core).wait_recv()

            hid = hid_all[k, m * rows:(m + 1) * rows]
            y_lo = jnp.dot(hid, down_pair[0], preferred_element_type=F32).astype(BF16)
            y_hi = jnp.dot(hid, down_pair[1], preferred_element_type=F32).astype(BF16)

            @pl.when(k == own)
            def _():
                y_in[t, m * rows:(m + 1) * rows, 0:half] = y_lo
                y_in[t, m * rows:(m + 1) * rows, half:] = y_hi

            @pl.when(k != own)
            def _():
                y_out[k, m * rows:(m + 1) * rows, 0:half] = y_lo
                y_out[k, m * rows:(m + 1) * rows, half:] = y_hi
                y_copy(m, k).start()

    def core_send(m):
        return rdma(x_next.at[part(m)], x_all.at[own, part(m)], core_s.at[m], xin_r.at[m], core)

    def state_send(m):
        return rdma(x_next.at[part(m)], state_ref.at[0, part(m)], out_s.at[m], out_r.at[m], back)

    def state_here(m):
        return pltpu.make_async_copy(x_next.at[part(m)], state_ref.at[0, part(m)], out_r.at[m])

    def next_stage(m):
        def add_y(i, total):
            k = tensor_at(i)
            rdma(
                y_out.at[k, part(m)], y_in.at[k, part(m)],
                rt_s.at[m * NT + k], rt_r.at[m * NT + k], to_tensor(k),
            ).wait_recv()
            return total + y_in[k, m * rows:(m + 1) * rows].astype(F32)

        first = x_all[own, m * rows:(m + 1) * rows].astype(F32)
        first = first + y_in[t, m * rows:(m + 1) * rows].astype(F32)
        x_next[m * rows:(m + 1) * rows] = lax.fori_loop(1, NT, add_y, first).astype(BF16)

        @pl.when(section == 0)
        def _():
            core_send(m).start()

        @pl.when(section == 1)
        def _():
            store_state(m)

    def store_state(m):
        @pl.when(moves)
        def _():
            state_send(m).start()

        @pl.when(z + t == 0)
        def _():
            state_here(m).start()

    with jax.named_scope("up0"):
        up_stage(0, 0, UP_SPLIT)
    with jax.named_scope("waitx1"):
        @pl.when(section == 1)
        def _():
            take_x(1)
    with jax.named_scope("up0b"):
        up_stage(0, UP_SPLIT, NT)
    with jax.named_scope("up1"):
        up_stage(1, 0, NT)

    with jax.named_scope("after_up"):
        @pl.when(section == 0)
        def _():
            down_send.start()

        go_on()

    for m in range(PARTS):
        with jax.named_scope("hid%d" % m):
            hid_stage(m)

    with jax.named_scope("waitdown"):
        down_here.wait()
        down_send.wait_recv()

    with jax.named_scope("down0"):
        down_stage(0, 0, NZ)
    with jax.named_scope("down1a"):
        down_stage(1, 0, NZ // 2 + 1)
    with jax.named_scope("next0"):
        next_stage(0)
    with jax.named_scope("down1b"):
        down_stage(1, NZ // 2 + 1, NZ)

    def wait_cot():
        @pl.loop(1, NT)
        def _(i):
            k = block_at(i)

            @pl.when((k != z) & (i != NY))
            def _():
                ref = c_all.at[k]
                rdma(ref, ref, cg_s.at[0], cg_r.at[k], pair).wait_recv()

        cot_here.wait()

    def grad_half(which):
        hid_t = hid_all[...].reshape(NZ * tokens, hidden)
        cols = pl.ds(pl.multiple_of(which * half, 128), half)
        cot = c_all[:, :, cols].reshape(NZ * tokens, half)
        return lax.dot_general(hid_t, cot, (((0,), (0,)), ((), ())), preferred_element_type=F32)

    grad_send = rdma(grad_out, grad_in, gr_s, gr_r, pair)

    with jax.named_scope("grad1"):
        @pl.when(section == 1)
        def _():
            wait_cot()
            grad_out[...] = grad_half(1 - xl).astype(BF16)
            grad_send.start()
            grad_own[...] = grad_half(xl)

    with jax.named_scope("next%d" % (PARTS - 1)):
        next_stage(PARTS - 1)

    with jax.named_scope("grad0"):
        @pl.when(section == 0)
        def _():
            for m in range(PARTS):
                relay_sum(m)
            pl.semaphore_wait(go, 1)
            spread_cot()
            for m in range(PARTS):
                store_state(m)
            relay_hid(0)
            pass_cot()
            relay_hid(1)
            wait_cot()
            grad_out[...] = grad_half(1 - xl).astype(BF16)
            grad_send.start()
            grad_own[...] = grad_half(xl)

    with jax.named_scope("waitgrad"):
        grad_send.wait_recv()
        grad_done[...] = (grad_own[...] + grad_in[...].astype(F32)).astype(BF16)
        grad_store = pltpu.make_async_copy(grad_done, grad_ref.at[0], gd_s)
        grad_store.start()

    with jax.named_scope("drain"):
        @pl.when(section == 0)
        def _():
            for m in range(PARTS):
                core_send(m).wait_send()

        @pl.when(moves & (section == 0))
        def _():
            for m in range(PARTS):
                tok_send(m).wait_send()

        @pl.when(shares_cot)
        def _():
            cot_send.wait_send()
            for i in range(1, NY + 1):
                cot_spread(i).wait_send()

        @pl.when(beside != z)
        def _():
            for i in range(1, NY):
                cot_pass(i).wait_send()

        @pl.when(moves)
        def _():
            gain_send.wait_send()
            for m in range(PARTS):
                state_send(m).wait_send()

        up_send.wait_send()
        down_send.wait_send()
        grad_send.wait_send()

        @pl.loop(1, NT)
        def _(i):
            for m in range(PARTS):
                spread(m, i).wait_send()
                y_copy(m, block_at(i)).wait_send()

        @pl.loop(1, NZ)
        def _(i):
            for m in range(PARTS):
                sq_copy(m, z_at(i)).wait_send()

        for m in range(PARTS):
            for way in range(2):
                for dist in range(1, 4):
                    k = (z + dist * (1 - 2 * way) + NZ) % NZ
                    for copy in part_copies(m, k, way, dist):
                        copy.wait_send()
                sum_send(m, way).wait_send()
                for copy in relay_sends(m, way):
                    copy.wait_send()
            for copy in part_copies(m, (z + 4) % NZ, 0, 4):
                copy.wait_send()
            for copy in hid_sends(m):
                copy.wait_send()

    with jax.named_scope("waitstate"):
        for m in range(PARTS):
            state_send(m).wait_recv()
        grad_store.wait()


def body(tokens, gain, w_up, w_down, cotangent):
    rows, feats = tokens.shape
    half, hidden = w_up.shape[1:]
    width = cotangent.shape[2]
    dma = pltpu.SemaphoreType.DMA
    vmem = pl.BlockSpec(memory_space=pltpu.VMEM)
    hbm = pl.BlockSpec(memory_space=pl.ANY)

    def run(*refs):
        kernel(width, *refs)

    one = dma(())
    states, grads = pl.pallas_call(
        run,
        out_shape=(
            jax.ShapeDtypeStruct((1, rows, feats), BF16),
            jax.ShapeDtypeStruct((1, hidden, half), BF16),
        ),
        in_specs=[hbm] * 5,
        out_specs=(hbm, hbm),
        scratch_shapes=[
            pltpu.VMEM((NT, rows, feats), BF16),
            pltpu.VMEM((NT, rows, feats), BF16),
            pltpu.VMEM((1, feats), BF16),
            pltpu.VMEM((2 * half, hidden), BF16),
            pltpu.VMEM((2, hidden, half), BF16),
            pltpu.VMEM((NZ, rows, hidden), BF16),
            pltpu.VMEM((rows, hidden), BF16),
            pltpu.VMEM((4, rows, hidden), BF16),
            pltpu.VMEM((PARTS, 2, 3, rows // PARTS, hidden), BF16),
            pltpu.VMEM((PARTS, 2, rows // PARTS, hidden), BF16),
            pltpu.VMEM((PARTS, 2, rows // PARTS, hidden), BF16),
            pltpu.VMEM((PARTS, NZ, 8, rows), F32),
            pltpu.VMEM((PARTS, NZ, 8, rows), F32),
            pltpu.VMEM((rows // PARTS, hidden), F32),
            pltpu.VMEM((NZ, rows, hidden), BF16),
            pltpu.VMEM((NT, rows, feats), BF16),
            pltpu.VMEM((NT, rows, feats), BF16),
            pltpu.VMEM((rows, feats), BF16),
            pltpu.VMEM((hidden, half), F32),
            pltpu.VMEM((hidden, half), BF16),
            pltpu.VMEM((hidden, half), BF16),
            pltpu.VMEM((hidden, half), BF16),
        ]
        + [one] * 14
        + [dma((8,))] * 2
        + [dma((PARTS,))] * 5
        + [dma((8 * PARTS,))] * 6
        + [dma((n * PARTS,)) for n in (8, 4, 6, 2, 4, 8, 2, 6)]
        + [pltpu.SemaphoreType.REGULAR],
        compiler_params=pltpu.CompilerParams(
            collective_id=0, has_side_effects=True, vmem_limit_bytes=60 * 1024 * 1024
        ),
    )(tokens, gain, w_up, w_down, cotangent)
    return states, grads


def solution(mesh):
    torus = Mesh(
        mesh.devices.reshape(mesh.shape["section"], NZ, 2, NY, NX),
        ("section", "z", "xl", "y", "xh"),
    )
    dp, tensor = ("z", "xl"), ("y", "xh")
    in_specs = (
        P(dp, tensor),
        P("section", tensor),
        P("section", dp, tensor),
        P("section", tensor, dp),
        P("section", dp, None),
    )
    out_specs = (P("section", dp, tensor), P("section", tensor, dp))
    return jax.shard_map(body, mesh=torus, in_specs=in_specs, out_specs=out_specs, check_vma=False)
```

```python
import jax
import jax.numpy as jnp
from jax import lax
from jax.experimental import pallas as pl
from jax.experimental.pallas import tpu as pltpu
from jax.sharding import Mesh
from jax.sharding import PartitionSpec as P

EPS = 1e-06
MESH = pl.DeviceIdType.MESH
NZ, NY, NX = 8, 4, 2
NT = NY * NX
F32, BF16 = jnp.float32, jnp.bfloat16

SIZES = (32,)*4
STARTS = tuple(sum(SIZES[:m]) for m in range(len(SIZES)))
PARTS = len(SIZES)


def order_of(section):
    gap = 4 / PARTS
    todo = []
    for m in range(PARTS):
        up0 = 18 + 2.5 * gap * m
        pass0 = 31 + 2.7 * gap * m
        down0 = 38 + 3 * gap * m
        up1 = 50 + 3 * gap * m
        if section == 0:
            todo += [(up0, "up", m), (up0 + 10, "hid", m), (down0, "down", m)]
            todo += [(down0 + 6.1, "next", m), (up1 + 4, "sum", m), (up1 + 11.5, "pass", m)]
        else:
            todo += [(up0 + 4, "sum", m), (pass0, "pass", m), (up1 - 5.9, "take", m)]
            todo += [(up1, "up", m), (up1 + 8.5, "hid", m), (up1 + 15.5, "down", m)]
            todo += [(up1 + 19.5, "next", m)]
    last = 50 + 3 * gap * (PARTS - 1)
    if section == 0:
        todo += [(18.1, "down_copy", 0), (18.2, "cot_spread", 0), (26, "cot_pass", 0)]
        todo += [(last + 1, "state", 0), (53.9, "grad", 0)]
    else:
        todo += [(25, "cot_spread", 0), (30.7, "up_copy", 0), (30.8, "cot_pass", 0)]
        todo += [(last + 0.1, "down_copy", 0), (last + 16, "grad", 0)]
    return [(name, m) for _, name, m in sorted(todo)]


def ring_offset(i):
    return ((i + 1) // 2) * (1 - 2 * ((i + 1) % 2))


def kernel(
    width,
    tok_ref, gain_ref, up_ref, down_ref, cot_ref,
    state_ref, grad_ref,
    x_all, c_all, gain_z, up_pair, down_pair,
    part_out, part_own, part_in, sum_in, sum_out, relay, sq_out, sq_in, hid_all,
    y_out, y_in, x_next, grad_own, grad_out, grad_in, grad_done,
    gain_s, gain_r, cotp_s, cotp_r, up_s, up_r, down_s, down_r, upl, downl,
    gr_s, gr_r, gd_s, cotl, cg_s, cg_r,
    xin_s, xin_r, core_s, out_s, out_r, sqh_s, sqh_r,
    ag_s, ag_r, sq_s, sq_r, rt_s, rt_r,
    rz_s, rz_r, sum_r, sum_s, az_s, az_r, rel_r, rel_s,
    go,
):
    section = lax.axis_index("section")
    z = lax.axis_index("z")
    xl = lax.axis_index("xl")
    y = lax.axis_index("y")
    xh = lax.axis_index("xh")
    t = y * NX + xh
    half = up_ref.shape[1]
    feats = tok_ref.shape[1]
    tokens = tok_ref.shape[0]
    hidden = up_ref.shape[2]
    pair = {"xl": 1 - xl}
    core = {"section": 1 - section}
    own = (t - z + NT) % NT
    ahead_t = (z + t) % NT
    ahead = {"z": t, "y": ahead_t // NX, "xh": ahead_t % NX}
    back = {"z": own, "y": z // NX, "xh": z % NX}
    moves = (z + t) > 0
    shares_cot = own != z

    def to_tensor(k):
        return {"y": k // NX, "xh": k % NX}

    def tensor_at(i):
        k = i % NY
        step = k + (k // 2) * (1 - 2 * (k % 2))
        return ((y + step) % NY) * NX + (xh + i // NY) % NX

    def block_at(i):
        return (tensor_at(i) - z + NT) % NT

    def z_at(i):
        return (z + ring_offset(i) + NZ) % NZ

    def helper(step):
        return {"section": 1 - section, "z": (z + step + NZ) % NZ}

    def part(m):
        return pl.ds(STARTS[m], SIZES[m])

    def span_of(m):
        return slice(STARTS[m], STARTS[m] + SIZES[m])

    def side(m, way):
        piece = SIZES[m] // 2
        return pl.ds(STARTS[m] + way * piece, piece)

    def rdma(src, dst, ssem, rsem, dev):
        return pltpu.make_async_remote_copy(
            src_ref=src, dst_ref=dst, send_sem=ssem, recv_sem=rsem,
            device_id=dev, device_id_type=MESH,
        )

    def arrived(ref, sem):
        rdma(ref, ref, gain_s, sem, core).wait_recv()

    def greet(dev):
        pl.semaphore_signal(barrier, inc=1, device_id=dev, device_id_type=MESH)

    with jax.named_scope("barrier"):
        mine = pl.ds(pl.multiple_of(xl * half, 128), half)
        up_here = pltpu.make_async_copy(up_ref.at[0], up_pair.at[mine], upl)
        down_here = pltpu.make_async_copy(down_ref.at[0], down_pair.at[xl], downl)
        up_here.start()
        down_here.start()
        barrier = pltpu.get_barrier_semaphore()

        @pl.loop(1, NZ)
        def _(i):
            greet({"z": z_at(i)})

        @pl.loop(1, NT)
        def _(i):
            greet(to_tensor(tensor_at(i)))

        greet(pair)
        greet(core)
        for step in (1, -1, 2, -2):
            greet(helper(step))

        @pl.when(moves)
        def _():
            greet(ahead)
            greet(back)
            pl.semaphore_wait(barrier, NZ + NT + 6)

        @pl.when(z + t == 0)
        def _():
            pl.semaphore_wait(barrier, NZ + NT + 4)

    def tok_send(m):
        return rdma(tok_ref.at[part(m)], x_all.at[z, part(m)], xin_s.at[m], xin_r.at[m], ahead)

    def tok_here(m):
        return pltpu.make_async_copy(tok_ref.at[part(m)], x_all.at[own, part(m)], xin_r.at[m])

    gain_send = rdma(gain_ref, gain_z, gain_s, gain_r, ahead)
    gain_here = pltpu.make_async_copy(gain_ref, gain_z, gain_r)

    def cot_cols(k):
        return cot_ref.at[0, :, pl.ds(pl.multiple_of(k * feats, 128), feats)]

    cot_send = rdma(cot_cols(own), c_all.at[z], cotp_s, cotp_r, {"z": own})
    cot_here = pltpu.make_async_copy(cot_cols(z), c_all.at[z], cotl)
    up_send = rdma(up_ref.at[0], up_pair.at[mine], up_s, up_r, pair)
    down_send = rdma(down_ref.at[0], down_pair.at[xl], down_s, down_r, pair)
    grad_send = rdma(grad_out, grad_in, gr_s, gr_r, pair)

    def start_cot():
        @pl.when(shares_cot)
        def _():
            cot_send.start()

    beside = (y * NX + 1 - xh - z + NT) % NT

    def cot_spread(i):
        return rdma(
            c_all.at[own], c_all.at[own], cg_s.at[i - 1], cg_r.at[own], to_tensor(tensor_at(i))
        )

    def cot_pass(i):
        return rdma(
            c_all.at[beside], c_all.at[beside], cg_s.at[i + 3], cg_r.at[beside],
            to_tensor(tensor_at(i)),
        )

    def spread_cot():
        @pl.when(shares_cot)
        def _():
            arrived(c_all.at[own], cotp_r)
            for i in (NY, 1, 2, 3):
                cot_spread(i).start()

    def pass_cot():
        @pl.when(beside != z)
        def _():
            arrived(c_all.at[beside], cg_r.at[beside])
            for i in range(1, NY):
                cot_pass(i).start()

    def wait_cot():
        @pl.loop(1, NT)
        def _(i):
            k = block_at(i)

            @pl.when((k != z) & (i != NY))
            def _():
                arrived(c_all.at[k], cg_r.at[k])

        cot_here.wait()

    def sum_send(m, way):
        return rdma(
            sum_out.at[way, part(m)], part_in.at[2 + way, part(m)],
            sum_s.at[m * 2 + way], rz_r.at[m * 4 + 2 + way], helper(2 - 4 * way),
        )

    def sum_stage(m):
        for way in range(2):
            first = m * 6 + way * 3
            arrived(sum_in.at[way, 0, part(m)], sum_r.at[first])
            arrived(sum_in.at[way, 1, part(m)], sum_r.at[first + 1])
            arrived(sum_in.at[way, 2, side(m, way)], sum_r.at[first + 2])
            for which in range(2):
                piece = SIZES[m] // 2
                rows = slice(STARTS[m] + which * piece, STARTS[m] + (which + 1) * piece)
                total = sum_in[way, 0, rows].astype(F32) + sum_in[way, 1, rows].astype(F32)
                if which == way:
                    total = total + sum_in[way, 2, rows].astype(F32)
                sum_out[way, rows] = total.astype(BF16)
            sum_send(m, way).start()

    def relay_sends(m, way):
        sign = 1 - 2 * way
        block = (z - 2 * sign + NZ) % NZ
        slot = m * 6 + way * 3
        first = m * 8 + way * 4
        full = relay.at[way, part(m)]
        whole = hid_all.at[block, part(m)]
        return (
            rdma(
                relay.at[way, side(m, way)], hid_all.at[block, side(m, way)],
                rel_s.at[slot], az_r.at[first + 3], helper(2 * sign),
            ),
            rdma(full, whole, rel_s.at[slot + 1], az_r.at[first + 2], helper(sign)),
            rdma(full, whole, rel_s.at[slot + 2], az_r.at[first + 1], core),
        )

    def pass_stage(m):
        for way in range(2):
            arrived(relay.at[way, part(m)], rel_r.at[m * 2 + way])
            for copy in relay_sends(m, way):
                copy.start()

    def spread(m, i):
        return rdma(
            x_all.at[own, part(m)], x_all.at[own, part(m)],
            ag_s.at[m * NT + i], ag_r.at[m * NT + own], to_tensor(tensor_at(i)),
        )

    def sq_copy(m):
        return rdma(sq_out.at[m], sq_in.at[m, z], sqh_s.at[m], sqh_r.at[m], {"z": own})

    def sq_spread(m, i):
        return rdma(
            sq_in.at[m, own], sq_in.at[m, own],
            sq_s.at[m * NT + i], sq_r.at[m * NT + own], to_tensor(tensor_at(i)),
        )

    def sq_stage(m):
        @pl.when(shares_cot)
        def _():
            arrived(sq_in.at[m, own], sqh_r.at[m])

        @pl.loop(1, NT)
        def _(i):
            sq_spread(m, i).start()

    def take_stage(m):
        arrived(x_all.at[own, part(m)], xin_r.at[m])

        @pl.loop(1, NT)
        def _(i):
            spread(m, i).start()

        x_f = x_all[own, span_of(m)].astype(F32)
        sq = x_f * x_f
        sq = sum(sq[:, c:c + tokens] for c in range(0, feats, tokens))
        sq = jnp.concatenate([sq] * (tokens // SIZES[m]), axis=0)
        sq_hi = sq.astype(BF16)
        sq_lo = (sq - sq_hi.astype(F32)).astype(BF16)
        ones = jnp.ones((8, tokens), BF16)
        row_dims = (((1,), (1,)), ((), ()))
        sq_row = lax.dot_general(ones, sq_hi, row_dims, preferred_element_type=F32)
        sq_row = sq_row + lax.dot_general(ones, sq_lo, row_dims, preferred_element_type=F32)
        sq_out[m] = sq_row

        @pl.when(own == z)
        def _():
            sq_in[m, z] = sq_row

        @pl.when(shares_cot)
        def _():
            sq_copy(m).start()

    def part_copies(m, k, way, dist):
        sign = 1 - 2 * way
        src = part_out.at[k, part(m)]
        slot = m * 8 + way
        first = m * 6 + way * 3
        if dist == 1:
            dst = part_in.at[way, part(m)]
            return (rdma(src, dst, rz_s.at[slot], rz_r.at[m * 4 + way], {"z": k}),)
        if dist == 2:
            return (rdma(src, sum_in.at[way, 0, part(m)], rz_s.at[slot + 2], sum_r.at[first], core),)
        if dist == 3:
            dst = sum_in.at[way, 1, part(m)]
            return (rdma(src, dst, rz_s.at[slot + 4], sum_r.at[first + 1], helper(sign)),)
        return tuple(
            rdma(
                part_out.at[k, side(m, w)], sum_in.at[w, 2, side(m, w)],
                rz_s.at[m * 8 + 6 + w], sum_r.at[m * 6 + w * 3 + 2], helper(2 - 4 * w),
            )
            for w in range(2)
        )

    def up_stage(m):
        sq_stage(m)
        gain_f = gain_z[...].astype(F32)
        rows = SIZES[m]

        @pl.loop(0, NT // 2)
        def _(j):
            scaled = []
            for i in (2 * j, 2 * j + 1):
                k = block_at(i)

                @pl.when(i > 0)
                def _():
                    arrived(x_all.at[k, part(m)], ag_r.at[m * NT + k])

                scaled.append((x_all[k, span_of(m)].astype(F32) * gain_f).astype(BF16))
            both = jnp.dot(
                jnp.concatenate(scaled, axis=0), up_pair[...], preferred_element_type=F32
            ).astype(BF16)
            for n in range(2):
                k = block_at(2 * j + n)
                value = both[n * rows:(n + 1) * rows]
                delta = (k - z + NZ) % NZ
                way = delta // 5
                dist = delta + way * (NZ - 2 * delta)

                @pl.when(k == z)
                def _():
                    part_own[span_of(m)] = value

                @pl.when(k != z)
                def _():
                    part_out[k, span_of(m)] = value

                for far in range(1, 5):
                    @pl.when(dist == far)
                    def _():
                        for copy in part_copies(m, k, way, far):
                            copy.start()

    def hid_sends(m):
        block = hid_all.at[z, part(m)]
        out = []
        for way in range(2):
            sign = 1 - 2 * way
            out.append(
                rdma(
                    block, relay.at[way, part(m)], az_s.at[m * 4 + 2 + way],
                    rel_r.at[m * 2 + way], helper(2 * sign),
                )
            )
            out.append(
                rdma(
                    block, block, az_s.at[m * 4 + way], az_r.at[m * 8 + way * 4],
                    {"z": (z + sign + NZ) % NZ},
                )
            )
        return out

    def hid_stage(m):
        rows = SIZES[m]

        @pl.loop(1, NT)
        def _(i):
            k = block_at(i)
            arrived(sq_in.at[m, k], sq_r.at[m * NT + k])

        for slot in range(4):
            arrived(part_in.at[slot, part(m)], rz_r.at[m * 4 + slot])
        total = part_own[span_of(m)].astype(F32)
        for slot in range(4):
            total = total + part_in[slot, span_of(m)].astype(F32)
        sq_sum = sum(sq_in[m, k] for k in range(NZ))
        square = jnp.transpose(jnp.broadcast_to(sq_sum[0:1, :], (tokens, tokens)))
        mean_col = square[0:rows, 0:1] / width
        pre_act = total * lax.rsqrt(mean_col + EPS)
        hid_all[z, span_of(m)] = jax.nn.gelu(pre_act, approximate=True).astype(BF16)
        for copy in hid_sends(m):
            copy.start()

    def y_copy(m, k):
        return rdma(
            y_out.at[k, part(m)], y_in.at[t, part(m)],
            rt_s.at[m * NT + k], rt_r.at[m * NT + t], to_tensor((k + z) % NT),
        )

    def down_stage(m):
        rows = SIZES[m]

        @pl.loop(0, NZ // 2)
        def _(j):
            hid = []
            for i in (2 * j, 2 * j + 1):
                k = z_at(i)

                @pl.when((i > 0) & (i < NZ - 1))
                def _():
                    slot = m * 8 + (i % 2) * 4 + (i + 1) // 2 - 1
                    arrived(hid_all.at[k, part(m)], az_r.at[slot])

                @pl.when(i == NZ - 1)
                def _():
                    for way in range(2):
                        arrived(hid_all.at[k, side(m, way)], az_r.at[m * 8 + way * 4 + 3])

                hid.append(hid_all[k, span_of(m)])
            hid = jnp.concatenate(hid, axis=0)
            y_lo = jnp.dot(hid, down_pair[0], preferred_element_type=F32).astype(BF16)
            y_hi = jnp.dot(hid, down_pair[1], preferred_element_type=F32).astype(BF16)
            for n in range(2):
                k = z_at(2 * j + n)
                rng = slice(n * rows, (n + 1) * rows)

                @pl.when(k == own)
                def _():
                    y_in[t, span_of(m), 0:half] = y_lo[rng]
                    y_in[t, span_of(m), half:] = y_hi[rng]

                @pl.when(k != own)
                def _():
                    y_out[k, span_of(m), 0:half] = y_lo[rng]
                    y_out[k, span_of(m), half:] = y_hi[rng]
                    y_copy(m, k).start()

    def core_send(m):
        return rdma(x_next.at[part(m)], x_all.at[own, part(m)], core_s.at[m], xin_r.at[m], core)

    def state_send(m):
        return rdma(x_next.at[part(m)], state_ref.at[0, part(m)], out_s.at[m], out_r.at[m], back)

    def state_here(m):
        return pltpu.make_async_copy(x_next.at[part(m)], state_ref.at[0, part(m)], out_r.at[m])

    def store_state(m):
        @pl.when(moves)
        def _():
            state_send(m).start()

        @pl.when(z + t == 0)
        def _():
            state_here(m).start()

    def next_stage(m, first_section):
        @pl.loop(1, NT)
        def _(i):
            k = tensor_at(i)
            arrived(y_in.at[k, part(m)], rt_r.at[m * NT + k])

        total = x_all[own, span_of(m)].astype(F32)
        for k in range(NT):
            total = total + y_in[k, span_of(m)].astype(F32)
        x_next[span_of(m)] = total.astype(BF16)
        if first_section:
            core_send(m).start()
        else:
            store_state(m)

    def grad_half(which):
        hid_t = hid_all[...].reshape(NZ * tokens, hidden)
        cols = pl.ds(pl.multiple_of(which * half, 128), half)
        cot = c_all[:, :, cols].reshape(NZ * tokens, half)
        return lax.dot_general(hid_t, cot, (((0,), (0,)), ((), ())), preferred_element_type=F32)

    def grad_stage():
        wait_cot()
        grad_out[...] = grad_half(1 - xl).astype(BF16)
        grad_send.start()
        grad_own[...] = grad_half(xl)

    def wait_up():
        arrived(gain_z, gain_r)
        up_here.wait()
        up_send.wait_recv()

    def wait_down():
        down_here.wait()
        down_send.wait_recv()

    def run(which):
        met = set()
        for name, m in order_of(which):
            with jax.named_scope("%s%d" % (name, m)):
                if name == "up" and name not in met:
                    wait_up()
                if name == "down" and name not in met:
                    wait_down()
                met.add(name)
                if name == "take":
                    take_stage(m)
                elif name == "up":
                    up_stage(m)
                elif name == "sum":
                    sum_stage(m)
                elif name == "hid":
                    hid_stage(m)
                elif name == "pass":
                    pass_stage(m)
                elif name == "down":
                    down_stage(m)
                elif name == "next":
                    next_stage(m, which == 0)
                elif name == "up_copy":
                    up_send.start()
                elif name == "down_copy":
                    down_send.start()
                elif name == "cot_spread":
                    spread_cot()
                elif name == "cot_pass":
                    pass_cot()
                elif name == "state":
                    for n in range(PARTS):
                        store_state(n)
                elif name == "grad":
                    grad_stage()

    cot_here.start()

    @pl.when(moves)
    def _():
        gain_send.start()

    @pl.when(z + t == 0)
    def _():
        gain_here.start()

    @pl.when(section == 0)
    def _():
        with jax.named_scope("send0"):
            @pl.when(moves)
            def _():
                for m in range(PARTS):
                    tok_send(m).start()

            @pl.when(z + t == 0)
            def _():
                for m in range(PARTS):
                    tok_here(m).start()

            up_send.start()

        with jax.named_scope("waitx"):
            for m in range(PARTS):
                take_stage(m)
            start_cot()
            pl.semaphore_signal(go, inc=1, device_id=core, device_id_type=MESH)
        run(0)

    @pl.when(section == 1)
    def _():
        with jax.named_scope("waitgo"):
            pl.semaphore_wait(go, 1)
            start_cot()
        run(1)

    with jax.named_scope("waitgrad"):
        grad_send.wait_recv()
        grad_done[...] = (grad_own[...] + grad_in[...].astype(F32)).astype(BF16)
        grad_store = pltpu.make_async_copy(grad_done, grad_ref.at[0], gd_s)
        grad_store.start()

    with jax.named_scope("drain"):
        @pl.when(section == 0)
        def _():
            for m in range(PARTS):
                core_send(m).wait_send()

        @pl.when(moves & (section == 0))
        def _():
            for m in range(PARTS):
                tok_send(m).wait_send()

        @pl.when(shares_cot)
        def _():
            cot_send.wait_send()
            for i in range(1, NY + 1):
                cot_spread(i).wait_send()

        @pl.when(beside != z)
        def _():
            for i in range(1, NY):
                cot_pass(i).wait_send()

        @pl.when(moves)
        def _():
            gain_send.wait_send()
            for m in range(PARTS):
                state_send(m).wait_send()

        up_send.wait_send()
        down_send.wait_send()
        grad_send.wait_send()

        @pl.loop(1, NT)
        def _(i):
            for m in range(PARTS):
                spread(m, i).wait_send()
                sq_spread(m, i).wait_send()
                y_copy(m, block_at(i)).wait_send()

        @pl.when(shares_cot)
        def _():
            for m in range(PARTS):
                sq_copy(m).wait_send()

        for m in range(PARTS):
            for way in range(2):
                for dist in range(1, 4):
                    k = (z + dist * (1 - 2 * way) + NZ) % NZ
                    for copy in part_copies(m, k, way, dist):
                        copy.wait_send()
                sum_send(m, way).wait_send()
                for copy in relay_sends(m, way):
                    copy.wait_send()
            for copy in part_copies(m, (z + 4) % NZ, 0, 4):
                copy.wait_send()
            for copy in hid_sends(m):
                copy.wait_send()

    with jax.named_scope("waitstate"):
        for m in range(PARTS):
            arrived(state_ref.at[0, part(m)], out_r.at[m])
        grad_store.wait()


def body(tokens, gain, w_up, w_down, cotangent):
    rows, feats = tokens.shape
    half, hidden = w_up.shape[1:]
    width = cotangent.shape[2]
    dma = pltpu.SemaphoreType.DMA
    hbm = pl.BlockSpec(memory_space=pl.ANY)

    def run(*refs):
        kernel(width, *refs)

    one = dma(())
    states, grads = pl.pallas_call(
        run,
        out_shape=(
            jax.ShapeDtypeStruct((1, rows, feats), BF16),
            jax.ShapeDtypeStruct((1, hidden, half), BF16),
        ),
        in_specs=[hbm] * 5,
        out_specs=(hbm, hbm),
        scratch_shapes=[
            pltpu.VMEM((NT, rows, feats), BF16),
            pltpu.VMEM((NT, rows, feats), BF16),
            pltpu.VMEM((1, feats), BF16),
            pltpu.VMEM((2 * half, hidden), BF16),
            pltpu.VMEM((2, hidden, half), BF16),
            pltpu.VMEM((NZ, rows, hidden), BF16),
            pltpu.VMEM((rows, hidden), BF16),
            pltpu.VMEM((4, rows, hidden), BF16),
            pltpu.VMEM((2, 3, rows, hidden), BF16),
            pltpu.VMEM((2, rows, hidden), BF16),
            pltpu.VMEM((2, rows, hidden), BF16),
            pltpu.VMEM((PARTS, 8, rows), F32),
            pltpu.VMEM((PARTS, NZ, 8, rows), F32),
            pltpu.VMEM((NZ, rows, hidden), BF16),
            pltpu.VMEM((NT, rows, feats), BF16),
            pltpu.VMEM((NT, rows, feats), BF16),
            pltpu.VMEM((rows, feats), BF16),
            pltpu.VMEM((hidden, half), F32),
            pltpu.VMEM((hidden, half), BF16),
            pltpu.VMEM((hidden, half), BF16),
            pltpu.VMEM((hidden, half), BF16),
        ]
        + [one] * 14
        + [dma((8,))] * 2
        + [dma((PARTS,))] * 7
        + [dma((8 * PARTS,))] * 6
        + [dma((n * PARTS,)) for n in (8, 4, 6, 2, 4, 8, 2, 6)]
        + [pltpu.SemaphoreType.REGULAR],
        compiler_params=pltpu.CompilerParams(
            collective_id=0, has_side_effects=True, vmem_limit_bytes=60 * 1024 * 1024
        ),
    )(tokens, gain, w_up, w_down, cotangent)
    return states, grads


def solution(mesh):
    torus = Mesh(
        mesh.devices.reshape(mesh.shape["section"], NZ, 2, NY, NX),
        ("section", "z", "xl", "y", "xh"),
    )
    dp, tensor = ("z", "xl"), ("y", "xh")
    in_specs = (
        P(dp, tensor),
        P("section", tensor),
        P("section", dp, tensor),
        P("section", tensor, dp),
        P("section", dp, None),
    )
    out_specs = (P("section", dp, tensor), P("section", tensor, dp))
    return jax.shard_map(body, mesh=torus, in_specs=in_specs, out_specs=out_specs, check_vma=False)
```

```python
import jax
import jax.numpy as jnp
from jax import lax
from jax.experimental import pallas as pl
from jax.experimental.pallas import tpu as pltpu
from jax.sharding import Mesh
from jax.sharding import PartitionSpec as P

EPS = 1e-06
MESH = pl.DeviceIdType.MESH
NZ, NY, NX = 8, 4, 2
NT = NY * NX
F32, BF16 = jnp.float32, jnp.bfloat16

SIZES = (32,)*4
STARTS = tuple(sum(SIZES[:m]) for m in range(len(SIZES)))
PARTS = len(SIZES)


def order_of(section):
    gap = 4 / PARTS
    todo = []
    for m in range(PARTS):
        up0 = 18 + 2.5 * gap * m
        pass0 = 31 + 2.7 * gap * m
        down0 = 38 + 3 * gap * m
        up1 = 50 + 3 * gap * m
        if section == 0:
            todo += [(up0, "up", m), (up0 + 10, "hid", m), (down0, "down", m)]
            todo += [(down0 + 6.1, "next", m), (up1 + 4, "sum", m), (up1 + 11.5, "pass", m)]
        else:
            todo += [(up0 + 4, "sum", m), (pass0, "pass", m), (up1 - 6.1, "take", m)]
            todo += [(up1, "up", m), (up1 + 8.5, "hid", m), (up1 + 15.5, "down", m)]
            todo += [(up1 + 19.5, "next", m)]
    last = 50 + 3 * gap * (PARTS - 1)
    if section == 0:
        todo += [(18.1, "down_copy", 0), (18.2, "cot_spread", 0), (31, "cot_pass", 0)]
        todo += [(last + 1, "state", 0), (53.9, "grad", 0)]
    else:
        todo += [(25, "cot_spread", 0), (30.7, "up_copy", 0), (30.8, "cot_pass", 0)]
        todo += [(last + 0.1, "down_copy", 0), (last + 16, "grad", 0)]
    return [(name, m) for _, name, m in sorted(todo)]


def ring_offset(i):
    return ((i + 1) // 2) * (1 - 2 * ((i + 1) % 2))


def kernel(
    width,
    tok_ref, gain_ref, up_ref, down_ref, cot_ref,
    state_ref, grad_ref,
    x_all, c_all, gain_z, up_pair, down_pair,
    part_out, part_own, part_in, sum_in, sum_out, relay, sq_out, sq_in, hid_all,
    y_out, y_in, x_next, grad_own, grad_out, grad_in, grad_done,
    gain_s, gain_r, cotp_s, cotp_r, up_s, up_r, down_s, down_r, upl, downl,
    gr_s, gr_r, gd_s, cotl, cg_s, cp_s, cg_r,
    xin_s, core_s, out_s, out_r, sqh_s, ag_s, sq_s, rt_s, rz_s, sum_s, az_s, rel_s,
    xin_r, sqh_r, ag_r, sq_r, rt_r, rz_r, sum_r, az_r, rel_r,
    go,
):
    section = lax.axis_index("section")
    z = lax.axis_index("z")
    xl = lax.axis_index("xl")
    y = lax.axis_index("y")
    xh = lax.axis_index("xh")
    t = y * NX + xh
    half = up_ref.shape[1]
    feats = tok_ref.shape[1]
    tokens = tok_ref.shape[0]
    hidden = up_ref.shape[2]
    pair = {"xl": 1 - xl}
    core = {"section": 1 - section}
    own = (t - z + NT) % NT
    ahead_t = (z + t) % NT
    ahead = {"z": t, "y": ahead_t // NX, "xh": ahead_t % NX}
    back = {"z": own, "y": z // NX, "xh": z % NX}
    moves = (z + t) > 0
    shares_cot = own != z

    def to_tensor(k):
        return {"y": k // NX, "xh": k % NX}

    def tensor_at(i):
        k = i % NY
        step = k + (k // 2) * (1 - 2 * (k % 2))
        return ((y + step) % NY) * NX + (xh + i // NY) % NX

    def block_at(i):
        return (tensor_at(i) - z + NT) % NT

    def z_at(i):
        return (z + ring_offset(i) + NZ) % NZ

    def helper(step):
        return {"section": 1 - section, "z": (z + step + NZ) % NZ}

    def part(m):
        return pl.ds(STARTS[m], SIZES[m])

    def span_of(m):
        return slice(STARTS[m], STARTS[m] + SIZES[m])

    def side(m, way):
        piece = SIZES[m] // 2
        return pl.ds(STARTS[m] + way * piece, piece)

    def rdma(src, dst, ssem, rsem, dev):
        return pltpu.make_async_remote_copy(
            src_ref=src, dst_ref=dst, send_sem=ssem, recv_sem=rsem,
            device_id=dev, device_id_type=MESH,
        )

    def arrived(ref, sem):
        rdma(ref, ref, gain_s, sem, core).wait_recv()

    def greet(dev):
        pl.semaphore_signal(barrier, inc=1, device_id=dev, device_id_type=MESH)

    with jax.named_scope("barrier"):
        mine = pl.ds(pl.multiple_of(xl * half, 128), half)
        up_here = pltpu.make_async_copy(up_ref.at[0], up_pair.at[mine], upl)
        down_here = pltpu.make_async_copy(down_ref.at[0], down_pair.at[xl], downl)
        up_here.start()
        down_here.start()
        barrier = pltpu.get_barrier_semaphore()

        @pl.loop(1, NZ)
        def _(i):
            greet({"z": z_at(i)})

        @pl.loop(1, NT)
        def _(i):
            greet(to_tensor(tensor_at(i)))

        greet(pair)
        greet(core)
        for step in (1, -1, 2, -2):
            greet(helper(step))

        @pl.when(moves)
        def _():
            greet(ahead)
            greet(back)
            pl.semaphore_wait(barrier, NZ + NT + 6)

        @pl.when(z + t == 0)
        def _():
            pl.semaphore_wait(barrier, NZ + NT + 4)

    def tok_send(m):
        return rdma(tok_ref.at[part(m)], x_all.at[z, part(m)], xin_s, xin_r.at[m], ahead)

    def tok_here(m):
        return pltpu.make_async_copy(tok_ref.at[part(m)], x_all.at[own, part(m)], xin_r.at[m])

    gain_send = rdma(gain_ref, gain_z, gain_s, gain_r, ahead)
    gain_here = pltpu.make_async_copy(gain_ref, gain_z, gain_r)

    def cot_cols(k):
        return cot_ref.at[0, :, pl.ds(pl.multiple_of(k * feats, 128), feats)]

    cot_send = rdma(cot_cols(own), c_all.at[z], cotp_s, cotp_r, {"z": own})
    cot_here = pltpu.make_async_copy(cot_cols(z), c_all.at[z], cotl)
    up_send = rdma(up_ref.at[0], up_pair.at[mine], up_s, up_r, pair)
    down_send = rdma(down_ref.at[0], down_pair.at[xl], down_s, down_r, pair)
    grad_send = rdma(grad_out, grad_in, gr_s, gr_r, pair)

    def start_cot():
        @pl.when(shares_cot)
        def _():
            cot_send.start()

    beside = (y * NX + 1 - xh - z + NT) % NT

    def cot_spread(i):
        return rdma(
            c_all.at[own], c_all.at[own], cg_s, cg_r.at[own], to_tensor(tensor_at(i))
        )

    def cot_pass(i):
        return rdma(
            c_all.at[beside], c_all.at[beside], cp_s, cg_r.at[beside],
            to_tensor(tensor_at(i)),
        )

    def spread_cot():
        @pl.when(shares_cot)
        def _():
            arrived(c_all.at[own], cotp_r)
            for i in (NY, 1, 2, 3):
                cot_spread(i).start()

    def pass_cot():
        @pl.when(beside != z)
        def _():
            arrived(c_all.at[beside], cg_r.at[beside])
            for i in range(1, NY):
                cot_pass(i).start()

    def wait_cot():
        @pl.loop(1, NT)
        def _(i):
            k = block_at(i)

            @pl.when((k != z) & (i != NY))
            def _():
                arrived(c_all.at[k], cg_r.at[k])

        cot_here.wait()

    def sum_send(m, way):
        return rdma(
            sum_out.at[way, part(m)], part_in.at[2 + way, part(m)],
            sum_s, rz_r.at[m], helper(2 - 4 * way),
        )

    def sum_stage(m):
        for way in range(2):
            arrived(part_out.at[0, pl.ds(0, SIZES[m] * 5 // 2)], sum_r.at[m * 2 + way])
            for which in range(2):
                piece = SIZES[m] // 2
                rows = slice(STARTS[m] + which * piece, STARTS[m] + (which + 1) * piece)
                total = sum_in[way, 0, rows].astype(F32) + sum_in[way, 1, rows].astype(F32)
                if which == way:
                    total = total + sum_in[way, 2, rows].astype(F32)
                sum_out[way, rows] = total.astype(BF16)
            sum_send(m, way).start()

    def relay_sends(m, way):
        sign = 1 - 2 * way
        block = (z - 2 * sign + NZ) % NZ
        first = m * 8 + way * 4
        full = relay.at[way, part(m)]
        whole = hid_all.at[block, part(m)]
        return (
            rdma(
                relay.at[way, side(m, way)], hid_all.at[block, side(m, way)],
                rel_s, az_r.at[first + 3], helper(2 * sign),
            ),
            rdma(full, whole, rel_s, az_r.at[first + 2], helper(sign)),
            rdma(full, whole, rel_s, az_r.at[first + 1], core),
        )

    def pass_stage(m):
        for way in range(2):
            arrived(relay.at[way, part(m)], rel_r.at[m * 2 + way])
            for copy in relay_sends(m, way):
                copy.start()

    def spread(m, i):
        return rdma(
            x_all.at[own, part(m)], x_all.at[own, part(m)],
            ag_s, ag_r.at[m * NT + own], to_tensor(tensor_at(i)),
        )

    def sq_copy(m):
        return rdma(sq_out.at[m], sq_in.at[m, z], sqh_s, sqh_r.at[m], {"z": own})

    def sq_spread(m, i):
        return rdma(
            sq_in.at[m, own], sq_in.at[m, own],
            sq_s, sq_r.at[m], to_tensor(tensor_at(i)),
        )

    def sq_stage(m):
        @pl.when(shares_cot)
        def _():
            arrived(sq_in.at[m, own], sqh_r.at[m])

        @pl.loop(1, NT)
        def _(i):
            sq_spread(m, i).start()

    def take_stage(m):
        arrived(x_all.at[own, part(m)], xin_r.at[m])

        @pl.loop(1, NT)
        def _(i):
            spread(m, i).start()

        x_f = x_all[own, span_of(m)].astype(F32)
        sq = x_f * x_f
        sq = sum(sq[:, c:c + tokens] for c in range(0, feats, tokens))
        sq = jnp.concatenate([sq] * (tokens // SIZES[m]), axis=0)
        sq_hi = sq.astype(BF16)
        sq_lo = (sq - sq_hi.astype(F32)).astype(BF16)
        ones = jnp.ones((8, tokens), BF16)
        row_dims = (((1,), (1,)), ((), ()))
        sq_row = lax.dot_general(ones, sq_hi, row_dims, preferred_element_type=F32)
        sq_row = sq_row + lax.dot_general(ones, sq_lo, row_dims, preferred_element_type=F32)
        sq_out[m] = sq_row

        @pl.when(own == z)
        def _():
            sq_in[m, z] = sq_row

        @pl.when(shares_cot)
        def _():
            sq_copy(m).start()

    def part_copies(m, k, way, dist):
        sign = 1 - 2 * way
        src = part_out.at[k, part(m)]
        summed = sum_r.at[m * 2 + way]
        if dist == 1:
            dst = part_in.at[way, part(m)]
            return (rdma(src, dst, rz_s, rz_r.at[m], {"z": k}),)
        if dist == 2:
            return (rdma(src, sum_in.at[way, 0, part(m)], rz_s, summed, core),)
        if dist == 3:
            dst = sum_in.at[way, 1, part(m)]
            return (rdma(src, dst, rz_s, summed, helper(sign)),)
        return tuple(
            rdma(
                part_out.at[k, side(m, w)], sum_in.at[w, 2, side(m, w)],
                rz_s, sum_r.at[m * 2 + w], helper(2 - 4 * w),
            )
            for w in range(2)
        )

    def up_stage(m):
        gain_f = gain_z[...].astype(F32)
        rows = SIZES[m]
        group = 4 if m else 2

        @pl.loop(0, NT // group)
        def _(j):
            scaled = []
            for n in range(group):
                i = group * j + n
                k = block_at(i)

                @pl.when(i > 0)
                def _():
                    arrived(x_all.at[k, part(m)], ag_r.at[m * NT + k])

                scaled.append((x_all[k, span_of(m)].astype(F32) * gain_f).astype(BF16))
            both = jnp.dot(
                jnp.concatenate(scaled, axis=0), up_pair[...], preferred_element_type=F32
            ).astype(BF16)
            for n in range(group):
                k = block_at(group * j + n)
                value = both[n * rows:(n + 1) * rows]
                delta = (k - z + NZ) % NZ
                way = delta // 5
                dist = delta + way * (NZ - 2 * delta)

                @pl.when(k == z)
                def _():
                    part_own[span_of(m)] = value

                @pl.when(k != z)
                def _():
                    part_out[k, span_of(m)] = value

                for far in range(1, 5):
                    @pl.when(dist == far)
                    def _():
                        for copy in part_copies(m, k, way, far):
                            copy.start()

        sq_stage(m)

    def hid_sends(m):
        block = hid_all.at[z, part(m)]
        out = []
        for way in range(2):
            sign = 1 - 2 * way
            out.append(
                rdma(
                    block, relay.at[way, part(m)], az_s,
                    rel_r.at[m * 2 + way], helper(2 * sign),
                )
            )
            out.append(
                rdma(
                    block, block, az_s, az_r.at[m * 8 + way * 4],
                    {"z": (z + sign + NZ) % NZ},
                )
            )
        return out

    def hid_stage(m):
        rows = SIZES[m]

        arrived(sq_in.at[m, pl.ds(0, NZ - 1)], sq_r.at[m])
        arrived(part_in.at[:, part(m)], rz_r.at[m])
        total = part_own[span_of(m)].astype(F32)
        for slot in range(4):
            total = total + part_in[slot, span_of(m)].astype(F32)
        sq_sum = sum(sq_in[m, k] for k in range(NZ))
        square = jnp.transpose(jnp.broadcast_to(sq_sum[0:1, :], (tokens, tokens)))
        mean_col = square[0:rows, 0:1] / width
        pre_act = total * lax.rsqrt(mean_col + EPS)
        hid_all[z, span_of(m)] = jax.nn.gelu(pre_act, approximate=True).astype(BF16)
        for copy in hid_sends(m):
            copy.start()

    def y_copy(m, k):
        return rdma(
            y_out.at[k, part(m)], y_in.at[t, part(m)],
            rt_s, rt_r.at[m], to_tensor((k + z) % NT),
        )

    def down_stage(m):
        rows = SIZES[m]

        @pl.loop(0, NZ // 2)
        def _(j):
            hid = []
            for i in (2 * j, 2 * j + 1):
                k = z_at(i)

                @pl.when((i > 0) & (i < NZ - 1))
                def _():
                    slot = m * 8 + (i % 2) * 4 + (i + 1) // 2 - 1
                    arrived(hid_all.at[k, part(m)], az_r.at[slot])

                @pl.when(i == NZ - 1)
                def _():
                    for way in range(2):
                        arrived(hid_all.at[k, side(m, way)], az_r.at[m * 8 + way * 4 + 3])

                hid.append(hid_all[k, span_of(m)])
            hid = jnp.concatenate(hid, axis=0)
            y_lo = jnp.dot(hid, down_pair[0], preferred_element_type=F32).astype(BF16)
            y_hi = jnp.dot(hid, down_pair[1], preferred_element_type=F32).astype(BF16)
            for n in range(2):
                k = z_at(2 * j + n)
                rng = slice(n * rows, (n + 1) * rows)

                @pl.when(k == own)
                def _():
                    y_in[t, span_of(m), 0:half] = y_lo[rng]
                    y_in[t, span_of(m), half:] = y_hi[rng]

                @pl.when(k != own)
                def _():
                    y_out[k, span_of(m), 0:half] = y_lo[rng]
                    y_out[k, span_of(m), half:] = y_hi[rng]
                    y_copy(m, k).start()

    def core_send(m):
        return rdma(x_next.at[part(m)], x_all.at[own, part(m)], core_s, xin_r.at[m], core)

    def state_send(m):
        return rdma(x_next.at[part(m)], state_ref.at[0, part(m)], out_s, out_r, back)

    def state_here(m):
        return pltpu.make_async_copy(x_next.at[part(m)], state_ref.at[0, part(m)], out_r)

    def store_state(m):
        @pl.when(moves)
        def _():
            state_send(m).start()

        @pl.when(z + t == 0)
        def _():
            state_here(m).start()

    def next_stage(m, first_section):
        arrived(y_in.at[pl.ds(0, NT - 1), part(m)], rt_r.at[m])

        total = x_all[own, span_of(m)].astype(F32)
        for k in range(NT):
            total = total + y_in[k, span_of(m)].astype(F32)
        x_next[span_of(m)] = total.astype(BF16)
        if first_section:
            core_send(m).start()
        else:
            store_state(m)

    def grad_half(which):
        hid_t = hid_all[...].reshape(NZ * tokens, hidden)
        cols = pl.ds(pl.multiple_of(which * half, 128), half)
        cot = c_all[:, :, cols].reshape(NZ * tokens, half)
        return lax.dot_general(hid_t, cot, (((0,), (0,)), ((), ())), preferred_element_type=F32)

    def grad_stage():
        wait_cot()
        grad_out[...] = grad_half(1 - xl).astype(BF16)
        grad_send.start()
        grad_own[...] = grad_half(xl)

    def wait_up():
        arrived(gain_z, gain_r)
        up_here.wait()
        up_send.wait_recv()

    def wait_down():
        down_here.wait()
        down_send.wait_recv()

    def run(which):
        met = set()
        for name, m in order_of(which):
            with jax.named_scope("%s%d" % (name, m)):
                if name == "up" and name not in met:
                    wait_up()
                if name == "down" and name not in met:
                    wait_down()
                met.add(name)
                if name == "take":
                    take_stage(m)
                elif name == "up":
                    up_stage(m)
                elif name == "sum":
                    sum_stage(m)
                elif name == "hid":
                    hid_stage(m)
                elif name == "pass":
                    pass_stage(m)
                elif name == "down":
                    down_stage(m)
                elif name == "next":
                    next_stage(m, which == 0)
                elif name == "up_copy":
                    up_send.start()
                elif name == "down_copy":
                    down_send.start()
                elif name == "cot_spread":
                    spread_cot()
                elif name == "cot_pass":
                    pass_cot()
                elif name == "state":
                    for n in range(PARTS):
                        store_state(n)
                elif name == "grad":
                    grad_stage()

    cot_here.start()

    @pl.when(moves)
    def _():
        gain_send.start()

    @pl.when(z + t == 0)
    def _():
        gain_here.start()

    @pl.when(section == 0)
    def _():
        with jax.named_scope("send0"):
            @pl.when(moves)
            def _():
                for m in range(PARTS):
                    tok_send(m).start()

            @pl.when(z + t == 0)
            def _():
                for m in range(PARTS):
                    tok_here(m).start()

            up_send.start()

        with jax.named_scope("waitx"):
            for m in range(PARTS):
                take_stage(m)
            start_cot()
            pl.semaphore_signal(go, inc=1, device_id=core, device_id_type=MESH)
        run(0)

    @pl.when(section == 1)
    def _():
        with jax.named_scope("waitgo"):
            pl.semaphore_wait(go, 1)
            start_cot()
        run(1)

    with jax.named_scope("waitgrad"):
        grad_send.wait_recv()
        grad_done[...] = (grad_own[...] + grad_in[...].astype(F32)).astype(BF16)
        grad_store = pltpu.make_async_copy(grad_done, grad_ref.at[0], gd_s)
        grad_store.start()

    with jax.named_scope("drain"):
        def left(ref, sem):
            rdma(ref, ref, sem, gain_r, core).wait_send()

        @pl.when(section == 0)
        def _():
            left(x_next, core_s)

        @pl.when(moves & (section == 0))
        def _():
            left(x_next, xin_s)

        @pl.when(shares_cot)
        def _():
            cot_send.wait_send()
            left(c_all.at[pl.ds(0, NY)], cg_s)
            left(sq_out, sqh_s)

        @pl.when(beside != z)
        def _():
            left(c_all.at[pl.ds(0, NY - 1)], cp_s)

        @pl.when(moves)
        def _():
            gain_send.wait_send()
            left(x_next, out_s)

        up_send.wait_send()
        down_send.wait_send()
        grad_send.wait_send()
        left(x_all.at[pl.ds(0, NT - 1)], ag_s)
        left(sq_in.at[:, pl.ds(0, NT - 1)], sq_s)
        left(y_out.at[pl.ds(0, NT - 1)], rt_s)
        left(part_out.at[pl.ds(0, NZ - 1)], rz_s)
        left(sum_out, sum_s)
        left(hid_all.at[pl.ds(0, 4)], az_s)
        left(hid_all.at[pl.ds(0, 5)], rel_s)

    with jax.named_scope("waitstate"):
        arrived(state_ref.at[0], out_r)
        grad_store.wait()


def body(tokens, gain, w_up, w_down, cotangent):
    rows, feats = tokens.shape
    half, hidden = w_up.shape[1:]
    width = cotangent.shape[2]
    dma = pltpu.SemaphoreType.DMA
    hbm = pl.BlockSpec(memory_space=pl.ANY)

    def run(*refs):
        kernel(width, *refs)

    one = dma(())
    states, grads = pl.pallas_call(
        run,
        out_shape=(
            jax.ShapeDtypeStruct((1, rows, feats), BF16),
            jax.ShapeDtypeStruct((1, hidden, half), BF16),
        ),
        in_specs=[hbm] * 5,
        out_specs=(hbm, hbm),
        scratch_shapes=[
            pltpu.VMEM((NT, rows, feats), BF16),
            pltpu.VMEM((NT, rows, feats), BF16),
            pltpu.VMEM((1, feats), BF16),
            pltpu.VMEM((2 * half, hidden), BF16),
            pltpu.VMEM((2, hidden, half), BF16),
            pltpu.VMEM((NZ, rows, hidden), BF16),
            pltpu.VMEM((rows, hidden), BF16),
            pltpu.VMEM((4, rows, hidden), BF16),
            pltpu.VMEM((2, 3, rows, hidden), BF16),
            pltpu.VMEM((2, rows, hidden), BF16),
            pltpu.VMEM((2, rows, hidden), BF16),
            pltpu.VMEM((PARTS, 8, rows), F32),
            pltpu.VMEM((PARTS, NZ, 8, rows), F32),
            pltpu.VMEM((NZ, rows, hidden), BF16),
            pltpu.VMEM((NT, rows, feats), BF16),
            pltpu.VMEM((NT, rows, feats), BF16),
            pltpu.VMEM((rows, feats), BF16),
            pltpu.VMEM((hidden, half), F32),
            pltpu.VMEM((hidden, half), BF16),
            pltpu.VMEM((hidden, half), BF16),
            pltpu.VMEM((hidden, half), BF16),
        ]
        + [one] * 16
        + [dma((NT,))]
        + [one] * 12
        + [dma((n * PARTS,)) for n in (1, 1, 8, 1, 1, 1, 2, 8, 2)]
        + [pltpu.SemaphoreType.REGULAR],
        compiler_params=pltpu.CompilerParams(
            collective_id=0, has_side_effects=True, vmem_limit_bytes=60 * 1024 * 1024
        ),
    )(tokens, gain, w_up, w_down, cotangent)
    return states, grads


def solution(mesh):
    torus = Mesh(
        mesh.devices.reshape(mesh.shape["section"], NZ, 2, NY, NX),
        ("section", "z", "xl", "y", "xh"),
    )
    dp, tensor = ("z", "xl"), ("y", "xh")
    in_specs = (
        P(dp, tensor),
        P("section", tensor),
        P("section", dp, tensor),
        P("section", tensor, dp),
        P("section", dp, None),
    )
    out_specs = (P("section", dp, tensor), P("section", tensor, dp))
    return jax.shard_map(body, mesh=torus, in_specs=in_specs, out_specs=out_specs, check_vma=False)
```

```python
import jax
import jax.numpy as jnp
from jax import lax
from jax.experimental import pallas as pl
from jax.experimental.pallas import tpu as pltpu
from jax.sharding import Mesh
from jax.sharding import PartitionSpec as P

EPS = 1e-06
MESH = pl.DeviceIdType.MESH
NZ, NY, NX = 8, 4, 2
NT = NY * NX
F32, BF16 = jnp.float32, jnp.bfloat16

SIZES = (32,)*4
STARTS = tuple(sum(SIZES[:m]) for m in range(len(SIZES)))
PARTS = len(SIZES)


def order_of(section):
    gap = 4 / PARTS
    todo = []
    for m in range(PARTS):
        up0 = 18 + 2.5 * gap * m
        pass0 = 31 + 2.7 * gap * m
        down0 = 38 + 3 * gap * m
        up1 = 50 + 3 * gap * m
        if section == 0:
            todo += [(up0, "up", m), (up0 + 10, "hid", m), (down0, "down", m)]
            todo += [(down0 + 6.1, "next", m), (up1 + 4, "sum", m), (up1 + 13.1, "pass", m)]
        else:
            todo += [(up0 + 4, "sum", m), (pass0, "pass", m), (up1 - 6.1, "take", m)]
            todo += [(up1, "up", m), (up1 + 9.2, "hid", m), (up1 + 18.3, "down", m)]
            todo += [(up1 + 23, "next", m)]
    last = 50 + 3 * gap * (PARTS - 1)
    if section == 0:
        todo += [(18.1, "down_copy", 0), (25.8, "cot_spread", 0), (37.9, "cot_pass", 0)]
        todo += [(last + 11, "state", 0), (60.5, "grad", 0)]
    else:
        todo += [(25, "cot_spread", 0), (30.7, "up_copy", 0), (30.8, "cot_pass", 0)]
        todo += [(last + 0.1, "down_copy", 0), (last + 19, "grad", 0)]
    return [(name, m) for _, name, m in sorted(todo)]


def ring_offset(i):
    return ((i + 1) // 2) * (1 - 2 * ((i + 1) % 2))


def kernel(
    width,
    tok_ref, gain_ref, up_ref, down_ref, cot_ref,
    state_ref, grad_ref,
    x_all, c_all, gain_z, up_pair, down_pair,
    part_out, part_own, part_in, sum_in, sum_out, relay, sq_out, sq_in, hid_all,
    y_out, y_in, x_next, grad_own, grad_out, grad_in, grad_done,
    gain_s, gain_r, cotp_s, cotp_r, up_s, up_r, down_s, down_r, upl, downl,
    gr_s, gr_r, gd_s, cotl, cg_s, cp_s, cg_r,
    xin_s, core_s, out_s, out_r, sqh_s, ag_s, sq_s, rt_s, rz_s, sum_s, az_s, rel_s,
    xin_r, sqh_r, ag_r, sq_r, rt_r, rz_r, sum_r, az_r, rel_r,
    go,
):
    section = lax.axis_index("section")
    z = lax.axis_index("z")
    xl = lax.axis_index("xl")
    y = lax.axis_index("y")
    xh = lax.axis_index("xh")
    t = y * NX + xh
    half = up_ref.shape[1]
    feats = tok_ref.shape[1]
    tokens = tok_ref.shape[0]
    hidden = up_ref.shape[2]
    pair = {"xl": 1 - xl}
    core = {"section": 1 - section}
    own = (t - z + NT) % NT
    ahead_t = (z + t) % NT
    ahead = {"z": t, "y": ahead_t // NX, "xh": ahead_t % NX}
    back = {"z": own, "y": z // NX, "xh": z % NX}
    moves = (z + t) > 0
    shares_cot = own != z

    def to_tensor(k):
        return {"y": k // NX, "xh": k % NX}

    def tensor_at(i):
        k = i % NY
        step = k + (k // 2) * (1 - 2 * (k % 2))
        return ((y + step) % NY) * NX + (xh + i // NY) % NX

    def block_at(i):
        return (tensor_at(i) - z + NT) % NT

    def z_at(i):
        return (z + ring_offset(i) + NZ) % NZ

    def helper(step):
        return {"section": 1 - section, "z": (z + step + NZ) % NZ}

    def part(m):
        return pl.ds(STARTS[m], SIZES[m])

    def span_of(m):
        return slice(STARTS[m], STARTS[m] + SIZES[m])

    def side(m, way):
        piece = SIZES[m] // 2
        return pl.ds(STARTS[m] + way * piece, piece)

    def rdma(src, dst, ssem, rsem, dev):
        return pltpu.make_async_remote_copy(
            src_ref=src, dst_ref=dst, send_sem=ssem, recv_sem=rsem,
            device_id=dev, device_id_type=MESH,
        )

    def arrived(ref, sem):
        rdma(ref, ref, gain_s, sem, core).wait_recv()

    def greet(dev):
        pl.semaphore_signal(barrier, inc=1, device_id=dev, device_id_type=MESH)

    with jax.named_scope("barrier"):
        mine = pl.ds(pl.multiple_of(xl * half, 128), half)
        up_here = pltpu.make_async_copy(up_ref.at[0], up_pair.at[mine], upl)
        down_here = pltpu.make_async_copy(down_ref.at[0], down_pair.at[xl], downl)
        up_here.start()
        down_here.start()
        barrier = pltpu.get_barrier_semaphore()

        @pl.loop(1, NZ)
        def _(i):
            greet({"z": z_at(i)})

        @pl.loop(1, NT)
        def _(i):
            greet(to_tensor(tensor_at(i)))

        greet(pair)
        greet(core)
        for step in (1, -1, 2, -2):
            greet(helper(step))

        @pl.when(moves)
        def _():
            greet(ahead)
            greet(back)
            pl.semaphore_wait(barrier, NZ + NT + 6)

        @pl.when(z + t == 0)
        def _():
            pl.semaphore_wait(barrier, NZ + NT + 4)

    def tok_send(m):
        return rdma(tok_ref.at[part(m)], x_all.at[z, part(m)], xin_s, xin_r.at[m], ahead)

    def tok_here(m):
        return pltpu.make_async_copy(tok_ref.at[part(m)], x_all.at[own, part(m)], xin_r.at[m])

    gain_send = rdma(gain_ref, gain_z, gain_s, gain_r, ahead)
    gain_here = pltpu.make_async_copy(gain_ref, gain_z, gain_r)

    def cot_cols(k):
        return cot_ref.at[0, :, pl.ds(pl.multiple_of(k * feats, 128), feats)]

    cot_send = rdma(cot_cols(own), c_all.at[z], cotp_s, cotp_r, {"z": own})
    cot_here = pltpu.make_async_copy(cot_cols(z), c_all.at[z], cotl)
    up_send = rdma(up_ref.at[0], up_pair.at[mine], up_s, up_r, pair)
    down_send = rdma(down_ref.at[0], down_pair.at[xl], down_s, down_r, pair)
    grad_send = rdma(grad_out, grad_in, gr_s, gr_r, pair)

    def start_cot():
        @pl.when(shares_cot)
        def _():
            cot_send.start()

    beside = (y * NX + 1 - xh - z + NT) % NT

    def cot_spread(i):
        return rdma(
            c_all.at[own], c_all.at[own], cg_s, cg_r.at[own], to_tensor(tensor_at(i))
        )

    def cot_pass(i):
        return rdma(
            c_all.at[beside], c_all.at[beside], cp_s, cg_r.at[beside],
            to_tensor(tensor_at(i)),
        )

    def spread_cot():
        @pl.when(shares_cot)
        def _():
            arrived(c_all.at[own], cotp_r)
            for i in (NY, 1, 2, 3):
                cot_spread(i).start()

    def pass_cot():
        @pl.when(beside != z)
        def _():
            arrived(c_all.at[beside], cg_r.at[beside])
            for i in range(1, NY):
                cot_pass(i).start()

    def wait_cot():
        @pl.loop(1, NT)
        def _(i):
            k = block_at(i)

            @pl.when((k != z) & (i != NY))
            def _():
                arrived(c_all.at[k], cg_r.at[k])

        cot_here.wait()

    def sum_send(m, way):
        return rdma(
            sum_out.at[way, part(m)], part_in.at[2 + way, part(m)],
            sum_s, rz_r.at[m], helper(2 - 4 * way),
        )

    def sum_stage(m):
        for way in range(2):
            arrived(part_out.at[0, pl.ds(0, SIZES[m] * 5 // 2)], sum_r.at[m * 2 + way])
            for which in range(2):
                piece = SIZES[m] // 2
                rows = slice(STARTS[m] + which * piece, STARTS[m] + (which + 1) * piece)
                total = sum_in[way, 0, rows].astype(F32) + sum_in[way, 1, rows].astype(F32)
                if which == way:
                    total = total + sum_in[way, 2, rows].astype(F32)
                sum_out[way, rows] = total.astype(BF16)
            sum_send(m, way).start()

    def relay_sends(m, way):
        sign = 1 - 2 * way
        block = (z - 2 * sign + NZ) % NZ
        first = m * 4 - way
        full = relay.at[way, part(m)]
        whole = hid_all.at[block, part(m)]
        return (
            rdma(
                relay.at[way, side(m, way)], hid_all.at[block, side(m, way)],
                rel_s, az_r.at[m * 4 + 3], helper(2 * sign),
            ),
            rdma(full, whole, rel_s, az_r.at[first + 3], helper(sign)),
            rdma(full, whole, rel_s, az_r.at[first + 2], core),
        )

    def pass_stage(m):
        for way in range(2):
            arrived(relay.at[way, part(m)], rel_r.at[m * 2 + way])
            for copy in relay_sends(m, way):
                copy.start()

    def spread(m, i):
        return rdma(
            x_all.at[own, part(m)], x_all.at[own, part(m)],
            ag_s, ag_r.at[own if m == 0 else NT + 2 * (m - 1) + i // NY], to_tensor(tensor_at(i)),
        )

    def sq_copy(m):
        return rdma(sq_out.at[m], sq_in.at[m, z], sqh_s, sqh_r.at[m], {"z": own})

    def sq_spread(m, i):
        return rdma(
            sq_in.at[m, own], sq_in.at[m, own],
            sq_s, sq_r.at[m], to_tensor(tensor_at(i)),
        )

    def sq_stage(m):
        @pl.when(shares_cot)
        def _():
            arrived(sq_in.at[m, own], sqh_r.at[m])

        @pl.loop(1, NT)
        def _(i):
            sq_spread(m, i).start()

    def take_stage(m):
        arrived(x_all.at[own, part(m)], xin_r.at[m])

        @pl.loop(1, NT)
        def _(i):
            spread(m, i).start()

        x_f = x_all[own, span_of(m)].astype(F32)
        sq = x_f * x_f
        sq = sum(sq[:, c:c + tokens] for c in range(0, feats, tokens))
        sq = jnp.concatenate([sq] * (tokens // SIZES[m]), axis=0)
        sq_hi = sq.astype(BF16)
        sq_lo = (sq - sq_hi.astype(F32)).astype(BF16)
        ones = jnp.ones((8, tokens), BF16)
        row_dims = (((1,), (1,)), ((), ()))
        sq_row = lax.dot_general(ones, sq_hi, row_dims, preferred_element_type=F32)
        sq_row = sq_row + lax.dot_general(ones, sq_lo, row_dims, preferred_element_type=F32)
        sq_out[m] = sq_row

        @pl.when(own == z)
        def _():
            sq_in[m, z] = sq_row

        @pl.when(shares_cot)
        def _():
            sq_copy(m).start()

    def part_copies(m, k, way, dist):
        sign = 1 - 2 * way
        src = part_out.at[k, part(m)]
        summed = sum_r.at[m * 2 + way]
        if dist == 1:
            dst = part_in.at[way, part(m)]
            return (rdma(src, dst, rz_s, rz_r.at[m], {"z": k}),)
        if dist == 2:
            return (rdma(src, sum_in.at[way, 0, part(m)], rz_s, summed, core),)
        if dist == 3:
            dst = sum_in.at[way, 1, part(m)]
            return (rdma(src, dst, rz_s, summed, helper(sign)),)
        return tuple(
            rdma(
                part_out.at[k, side(m, w)], sum_in.at[w, 2, side(m, w)],
                rz_s, sum_r.at[m * 2 + w], helper(2 - 4 * w),
            )
            for w in range(2)
        )

    def up_stage(m):
        gain_f = gain_z[...].astype(F32)
        rows = SIZES[m]
        group = 4 if m else 2

        @pl.loop(0, NT // group)
        def _(j):
            scaled = []
            if m > 0:
                @pl.when(j == 0)
                def _():
                    arrived(x_all.at[pl.ds(0, NY - 1), part(m)], ag_r.at[NT + 2 * (m - 1)])

                @pl.when(j == 1)
                def _():
                    arrived(x_all.at[pl.ds(0, NY), part(m)], ag_r.at[NT + 2 * (m - 1) + 1])

            for n in range(group):
                i = group * j + n
                k = block_at(i)
                if m == 0:
                    @pl.when(i > 0)
                    def _():
                        arrived(x_all.at[k, part(m)], ag_r.at[k])

                scaled.append((x_all[k, span_of(m)].astype(F32) * gain_f).astype(BF16))
            both = jnp.dot(
                jnp.concatenate(scaled, axis=0), up_pair[...], preferred_element_type=F32
            ).astype(BF16)
            for n in range(group):
                k = block_at(group * j + n)
                value = both[n * rows:(n + 1) * rows]
                delta = (k - z + NZ) % NZ
                way = delta // 5
                dist = delta + way * (NZ - 2 * delta)

                @pl.when(k == z)
                def _():
                    part_own[span_of(m)] = value

                @pl.when(k != z)
                def _():
                    part_out[k, span_of(m)] = value

                for far in range(1, 5):
                    @pl.when(dist == far)
                    def _():
                        for copy in part_copies(m, k, way, far):
                            copy.start()

        sq_stage(m)

    def hid_sends(m):
        block = hid_all.at[z, part(m)]
        out = []
        for way in range(2):
            sign = 1 - 2 * way
            out.append(
                rdma(
                    block, relay.at[way, part(m)], az_s,
                    rel_r.at[m * 2 + way], helper(2 * sign),
                )
            )
            out.append(
                rdma(
                    block, block, az_s, az_r.at[m * 4 + 1 - way],
                    {"z": (z + sign + NZ) % NZ},
                )
            )
        return out

    def hid_stage(m):
        rows = SIZES[m]

        arrived(sq_in.at[m, pl.ds(0, NZ - 1)], sq_r.at[m])
        arrived(part_in.at[:, part(m)], rz_r.at[m])
        total = part_own[span_of(m)].astype(F32)
        for slot in range(4):
            total = total + part_in[slot, span_of(m)].astype(F32)
        sq_sum = sum(sq_in[m, k] for k in range(NZ))
        square = jnp.transpose(jnp.broadcast_to(sq_sum[0:1, :], (tokens, tokens)))
        mean_col = square[0:rows, 0:1] / width
        pre_act = total * lax.rsqrt(mean_col + EPS)
        hid_all[z, span_of(m)] = jax.nn.gelu(pre_act, approximate=True).astype(BF16)
        for copy in hid_sends(m):
            copy.start()

    def y_copy(m, k):
        return rdma(
            y_out.at[k, part(m)], y_in.at[t, part(m)],
            rt_s, rt_r.at[m], to_tensor((k + z) % NT),
        )

    def down_stage(m):
        rows = SIZES[m]

        @pl.loop(0, NZ // 2)
        def _(j):
            @pl.when(j == 0)
            def _():
                arrived(hid_all.at[0, part(m)], az_r.at[m * 4])

            @pl.when(j > 0)
            def _():
                arrived(hid_all.at[pl.ds(0, 2), part(m)], az_r.at[m * 4 + j])

            hid = [hid_all[z_at(2 * j + n), span_of(m)] for n in range(2)]
            hid = jnp.concatenate(hid, axis=0)
            y_lo = jnp.dot(hid, down_pair[0], preferred_element_type=F32).astype(BF16)
            y_hi = jnp.dot(hid, down_pair[1], preferred_element_type=F32).astype(BF16)
            for n in range(2):
                k = z_at(2 * j + n)
                rng = slice(n * rows, (n + 1) * rows)

                @pl.when(k == own)
                def _():
                    y_in[t, span_of(m), 0:half] = y_lo[rng]
                    y_in[t, span_of(m), half:] = y_hi[rng]

                @pl.when(k != own)
                def _():
                    y_out[k, span_of(m), 0:half] = y_lo[rng]
                    y_out[k, span_of(m), half:] = y_hi[rng]
                    y_copy(m, k).start()

    def core_send(m):
        return rdma(x_next.at[part(m)], x_all.at[own, part(m)], core_s, xin_r.at[m], core)

    def state_send(m):
        return rdma(x_next.at[part(m)], state_ref.at[0, part(m)], out_s, out_r, back)

    def state_here(m):
        return pltpu.make_async_copy(x_next.at[part(m)], state_ref.at[0, part(m)], out_r)

    def store_state(m):
        @pl.when(moves)
        def _():
            state_send(m).start()

        @pl.when(z + t == 0)
        def _():
            state_here(m).start()

    def next_stage(m, first_section):
        arrived(y_in.at[pl.ds(0, NT - 1), part(m)], rt_r.at[m])

        total = x_all[own, span_of(m)].astype(F32)
        for k in range(NT):
            total = total + y_in[k, span_of(m)].astype(F32)
        x_next[span_of(m)] = total.astype(BF16)
        if first_section:
            core_send(m).start()
        else:
            store_state(m)

    def grad_half(which):
        hid_t = hid_all[...].reshape(NZ * tokens, hidden)
        cols = pl.ds(pl.multiple_of(which * half, 128), half)
        cot = c_all[:, :, cols].reshape(NZ * tokens, half)
        return lax.dot_general(hid_t, cot, (((0,), (0,)), ((), ())), preferred_element_type=F32)

    def grad_stage():
        wait_cot()
        grad_out[...] = grad_half(1 - xl).astype(BF16)
        grad_send.start()
        grad_own[...] = grad_half(xl)

    def wait_up():
        arrived(gain_z, gain_r)
        up_here.wait()
        up_send.wait_recv()

    def wait_down():
        down_here.wait()
        down_send.wait_recv()

    def run(which):
        met = set()
        for name, m in order_of(which):
            with jax.named_scope("%s%d" % (name, m)):
                if name == "up" and name not in met:
                    wait_up()
                if name == "down" and name not in met:
                    wait_down()
                met.add(name)
                if name == "take":
                    take_stage(m)
                elif name == "up":
                    up_stage(m)
                elif name == "sum":
                    sum_stage(m)
                elif name == "hid":
                    hid_stage(m)
                elif name == "pass":
                    pass_stage(m)
                elif name == "down":
                    down_stage(m)
                elif name == "next":
                    next_stage(m, which == 0)
                elif name == "up_copy":
                    up_send.start()
                elif name == "down_copy":
                    down_send.start()
                elif name == "cot_spread":
                    spread_cot()
                elif name == "cot_pass":
                    pass_cot()
                elif name == "state":
                    for n in range(PARTS):
                        store_state(n)
                elif name == "grad":
                    grad_stage()

    cot_here.start()

    @pl.when(moves)
    def _():
        gain_send.start()

    @pl.when(z + t == 0)
    def _():
        gain_here.start()

    @pl.when(section == 0)
    def _():
        with jax.named_scope("send0"):
            @pl.when(moves)
            def _():
                for m in range(PARTS):
                    tok_send(m).start()

            @pl.when(z + t == 0)
            def _():
                for m in range(PARTS):
                    tok_here(m).start()

            up_send.start()

        with jax.named_scope("waitx"):
            for m in range(PARTS):
                take_stage(m)
            start_cot()
            pl.semaphore_signal(go, inc=1, device_id=core, device_id_type=MESH)
        run(0)

    @pl.when(section == 1)
    def _():
        with jax.named_scope("waitgo"):
            pl.semaphore_wait(go, 1)
            start_cot()
        run(1)

    with jax.named_scope("waitgrad"):
        grad_send.wait_recv()
        grad_done[...] = (grad_own[...] + grad_in[...].astype(F32)).astype(BF16)
        grad_store = pltpu.make_async_copy(grad_done, grad_ref.at[0], gd_s)
        grad_store.start()

    with jax.named_scope("drain"):
        def left(ref, sem):
            rdma(ref, ref, sem, gain_r, core).wait_send()

        @pl.when(section == 0)
        def _():
            left(x_next, core_s)

        @pl.when(moves & (section == 0))
        def _():
            left(x_next, xin_s)

        @pl.when(shares_cot)
        def _():
            cot_send.wait_send()
            left(c_all.at[pl.ds(0, NY)], cg_s)
            left(sq_out, sqh_s)

        @pl.when(beside != z)
        def _():
            left(c_all.at[pl.ds(0, NY - 1)], cp_s)

        @pl.when(moves)
        def _():
            gain_send.wait_send()
            left(x_next, out_s)

        up_send.wait_send()
        down_send.wait_send()
        grad_send.wait_send()
        left(x_all.at[pl.ds(0, NT - 1)], ag_s)
        left(sq_in.at[:, pl.ds(0, NT - 1)], sq_s)
        left(y_out.at[pl.ds(0, NT - 1)], rt_s)
        left(part_out.at[pl.ds(0, NZ - 1)], rz_s)
        left(sum_out, sum_s)
        left(hid_all.at[pl.ds(0, 4)], az_s)
        left(hid_all.at[pl.ds(0, 5)], rel_s)

    with jax.named_scope("waitstate"):
        arrived(state_ref.at[0], out_r)
        grad_store.wait()


def body(tokens, gain, w_up, w_down, cotangent):
    rows, feats = tokens.shape
    half, hidden = w_up.shape[1:]
    width = cotangent.shape[2]
    dma = pltpu.SemaphoreType.DMA
    hbm = pl.BlockSpec(memory_space=pl.ANY)

    def run(*refs):
        kernel(width, *refs)

    one = dma(())
    states, grads = pl.pallas_call(
        run,
        out_shape=(
            jax.ShapeDtypeStruct((1, rows, feats), BF16),
            jax.ShapeDtypeStruct((1, hidden, half), BF16),
        ),
        in_specs=[hbm] * 5,
        out_specs=(hbm, hbm),
        scratch_shapes=[
            pltpu.VMEM((NT, rows, feats), BF16),
            pltpu.VMEM((NT, rows, feats), BF16),
            pltpu.VMEM((1, feats), BF16),
            pltpu.VMEM((2 * half, hidden), BF16),
            pltpu.VMEM((2, hidden, half), BF16),
            pltpu.VMEM((NZ, rows, hidden), BF16),
            pltpu.VMEM((rows, hidden), BF16),
            pltpu.VMEM((4, rows, hidden), BF16),
            pltpu.VMEM((2, 3, rows, hidden), BF16),
            pltpu.VMEM((2, rows, hidden), BF16),
            pltpu.VMEM((2, rows, hidden), BF16),
            pltpu.VMEM((PARTS, 8, rows), F32),
            pltpu.VMEM((PARTS, NZ, 8, rows), F32),
            pltpu.VMEM((NZ, rows, hidden), BF16),
            pltpu.VMEM((NT, rows, feats), BF16),
            pltpu.VMEM((NT, rows, feats), BF16),
            pltpu.VMEM((rows, feats), BF16),
            pltpu.VMEM((hidden, half), F32),
            pltpu.VMEM((hidden, half), BF16),
            pltpu.VMEM((hidden, half), BF16),
            pltpu.VMEM((hidden, half), BF16),
        ]
        + [one] * 16
        + [dma((NT,))]
        + [one] * 12
        + [dma((n * PARTS,)) for n in (1, 1, 4, 1, 1, 1, 2, 4, 2)]
        + [pltpu.SemaphoreType.REGULAR],
        compiler_params=pltpu.CompilerParams(
            collective_id=0, has_side_effects=True, vmem_limit_bytes=60 * 1024 * 1024
        ),
    )(tokens, gain, w_up, w_down, cotangent)
    return states, grads


def solution(mesh):
    torus = Mesh(
        mesh.devices.reshape(mesh.shape["section"], NZ, 2, NY, NX),
        ("section", "z", "xl", "y", "xh"),
    )
    dp, tensor = ("z", "xl"), ("y", "xh")
    in_specs = (
        P(dp, tensor),
        P("section", tensor),
        P("section", dp, tensor),
        P("section", tensor, dp),
        P("section", dp, None),
    )
    out_specs = (P("section", dp, tensor), P("section", tensor, dp))
    return jax.shard_map(body, mesh=torus, in_specs=in_specs, out_specs=out_specs, check_vma=False)
```

```python
import jax
import jax.numpy as jnp
from jax import lax
from jax.experimental import pallas as pl
from jax.experimental.pallas import tpu as pltpu
from jax.sharding import Mesh
from jax.sharding import PartitionSpec as P

EPS = 1e-06
MESH = pl.DeviceIdType.MESH
NZ, NY, NX = 8, 4, 2
NT = NY * NX
F32, BF16 = jnp.float32, jnp.bfloat16

SIZES = (32,)*4
STARTS = tuple(sum(SIZES[:m]) for m in range(len(SIZES)))
PARTS = len(SIZES)


def order_of(section):
    gap = 4 / PARTS
    todo = []
    for m in range(PARTS):
        up0 = 18 + 2.5 * gap * m
        pass0 = 31 + 2.7 * gap * m
        down0 = 38 + 3 * gap * m
        up1 = 50 + 3 * gap * m
        if section == 0:
            todo += [(up0, "up", m), (up0 + 10, "hid", m), (down0, "down", m)]
            todo += [(down0 + 6.1, "next", m), (up1 + 4, "sum", m), (up1 + 13.1, "pass", m)]
        else:
            todo += [(up0 + 4, "sum", m), (pass0, "pass", m), (up1 - 6.1, "take", m)]
            todo += [(up1, "up", m), (up1 + 9.2, "hid", m), (up1 + 18.3, "down", m)]
            todo += [(up1 + 23, "next", m)]
    last = 50 + 3 * gap * (PARTS - 1)
    if section == 0:
        todo += [(18.1, "down_copy", 0), (25.8, "cot_spread", 0), (33.2, "cot_pass", 0)]
        todo += [(last + 14, "state", 0), (60.5, "grad", 0)]
    else:
        todo += [(25, "cot_spread", 0), (30.7, "up_copy", 0), (30.8, "cot_pass", 0)]
        todo += [(last + 0.1, "down_copy", 0), (last + 19, "grad", 0)]
    return [(name, m) for _, name, m in sorted(todo)]


def ring_offset(i):
    return ((i + 1) // 2) * (1 - 2 * ((i + 1) % 2))


def kernel(
    width,
    tok_ref, gain_ref, up_ref, down_ref, cot_ref,
    state_ref, grad_ref,
    x_all, c_all, gain_z, up_pair, down_pair,
    part_out, part_own, part_in, sum_in, sum_out, relay, sq_out, sq_in, hid_all,
    y_out, y_in, x_next, grad_own, grad_out, grad_in, grad_done,
    gain_s, gain_r, cotp_s, cotp_r, up_s, up_r, down_s, down_r, upl, downl,
    gr_s, gr_r, gd_s, cotl, cg_s, cp_s, cg_r,
    xin_s, core_s, out_s, out_r, sqh_s, ag_s, sq_s, rt_s, rz_s, sum_s, az_s, rel_s,
    xin_r, sqh_r, ag_r, sq_r, rt_r, rz_r, sum_r, az_r, rel_r,
    go,
):
    section = lax.axis_index("section")
    z = lax.axis_index("z")
    xl = lax.axis_index("xl")
    y = lax.axis_index("y")
    xh = lax.axis_index("xh")
    t = y * NX + xh
    half = up_ref.shape[1]
    feats = tok_ref.shape[1]
    tokens = tok_ref.shape[0]
    hidden = up_ref.shape[2]
    pair = {"xl": 1 - xl}
    core = {"section": 1 - section}
    own = (t - z + NT) % NT
    ahead_t = (z + t) % NT
    ahead = {"z": t, "y": ahead_t // NX, "xh": ahead_t % NX}
    back = {"z": own, "y": z // NX, "xh": z % NX}
    moves = (z + t) > 0
    shares_cot = own != z

    def to_tensor(k):
        return {"y": k // NX, "xh": k % NX}

    def tensor_at(i):
        k = i % NY
        step = k + (k // 2) * (1 - 2 * (k % 2))
        return ((y + step) % NY) * NX + (xh + i // NY) % NX

    def block_at(i):
        return (tensor_at(i) - z + NT) % NT

    def z_at(i):
        return (z + ring_offset(i) + NZ) % NZ

    def helper(step):
        return {"section": 1 - section, "z": (z + step + NZ) % NZ}

    def part(m):
        return pl.ds(STARTS[m], SIZES[m])

    def span_of(m):
        return slice(STARTS[m], STARTS[m] + SIZES[m])

    def side(m, way):
        piece = SIZES[m] // 2
        return pl.ds(STARTS[m] + way * piece, piece)

    def rdma(src, dst, ssem, rsem, dev):
        return pltpu.make_async_remote_copy(
            src_ref=src, dst_ref=dst, send_sem=ssem, recv_sem=rsem,
            device_id=dev, device_id_type=MESH,
        )

    def arrived(ref, sem):
        rdma(ref, ref, gain_s, sem, core).wait_recv()

    def greet(dev):
        pl.semaphore_signal(barrier, inc=1, device_id=dev, device_id_type=MESH)

    with jax.named_scope("barrier"):
        mine = pl.ds(pl.multiple_of(xl * half, 128), half)
        up_here = pltpu.make_async_copy(up_ref.at[0], up_pair.at[mine], upl)
        down_here = pltpu.make_async_copy(down_ref.at[0], down_pair.at[xl], downl)
        up_here.start()
        down_here.start()
        barrier = pltpu.get_barrier_semaphore()

        @pl.loop(1, NZ)
        def _(i):
            greet({"z": z_at(i)})

        @pl.loop(1, NT)
        def _(i):
            greet(to_tensor(tensor_at(i)))

        greet(pair)
        greet(core)
        for step in (1, -1, 2, -2):
            greet(helper(step))

        @pl.when(moves)
        def _():
            greet(ahead)
            greet(back)
            pl.semaphore_wait(barrier, NZ + NT + 6)

        @pl.when(z + t == 0)
        def _():
            pl.semaphore_wait(barrier, NZ + NT + 4)

    def tok_send(m):
        return rdma(tok_ref.at[part(m)], x_all.at[z, part(m)], xin_s, xin_r.at[m], ahead)

    def tok_here(m):
        return pltpu.make_async_copy(tok_ref.at[part(m)], x_all.at[own, part(m)], xin_r.at[m])

    gain_send = rdma(gain_ref, gain_z, gain_s, gain_r, ahead)
    gain_here = pltpu.make_async_copy(gain_ref, gain_z, gain_r)

    def cot_cols(k):
        return cot_ref.at[0, :, pl.ds(pl.multiple_of(k * feats, 128), feats)]

    cot_send = rdma(cot_cols(own), c_all.at[z], cotp_s, cotp_r, {"z": own})
    cot_here = pltpu.make_async_copy(cot_cols(z), c_all.at[z], cotl)
    up_send = rdma(up_ref.at[0], up_pair.at[mine], up_s, up_r, pair)
    down_send = rdma(down_ref.at[0], down_pair.at[xl], down_s, down_r, pair)
    grad_send = rdma(grad_out, grad_in, gr_s, gr_r, pair)

    def start_cot():
        @pl.when(shares_cot)
        def _():
            cot_send.start()

    beside = (y * NX + 1 - xh - z + NT) % NT

    def cot_spread(i):
        return rdma(
            c_all.at[own], c_all.at[own], cg_s, cg_r.at[own], to_tensor(tensor_at(i))
        )

    def cot_pass(i):
        return rdma(
            c_all.at[beside], c_all.at[beside], cp_s, cg_r.at[beside],
            to_tensor(tensor_at(i)),
        )

    def spread_cot():
        @pl.when(shares_cot)
        def _():
            arrived(c_all.at[own], cotp_r)
            for i in (NY, 1, 2, 3):
                cot_spread(i).start()

    def pass_cot():
        @pl.when(beside != z)
        def _():
            arrived(c_all.at[beside], cg_r.at[beside])
            for i in range(1, NY):
                cot_pass(i).start()

    def wait_cot():
        @pl.loop(1, NT)
        def _(i):
            k = block_at(i)

            @pl.when((k != z) & (i != NY))
            def _():
                arrived(c_all.at[k], cg_r.at[k])

        cot_here.wait()

    def sum_send(m, way):
        return rdma(
            sum_out.at[way, part(m)], part_in.at[2 + way, part(m)],
            sum_s, rz_r.at[m], helper(2 - 4 * way),
        )

    def sum_stage(m):
        for way in range(2):
            arrived(part_out.at[0, pl.ds(0, SIZES[m] * 5 // 2)], sum_r.at[m * 2 + way])
            for which in range(2):
                piece = SIZES[m] // 2
                rows = slice(STARTS[m] + which * piece, STARTS[m] + (which + 1) * piece)
                total = sum_in[way, 0, rows].astype(F32) + sum_in[way, 1, rows].astype(F32)
                if which == way:
                    total = total + sum_in[way, 2, rows].astype(F32)
                sum_out[way, rows] = total.astype(BF16)
            sum_send(m, way).start()

    def relay_sends(m, way):
        sign = 1 - 2 * way
        block = (z - 2 * sign + NZ) % NZ
        first = m * 4 - way
        full = relay.at[way, part(m)]
        whole = hid_all.at[block, part(m)]
        return (
            rdma(
                relay.at[way, side(m, way)], hid_all.at[block, side(m, way)],
                rel_s, az_r.at[m * 4 + 3], helper(2 * sign),
            ),
            rdma(full, whole, rel_s, az_r.at[first + 3], helper(sign)),
            rdma(full, whole, rel_s, az_r.at[first + 2], core),
        )

    def pass_stage(m):
        for way in range(2):
            arrived(relay.at[way, part(m)], rel_r.at[m * 2 + way])
            for copy in relay_sends(m, way):
                copy.start()

    def spread(m, i):
        return rdma(
            x_all.at[own, part(m)], x_all.at[own, part(m)],
            ag_s, ag_r.at[own if m == 0 else NT + 2 * (m - 1) + i // NY], to_tensor(tensor_at(i)),
        )

    def sq_copy(m):
        return rdma(sq_out.at[m], sq_in.at[m, z], sqh_s, sqh_r.at[m], {"z": own})

    def sq_spread(m, i):
        return rdma(
            sq_in.at[m, own], sq_in.at[m, own],
            sq_s, sq_r.at[m], to_tensor(tensor_at(i)),
        )

    def sq_stage(m):
        @pl.when(shares_cot)
        def _():
            arrived(sq_in.at[m, own], sqh_r.at[m])

        @pl.loop(1, NT)
        def _(i):
            sq_spread(m, i).start()

    def take_stage(m):
        arrived(x_all.at[own, part(m)], xin_r.at[m])

        @pl.loop(1, NT)
        def _(i):
            spread(m, i).start()

        x_f = x_all[own, span_of(m)].astype(F32)
        sq = x_f * x_f
        sq = sum(sq[:, c:c + tokens] for c in range(0, feats, tokens))
        sq = jnp.concatenate([sq] * (tokens // SIZES[m]), axis=0)
        sq_hi = sq.astype(BF16)
        sq_lo = (sq - sq_hi.astype(F32)).astype(BF16)
        ones = jnp.ones((8, tokens), BF16)
        row_dims = (((1,), (1,)), ((), ()))
        sq_row = lax.dot_general(ones, sq_hi, row_dims, preferred_element_type=F32)
        sq_row = sq_row + lax.dot_general(ones, sq_lo, row_dims, preferred_element_type=F32)
        sq_out[m] = sq_row

        @pl.when(own == z)
        def _():
            sq_in[m, z] = sq_row

        @pl.when(shares_cot)
        def _():
            sq_copy(m).start()

    def part_copies(m, k, way, dist):
        sign = 1 - 2 * way
        src = part_out.at[k, part(m)]
        summed = sum_r.at[m * 2 + way]
        if dist == 1:
            dst = part_in.at[way, part(m)]
            return (rdma(src, dst, rz_s, rz_r.at[m], {"z": k}),)
        if dist == 2:
            return (rdma(src, sum_in.at[way, 0, part(m)], rz_s, summed, core),)
        if dist == 3:
            dst = sum_in.at[way, 1, part(m)]
            return (rdma(src, dst, rz_s, summed, helper(sign)),)
        return tuple(
            rdma(
                part_out.at[k, side(m, w)], sum_in.at[w, 2, side(m, w)],
                rz_s, sum_r.at[m * 2 + w], helper(2 - 4 * w),
            )
            for w in range(2)
        )

    def up_stage(m):
        gain_f = gain_z[...].astype(F32)
        rows = SIZES[m]
        group = 4 if m else 2

        @pl.loop(0, NT // group)
        def _(j):
            scaled = []
            if m > 0:
                @pl.when(j == 0)
                def _():
                    arrived(x_all.at[pl.ds(0, NY - 1), part(m)], ag_r.at[NT + 2 * (m - 1)])

                @pl.when(j == 1)
                def _():
                    arrived(x_all.at[pl.ds(0, NY), part(m)], ag_r.at[NT + 2 * (m - 1) + 1])

            for n in range(group):
                i = group * j + n
                k = block_at(i)
                if m == 0:
                    @pl.when(i > 0)
                    def _():
                        arrived(x_all.at[k, part(m)], ag_r.at[k])

                scaled.append((x_all[k, span_of(m)].astype(F32) * gain_f).astype(BF16))
            both = jnp.dot(
                jnp.concatenate(scaled, axis=0), up_pair[...], preferred_element_type=F32
            ).astype(BF16)
            for n in range(group):
                k = block_at(group * j + n)
                value = both[n * rows:(n + 1) * rows]
                delta = (k - z + NZ) % NZ
                way = delta // 5
                dist = delta + way * (NZ - 2 * delta)

                @pl.when(k == z)
                def _():
                    part_own[span_of(m)] = value

                @pl.when(k != z)
                def _():
                    part_out[k, span_of(m)] = value

                for far in range(1, 5):
                    @pl.when(dist == far)
                    def _():
                        for copy in part_copies(m, k, way, far):
                            copy.start()

        sq_stage(m)

    def hid_sends(m):
        block = hid_all.at[z, part(m)]
        out = []
        for way in range(2):
            sign = 1 - 2 * way
            out.append(
                rdma(
                    block, relay.at[way, part(m)], az_s,
                    rel_r.at[m * 2 + way], helper(2 * sign),
                )
            )
            out.append(
                rdma(
                    block, block, az_s, az_r.at[m * 4 + 1 - way],
                    {"z": (z + sign + NZ) % NZ},
                )
            )
        return out

    def hid_stage(m):
        rows = SIZES[m]

        arrived(sq_in.at[m, pl.ds(0, NZ - 1)], sq_r.at[m])
        arrived(part_in.at[:, part(m)], rz_r.at[m])
        total = part_own[span_of(m)].astype(F32)
        for slot in range(4):
            total = total + part_in[slot, span_of(m)].astype(F32)
        sq_sum = sum(sq_in[m, k] for k in range(NZ))
        square = jnp.transpose(jnp.broadcast_to(sq_sum[0:1, :], (tokens, tokens)))
        mean_col = square[0:rows, 0:1] / width
        pre_act = total * lax.rsqrt(mean_col + EPS)
        hid_all[z, span_of(m)] = jax.nn.gelu(pre_act, approximate=True).astype(BF16)
        for copy in hid_sends(m):
            copy.start()

    def y_copy(m, k):
        return rdma(
            y_out.at[k, part(m)], y_in.at[t, part(m)],
            rt_s, rt_r.at[m], to_tensor((k + z) % NT),
        )

    def down_stage(m):
        rows = SIZES[m]

        @pl.loop(0, NZ // 2)
        def _(j):
            @pl.when(j == 0)
            def _():
                arrived(hid_all.at[0, part(m)], az_r.at[m * 4])

            @pl.when(j > 0)
            def _():
                arrived(hid_all.at[pl.ds(0, 2), part(m)], az_r.at[m * 4 + j])

            hid = [hid_all[z_at(2 * j + n), span_of(m)] for n in range(2)]
            hid = jnp.concatenate(hid, axis=0)
            y_lo = jnp.dot(hid, down_pair[0], preferred_element_type=F32).astype(BF16)
            y_hi = jnp.dot(hid, down_pair[1], preferred_element_type=F32).astype(BF16)
            for n in range(2):
                k = z_at(2 * j + n)
                rng = slice(n * rows, (n + 1) * rows)

                @pl.when(k == own)
                def _():
                    y_in[t, span_of(m), 0:half] = y_lo[rng]
                    y_in[t, span_of(m), half:] = y_hi[rng]

                @pl.when(k != own)
                def _():
                    y_out[k, span_of(m), 0:half] = y_lo[rng]
                    y_out[k, span_of(m), half:] = y_hi[rng]
                    y_copy(m, k).start()

    def core_send(m):
        return rdma(x_next.at[part(m)], x_all.at[own, part(m)], core_s, xin_r.at[m], core)

    def state_send(m):
        return rdma(x_next.at[part(m)], state_ref.at[0, part(m)], out_s, out_r, back)

    def state_here(m):
        return pltpu.make_async_copy(x_next.at[part(m)], state_ref.at[0, part(m)], out_r)

    def store_state(m):
        @pl.when(moves)
        def _():
            state_send(m).start()

        @pl.when(z + t == 0)
        def _():
            state_here(m).start()

    def next_stage(m, first_section):
        arrived(y_in.at[pl.ds(0, NT - 1), part(m)], rt_r.at[m])

        total = x_all[own, span_of(m)].astype(F32)
        for k in range(NT):
            total = total + y_in[k, span_of(m)].astype(F32)
        x_next[span_of(m)] = total.astype(BF16)
        if first_section:
            core_send(m).start()
        else:
            store_state(m)

    def grad_half(which):
        hid_t = hid_all[...].reshape(NZ * tokens, hidden)
        cols = pl.ds(pl.multiple_of(which * half, 128), half)
        cot = c_all[:, :, cols].reshape(NZ * tokens, half)
        return lax.dot_general(hid_t, cot, (((0,), (0,)), ((), ())), preferred_element_type=F32)

    def grad_stage():
        wait_cot()
        grad_out[...] = grad_half(1 - xl).astype(BF16)
        grad_send.start()
        grad_own[...] = grad_half(xl)

    def wait_up():
        arrived(gain_z, gain_r)
        up_here.wait()
        up_send.wait_recv()

    def wait_down():
        down_here.wait()
        down_send.wait_recv()

    def run(which):
        met = set()
        for name, m in order_of(which):
            with jax.named_scope("%s%d" % (name, m)):
                if name == "up" and name not in met:
                    wait_up()
                if name == "down" and name not in met:
                    wait_down()
                met.add(name)
                if name == "take":
                    take_stage(m)
                elif name == "up":
                    up_stage(m)
                elif name == "sum":
                    sum_stage(m)
                elif name == "hid":
                    hid_stage(m)
                elif name == "pass":
                    pass_stage(m)
                elif name == "down":
                    down_stage(m)
                elif name == "next":
                    next_stage(m, which == 0)
                elif name == "up_copy":
                    up_send.start()
                elif name == "down_copy":
                    down_send.start()
                elif name == "cot_spread":
                    spread_cot()
                elif name == "cot_pass":
                    pass_cot()
                elif name == "state":
                    for n in range(PARTS):
                        store_state(n)
                elif name == "grad":
                    grad_stage()

    cot_here.start()

    @pl.when(moves)
    def _():
        gain_send.start()

    @pl.when(z + t == 0)
    def _():
        gain_here.start()

    @pl.when(section == 0)
    def _():
        with jax.named_scope("send0"):
            @pl.when(moves)
            def _():
                for m in range(PARTS):
                    tok_send(m).start()

            @pl.when(z + t == 0)
            def _():
                for m in range(PARTS):
                    tok_here(m).start()

            up_send.start()

        with jax.named_scope("waitx"):
            for m in range(PARTS):
                take_stage(m)
            start_cot()
            pl.semaphore_signal(go, inc=1, device_id=core, device_id_type=MESH)
        run(0)

    @pl.when(section == 1)
    def _():
        with jax.named_scope("waitgo"):
            pl.semaphore_wait(go, 1)
            start_cot()
        run(1)

    with jax.named_scope("waitgrad"):
        grad_send.wait_recv()
        grad_done[...] = (grad_own[...] + grad_in[...].astype(F32)).astype(BF16)
        grad_store = pltpu.make_async_copy(grad_done, grad_ref.at[0], gd_s)
        grad_store.start()

    with jax.named_scope("drain"):
        def left(ref, sem):
            rdma(ref, ref, sem, gain_r, core).wait_send()

        @pl.when(section == 0)
        def _():
            left(x_next, core_s)

        @pl.when(moves & (section == 0))
        def _():
            left(x_next, xin_s)

        @pl.when(shares_cot)
        def _():
            cot_send.wait_send()
            left(c_all.at[pl.ds(0, NY)], cg_s)
            left(sq_out, sqh_s)

        @pl.when(beside != z)
        def _():
            left(c_all.at[pl.ds(0, NY - 1)], cp_s)

        @pl.when(moves)
        def _():
            gain_send.wait_send()
            left(x_next, out_s)

        up_send.wait_send()
        down_send.wait_send()
        grad_send.wait_send()
        left(x_all.at[pl.ds(0, NT - 1)], ag_s)
        left(sq_in.at[:, pl.ds(0, NT - 1)], sq_s)
        left(y_out.at[pl.ds(0, NT - 1)], rt_s)
        left(part_out.at[pl.ds(0, NZ - 1)], rz_s)
        left(sum_out, sum_s)
        left(hid_all.at[pl.ds(0, 4)], az_s)
        left(hid_all.at[pl.ds(0, 5)], rel_s)

    with jax.named_scope("waitstate"):
        arrived(state_ref.at[0], out_r)
        grad_store.wait()


def body(tokens, gain, w_up, w_down, cotangent):
    rows, feats = tokens.shape
    half, hidden = w_up.shape[1:]
    width = cotangent.shape[2]
    dma = pltpu.SemaphoreType.DMA
    hbm = pl.BlockSpec(memory_space=pl.ANY)

    def run(*refs):
        kernel(width, *refs)

    one = dma(())
    states, grads = pl.pallas_call(
        run,
        out_shape=(
            jax.ShapeDtypeStruct((1, rows, feats), BF16),
            jax.ShapeDtypeStruct((1, hidden, half), BF16),
        ),
        in_specs=[hbm] * 5,
        out_specs=(hbm, hbm),
        scratch_shapes=[
            pltpu.VMEM((NT, rows, feats), BF16),
            pltpu.VMEM((NT, rows, feats), BF16),
            pltpu.VMEM((1, feats), BF16),
            pltpu.VMEM((2 * half, hidden), BF16),
            pltpu.VMEM((2, hidden, half), BF16),
            pltpu.VMEM((NZ, rows, hidden), BF16),
            pltpu.VMEM((rows, hidden), BF16),
            pltpu.VMEM((4, rows, hidden), BF16),
            pltpu.VMEM((2, 3, rows, hidden), BF16),
            pltpu.VMEM((2, rows, hidden), BF16),
            pltpu.VMEM((2, rows, hidden), BF16),
            pltpu.VMEM((PARTS, 8, rows), F32),
            pltpu.VMEM((PARTS, NZ, 8, rows), F32),
            pltpu.VMEM((NZ, rows, hidden), BF16),
            pltpu.VMEM((NT, rows, feats), BF16),
            pltpu.VMEM((NT, rows, feats), BF16),
            pltpu.VMEM((rows, feats), BF16),
            pltpu.VMEM((hidden, half), F32),
            pltpu.VMEM((hidden, half), BF16),
            pltpu.VMEM((hidden, half), BF16),
            pltpu.VMEM((hidden, half), BF16),
        ]
        + [one] * 16
        + [dma((NT,))]
        + [one] * 12
        + [dma((n * PARTS,)) for n in (1, 1, 4, 1, 1, 1, 2, 4, 2)]
        + [pltpu.SemaphoreType.REGULAR],
        compiler_params=pltpu.CompilerParams(
            collective_id=0, has_side_effects=True, vmem_limit_bytes=60 * 1024 * 1024
        ),
    )(tokens, gain, w_up, w_down, cotangent)
    return states, grads


def solution(mesh):
    torus = Mesh(
        mesh.devices.reshape(mesh.shape["section"], NZ, 2, NY, NX),
        ("section", "z", "xl", "y", "xh"),
    )
    dp, tensor = ("z", "xl"), ("y", "xh")
    in_specs = (
        P(dp, tensor),
        P("section", tensor),
        P("section", dp, tensor),
        P("section", tensor, dp),
        P("section", dp, None),
    )
    out_specs = (P("section", dp, tensor), P("section", tensor, dp))
    return jax.shard_map(body, mesh=torus, in_specs=in_specs, out_specs=out_specs, check_vma=False)
```

```python
import jax
import jax.numpy as jnp
from jax import lax
from jax.experimental import pallas as pl
from jax.experimental.pallas import tpu as pltpu
from jax.sharding import Mesh
from jax.sharding import PartitionSpec as P

EPS = 1e-06
MESH = pl.DeviceIdType.MESH
NZ, NY, NX = 8, 4, 2
NT = NY * NX
F32, BF16 = jnp.float32, jnp.bfloat16

SIZES = (32,)*4
STARTS = tuple(sum(SIZES[:m]) for m in range(len(SIZES)))
PARTS = len(SIZES)


def order_of(section):
    gap = 4 / PARTS
    todo = []
    for m in range(PARTS):
        up0 = 18 + 2.5 * gap * m
        pass0 = 31 + 2.7 * gap * m
        down0 = 38 + 3 * gap * m
        up1 = 50 + 3 * gap * m
        if section == 0:
            todo += [(up0, "up", m), (up0 + 10, "hid", m), (down0, "down", m)]
            todo += [(down0 + 6.1, "next", m), (up1 + 4, "sum", m), (up1 + 13.1, "pass", m)]
        else:
            todo += [(up0 + 4, "sum", m), (pass0, "pass", m), (up1 - 6.1, "take", m)]
            todo += [(up1, "up", m), (up1 + 9.2, "hid", m), (up1 + 18.3, "down", m)]
            todo += [(up1 + 23, "next", m)]
    last = 50 + 3 * gap * (PARTS - 1)
    if section == 0:
        todo += [(18.1, "down_copy", 0), (25.8, "cot_spread", 0), (33.2, "cot_pass", 0)]
        todo += [(last + 14, "state", 0), (63.05, "grad", 0)]
    else:
        todo += [(25, "cot_spread", 0), (30.7, "up_copy", 0), (30.8, "cot_pass", 0)]
        todo += [(last + 0.1, "down_copy", 0), (last + 19, "grad", 0)]
    return [(name, m) for _, name, m in sorted(todo)]


def ring_offset(i):
    return ((i + 1) // 2) * (1 - 2 * ((i + 1) % 2))


def kernel(
    width,
    tok_ref, gain_ref, up_ref, down_ref, cot_ref,
    state_ref, grad_ref,
    x_all, c_all, gain_z, up_pair, down_pair,
    part_out, part_own, part_in, sum_in, sum_out, relay, sq_out, sq_in, hid_all,
    y_out, y_in, x_next, grad_own, grad_out, grad_in, grad_done,
    gain_s, gain_r, cotp_s, cotp_r, up_s, up_r, down_s, down_r, upl, downl,
    gr_s, gr_r, gd_s, cotl, cg_s, cp_s, cg_r,
    xin_s, core_s, out_s, out_r, sqh_s, ag_s, sq_s, rt_s, rz_s, sum_s, az_s, rel_s,
    xin_r, sqh_r, ag_r, sq_r, rt_r, rz_r, sum_r, az_r, rel_r,
    go,
):
    section = lax.axis_index("section")
    z = lax.axis_index("z")
    xl = lax.axis_index("xl")
    y = lax.axis_index("y")
    xh = lax.axis_index("xh")
    t = y * NX + xh
    half = up_ref.shape[1]
    feats = tok_ref.shape[1]
    tokens = tok_ref.shape[0]
    hidden = up_ref.shape[2]
    pair = {"xl": 1 - xl}
    core = {"section": 1 - section}
    own = (t - z + NT) % NT
    ahead_t = (z + t) % NT
    ahead = {"z": t, "y": ahead_t // NX, "xh": ahead_t % NX}
    back = {"z": own, "y": z // NX, "xh": z % NX}
    moves = (z + t) > 0
    shares_cot = own != z

    def to_tensor(k):
        return {"y": k // NX, "xh": k % NX}

    def tensor_at(i):
        k = i % NY
        step = k + (k // 2) * (1 - 2 * (k % 2))
        return ((y + step) % NY) * NX + (xh + i // NY) % NX

    def block_at(i):
        return (tensor_at(i) - z + NT) % NT

    def z_at(i):
        return (z + ring_offset(i) + NZ) % NZ

    def helper(step):
        return {"section": 1 - section, "z": (z + step + NZ) % NZ}

    def part(m):
        return pl.ds(STARTS[m], SIZES[m])

    def span_of(m):
        return slice(STARTS[m], STARTS[m] + SIZES[m])

    def side(m, way):
        piece = SIZES[m] // 2
        return pl.ds(STARTS[m] + way * piece, piece)

    def rdma(src, dst, ssem, rsem, dev):
        return pltpu.make_async_remote_copy(
            src_ref=src, dst_ref=dst, send_sem=ssem, recv_sem=rsem,
            device_id=dev, device_id_type=MESH,
        )

    def arrived(ref, sem):
        rdma(ref, ref, gain_s, sem, core).wait_recv()

    def greet(dev):
        pl.semaphore_signal(barrier, inc=1, device_id=dev, device_id_type=MESH)

    with jax.named_scope("barrier"):
        mine = pl.ds(pl.multiple_of(xl * half, 128), half)
        up_here = pltpu.make_async_copy(up_ref.at[0], up_pair.at[mine], upl)
        down_here = pltpu.make_async_copy(down_ref.at[0], down_pair.at[xl], downl)
        up_here.start()
        down_here.start()
        barrier = pltpu.get_barrier_semaphore()

        @pl.loop(1, NZ)
        def _(i):
            greet({"z": z_at(i)})

        @pl.loop(1, NT)
        def _(i):
            greet(to_tensor(tensor_at(i)))

        greet(pair)
        greet(core)
        for step in (1, -1, 2, -2):
            greet(helper(step))

        @pl.when(moves)
        def _():
            greet(ahead)
            greet(back)
            pl.semaphore_wait(barrier, NZ + NT + 6)

        @pl.when(z + t == 0)
        def _():
            pl.semaphore_wait(barrier, NZ + NT + 4)

    def tok_send(m):
        return rdma(tok_ref.at[part(m)], x_all.at[z, part(m)], xin_s, xin_r.at[m], ahead)

    def tok_here(m):
        return pltpu.make_async_copy(tok_ref.at[part(m)], x_all.at[own, part(m)], xin_r.at[m])

    gain_send = rdma(gain_ref, gain_z, gain_s, gain_r, ahead)
    gain_here = pltpu.make_async_copy(gain_ref, gain_z, gain_r)

    def cot_cols(k):
        return cot_ref.at[0, :, pl.ds(pl.multiple_of(k * feats, 128), feats)]

    cot_send = rdma(cot_cols(own), c_all.at[z], cotp_s, cotp_r, {"z": own})
    cot_here = pltpu.make_async_copy(cot_cols(z), c_all.at[z], cotl)
    up_send = rdma(up_ref.at[0], up_pair.at[mine], up_s, up_r, pair)
    down_send = rdma(down_ref.at[0], down_pair.at[xl], down_s, down_r, pair)
    grad_send = rdma(grad_out, grad_in, gr_s, gr_r, pair)

    def start_cot():
        @pl.when(shares_cot)
        def _():
            cot_send.start()

    beside = (y * NX + 1 - xh - z + NT) % NT

    def cot_spread(i):
        return rdma(
            c_all.at[own], c_all.at[own], cg_s, cg_r.at[own], to_tensor(tensor_at(i))
        )

    def cot_pass(i):
        return rdma(
            c_all.at[beside], c_all.at[beside], cp_s, cg_r.at[beside],
            to_tensor(tensor_at(i)),
        )

    def spread_cot():
        @pl.when(shares_cot)
        def _():
            arrived(c_all.at[own], cotp_r)
            for i in (NY, 1, 2, 3):
                cot_spread(i).start()

    def pass_cot():
        @pl.when(beside != z)
        def _():
            arrived(c_all.at[beside], cg_r.at[beside])
            for i in range(1, NY):
                cot_pass(i).start()

    def wait_cot():
        @pl.loop(1, NT)
        def _(i):
            k = block_at(i)

            @pl.when((k != z) & (i != NY))
            def _():
                arrived(c_all.at[k], cg_r.at[k])

        cot_here.wait()

    def sum_send(m, way):
        return rdma(
            sum_out.at[way, part(m)], part_in.at[2 + way, part(m)],
            sum_s, rz_r.at[m], helper(2 - 4 * way),
        )

    def sum_stage(m):
        for way in range(2):
            arrived(part_out.at[0, pl.ds(0, SIZES[m] * 5 // 2)], sum_r.at[m * 2 + way])
            for which in range(2):
                piece = SIZES[m] // 2
                rows = slice(STARTS[m] + which * piece, STARTS[m] + (which + 1) * piece)
                total = sum_in[way, 0, rows].astype(F32) + sum_in[way, 1, rows].astype(F32)
                if which == way:
                    total = total + sum_in[way, 2, rows].astype(F32)
                sum_out[way, rows] = total.astype(BF16)
            sum_send(m, way).start()

    def relay_sends(m, way):
        sign = 1 - 2 * way
        block = (z - 2 * sign + NZ) % NZ
        first = m * 4 - way
        full = relay.at[way, part(m)]
        whole = hid_all.at[block, part(m)]
        return (
            rdma(
                relay.at[way, side(m, way)], hid_all.at[block, side(m, way)],
                rel_s, az_r.at[m * 4 + 3], helper(2 * sign),
            ),
            rdma(full, whole, rel_s, az_r.at[first + 3], helper(sign)),
            rdma(full, whole, rel_s, az_r.at[first + 2], core),
        )

    def pass_stage(m):
        for way in range(2):
            arrived(relay.at[way, part(m)], rel_r.at[m * 2 + way])
            for copy in relay_sends(m, way):
                copy.start()

    def spread(m, i):
        return rdma(
            x_all.at[own, part(m)], x_all.at[own, part(m)],
            ag_s, ag_r.at[own if m == 0 else NT + 2 * (m - 1) + i // NY], to_tensor(tensor_at(i)),
        )

    def sq_copy(m):
        return rdma(sq_out.at[m], sq_in.at[m, z], sqh_s, sqh_r.at[m], {"z": own})

    def sq_spread(m, i):
        return rdma(
            sq_in.at[m, own], sq_in.at[m, own],
            sq_s, sq_r.at[m], to_tensor(tensor_at(i)),
        )

    def sq_stage(m):
        @pl.when(shares_cot)
        def _():
            arrived(sq_in.at[m, own], sqh_r.at[m])

        @pl.loop(1, NT)
        def _(i):
            sq_spread(m, i).start()

    def take_stage(m):
        arrived(x_all.at[own, part(m)], xin_r.at[m])

        @pl.loop(1, NT)
        def _(i):
            spread(m, i).start()

        x_f = x_all[own, span_of(m)].astype(F32)
        sq = x_f * x_f
        sq = sum(sq[:, c:c + tokens] for c in range(0, feats, tokens))
        sq = jnp.concatenate([sq] * (tokens // SIZES[m]), axis=0)
        sq_hi = sq.astype(BF16)
        sq_lo = (sq - sq_hi.astype(F32)).astype(BF16)
        ones = jnp.ones((8, tokens), BF16)
        row_dims = (((1,), (1,)), ((), ()))
        sq_row = lax.dot_general(ones, sq_hi, row_dims, preferred_element_type=F32)
        sq_row = sq_row + lax.dot_general(ones, sq_lo, row_dims, preferred_element_type=F32)
        sq_out[m] = sq_row

        @pl.when(own == z)
        def _():
            sq_in[m, z] = sq_row

        @pl.when(shares_cot)
        def _():
            sq_copy(m).start()

    def part_copies(m, k, way, dist):
        sign = 1 - 2 * way
        src = part_out.at[k, part(m)]
        summed = sum_r.at[m * 2 + way]
        if dist == 1:
            dst = part_in.at[way, part(m)]
            return (rdma(src, dst, rz_s, rz_r.at[m], {"z": k}),)
        if dist == 2:
            return (rdma(src, sum_in.at[way, 0, part(m)], rz_s, summed, core),)
        if dist == 3:
            dst = sum_in.at[way, 1, part(m)]
            return (rdma(src, dst, rz_s, summed, helper(sign)),)
        return tuple(
            rdma(
                part_out.at[k, side(m, w)], sum_in.at[w, 2, side(m, w)],
                rz_s, sum_r.at[m * 2 + w], helper(2 - 4 * w),
            )
            for w in range(2)
        )

    def up_stage(m):
        gain_f = gain_z[...].astype(F32)
        rows = SIZES[m]
        group = 4 if m else 2

        @pl.loop(0, NT // group)
        def _(j):
            scaled = []
            if m > 0:
                @pl.when(j == 0)
                def _():
                    arrived(x_all.at[pl.ds(0, NY - 1), part(m)], ag_r.at[NT + 2 * (m - 1)])

                @pl.when(j == 1)
                def _():
                    arrived(x_all.at[pl.ds(0, NY), part(m)], ag_r.at[NT + 2 * (m - 1) + 1])

            for n in range(group):
                i = group * j + n
                k = block_at(i)
                if m == 0:
                    @pl.when(i > 0)
                    def _():
                        arrived(x_all.at[k, part(m)], ag_r.at[k])

                scaled.append((x_all[k, span_of(m)].astype(F32) * gain_f).astype(BF16))
            both = jnp.dot(
                jnp.concatenate(scaled, axis=0), up_pair[...], preferred_element_type=F32
            ).astype(BF16)
            for n in range(group):
                k = block_at(group * j + n)
                value = both[n * rows:(n + 1) * rows]
                delta = (k - z + NZ) % NZ
                way = delta // 5
                dist = delta + way * (NZ - 2 * delta)

                @pl.when(k == z)
                def _():
                    part_own[span_of(m)] = value

                @pl.when(k != z)
                def _():
                    part_out[k, span_of(m)] = value

                for far in range(1, 5):
                    @pl.when(dist == far)
                    def _():
                        for copy in part_copies(m, k, way, far):
                            copy.start()

        sq_stage(m)

    def hid_sends(m):
        block = hid_all.at[z, part(m)]
        out = []
        for way in range(2):
            sign = 1 - 2 * way
            out.append(
                rdma(
                    block, relay.at[way, part(m)], az_s,
                    rel_r.at[m * 2 + way], helper(2 * sign),
                )
            )
            out.append(
                rdma(
                    block, block, az_s, az_r.at[m * 4 + 1 - way],
                    {"z": (z + sign + NZ) % NZ},
                )
            )
        return out

    def hid_stage(m):
        rows = SIZES[m]

        arrived(sq_in.at[m, pl.ds(0, NZ - 1)], sq_r.at[m])
        arrived(part_in.at[:, part(m)], rz_r.at[m])
        total = part_own[span_of(m)].astype(F32)
        for slot in range(4):
            total = total + part_in[slot, span_of(m)].astype(F32)
        sq_sum = sum(sq_in[m, k] for k in range(NZ))
        square = jnp.transpose(jnp.broadcast_to(sq_sum[0:1, :], (tokens, tokens)))
        mean_col = square[0:rows, 0:1] / width
        pre_act = total * lax.rsqrt(mean_col + EPS)
        hid_all[z, span_of(m)] = jax.nn.gelu(pre_act, approximate=True).astype(BF16)
        for copy in hid_sends(m):
            copy.start()

    def y_copy(m, k):
        return rdma(
            y_out.at[k, part(m)], y_in.at[t, part(m)],
            rt_s, rt_r.at[m], to_tensor((k + z) % NT),
        )

    def down_stage(m):
        rows = SIZES[m]

        @pl.loop(0, NZ // 2)
        def _(j):
            @pl.when(j == 0)
            def _():
                arrived(hid_all.at[0, part(m)], az_r.at[m * 4])

            @pl.when(j > 0)
            def _():
                arrived(hid_all.at[pl.ds(0, 2), part(m)], az_r.at[m * 4 + j])

            hid = [hid_all[z_at(2 * j + n), span_of(m)] for n in range(2)]
            hid = jnp.concatenate(hid, axis=0)
            y_lo = jnp.dot(hid, down_pair[0], preferred_element_type=F32).astype(BF16)
            y_hi = jnp.dot(hid, down_pair[1], preferred_element_type=F32).astype(BF16)
            for n in range(2):
                k = z_at(2 * j + n)
                rng = slice(n * rows, (n + 1) * rows)

                @pl.when(k == own)
                def _():
                    y_in[t, span_of(m), 0:half] = y_lo[rng]
                    y_in[t, span_of(m), half:] = y_hi[rng]

                @pl.when(k != own)
                def _():
                    y_out[k, span_of(m), 0:half] = y_lo[rng]
                    y_out[k, span_of(m), half:] = y_hi[rng]
                    y_copy(m, k).start()

    def core_send(m):
        return rdma(x_next.at[part(m)], x_all.at[own, part(m)], core_s, xin_r.at[m], core)

    def state_send(m):
        return rdma(x_next.at[part(m)], state_ref.at[0, part(m)], out_s, out_r, back)

    def state_here(m):
        return pltpu.make_async_copy(x_next.at[part(m)], state_ref.at[0, part(m)], out_r)

    def store_state(m):
        @pl.when(moves)
        def _():
            state_send(m).start()

        @pl.when(z + t == 0)
        def _():
            state_here(m).start()

    def next_stage(m, first_section):
        arrived(y_in.at[pl.ds(0, NT - 1), part(m)], rt_r.at[m])

        total = x_all[own, span_of(m)].astype(F32)
        for k in range(NT):
            total = total + y_in[k, span_of(m)].astype(F32)
        x_next[span_of(m)] = total.astype(BF16)
        if first_section:
            core_send(m).start()
        else:
            store_state(m)

    def grad_half(which):
        hid_t = hid_all[...].reshape(NZ * tokens, hidden)
        cols = pl.ds(pl.multiple_of(which * half, 128), half)
        cot = c_all[:, :, cols].reshape(NZ * tokens, half)
        return lax.dot_general(hid_t, cot, (((0,), (0,)), ((), ())), preferred_element_type=F32)

    def grad_stage():
        wait_cot()
        grad_out[...] = grad_half(1 - xl).astype(BF16)
        grad_send.start()
        grad_own[...] = grad_half(xl)

    def wait_up():
        arrived(gain_z, gain_r)
        up_here.wait()
        up_send.wait_recv()

    def wait_down():
        down_here.wait()
        down_send.wait_recv()

    def run(which):
        met = set()
        for name, m in order_of(which):
            with jax.named_scope("%s%d" % (name, m)):
                if name == "up" and name not in met:
                    wait_up()
                if name == "down" and name not in met:
                    wait_down()
                met.add(name)
                if name == "take":
                    take_stage(m)
                elif name == "up":
                    up_stage(m)
                elif name == "sum":
                    sum_stage(m)
                elif name == "hid":
                    hid_stage(m)
                elif name == "pass":
                    pass_stage(m)
                elif name == "down":
                    down_stage(m)
                elif name == "next":
                    next_stage(m, which == 0)
                elif name == "up_copy":
                    up_send.start()
                elif name == "down_copy":
                    down_send.start()
                elif name == "cot_spread":
                    spread_cot()
                elif name == "cot_pass":
                    pass_cot()
                elif name == "state":
                    for n in range(PARTS):
                        store_state(n)
                elif name == "grad":
                    grad_stage()

    cot_here.start()

    @pl.when(moves)
    def _():
        gain_send.start()

    @pl.when(z + t == 0)
    def _():
        gain_here.start()

    @pl.when(section == 0)
    def _():
        with jax.named_scope("send0"):
            @pl.when(moves)
            def _():
                for m in range(PARTS):
                    tok_send(m).start()

            @pl.when(z + t == 0)
            def _():
                for m in range(PARTS):
                    tok_here(m).start()

            up_send.start()

        with jax.named_scope("waitx"):
            for m in range(PARTS):
                take_stage(m)
            start_cot()
            pl.semaphore_signal(go, inc=1, device_id=core, device_id_type=MESH)
        run(0)

    @pl.when(section == 1)
    def _():
        with jax.named_scope("waitgo"):
            pl.semaphore_wait(go, 1)
            start_cot()
        run(1)

    with jax.named_scope("waitgrad"):
        grad_send.wait_recv()
        grad_done[...] = (grad_own[...] + grad_in[...].astype(F32)).astype(BF16)
        grad_store = pltpu.make_async_copy(grad_done, grad_ref.at[0], gd_s)
        grad_store.start()

    with jax.named_scope("drain"):
        def left(ref, sem):
            rdma(ref, ref, sem, gain_r, core).wait_send()

        @pl.when(section == 0)
        def _():
            left(x_next, core_s)

        @pl.when(moves & (section == 0))
        def _():
            left(x_next, xin_s)

        @pl.when(shares_cot)
        def _():
            cot_send.wait_send()
            left(c_all.at[pl.ds(0, NY)], cg_s)
            left(sq_out, sqh_s)

        @pl.when(beside != z)
        def _():
            left(c_all.at[pl.ds(0, NY - 1)], cp_s)

        @pl.when(moves)
        def _():
            gain_send.wait_send()
            left(x_next, out_s)

        up_send.wait_send()
        down_send.wait_send()
        grad_send.wait_send()
        left(x_all.at[pl.ds(0, NT - 1)], ag_s)
        left(sq_in.at[:, pl.ds(0, NT - 1)], sq_s)
        left(y_out.at[pl.ds(0, NT - 1)], rt_s)
        left(part_out.at[pl.ds(0, NZ - 1)], rz_s)
        left(sum_out, sum_s)
        left(hid_all.at[pl.ds(0, 4)], az_s)
        left(hid_all.at[pl.ds(0, 5)], rel_s)

    with jax.named_scope("waitstate"):
        arrived(state_ref.at[0], out_r)
        grad_store.wait()


def body(tokens, gain, w_up, w_down, cotangent):
    rows, feats = tokens.shape
    half, hidden = w_up.shape[1:]
    width = cotangent.shape[2]
    dma = pltpu.SemaphoreType.DMA
    hbm = pl.BlockSpec(memory_space=pl.ANY)

    def run(*refs):
        kernel(width, *refs)

    one = dma(())
    states, grads = pl.pallas_call(
        run,
        out_shape=(
            jax.ShapeDtypeStruct((1, rows, feats), BF16),
            jax.ShapeDtypeStruct((1, hidden, half), BF16),
        ),
        in_specs=[hbm] * 5,
        out_specs=(hbm, hbm),
        scratch_shapes=[
            pltpu.VMEM((NT, rows, feats), BF16),
            pltpu.VMEM((NT, rows, feats), BF16),
            pltpu.VMEM((1, feats), BF16),
            pltpu.VMEM((2 * half, hidden), BF16),
            pltpu.VMEM((2, hidden, half), BF16),
            pltpu.VMEM((NZ, rows, hidden), BF16),
            pltpu.VMEM((rows, hidden), BF16),
            pltpu.VMEM((4, rows, hidden), BF16),
            pltpu.VMEM((2, 3, rows, hidden), BF16),
            pltpu.VMEM((2, rows, hidden), BF16),
            pltpu.VMEM((2, rows, hidden), BF16),
            pltpu.VMEM((PARTS, 8, rows), F32),
            pltpu.VMEM((PARTS, NZ, 8, rows), F32),
            pltpu.VMEM((NZ, rows, hidden), BF16),
            pltpu.VMEM((NT, rows, feats), BF16),
            pltpu.VMEM((NT, rows, feats), BF16),
            pltpu.VMEM((rows, feats), BF16),
            pltpu.VMEM((hidden, half), F32),
            pltpu.VMEM((hidden, half), BF16),
            pltpu.VMEM((hidden, half), BF16),
            pltpu.VMEM((hidden, half), BF16),
        ]
        + [one] * 16
        + [dma((NT,))]
        + [one] * 12
        + [dma((n * PARTS,)) for n in (1, 1, 4, 1, 1, 1, 2, 4, 2)]
        + [pltpu.SemaphoreType.REGULAR],
        compiler_params=pltpu.CompilerParams(
            collective_id=0, has_side_effects=True, vmem_limit_bytes=60 * 1024 * 1024
        ),
    )(tokens, gain, w_up, w_down, cotangent)
    return states, grads


def solution(mesh):
    torus = Mesh(
        mesh.devices.reshape(mesh.shape["section"], NZ, 2, NY, NX),
        ("section", "z", "xl", "y", "xh"),
    )
    dp, tensor = ("z", "xl"), ("y", "xh")
    in_specs = (
        P(dp, tensor),
        P("section", tensor),
        P("section", dp, tensor),
        P("section", tensor, dp),
        P("section", dp, None),
    )
    out_specs = (P("section", dp, tensor), P("section", tensor, dp))
    return jax.shard_map(body, mesh=torus, in_specs=in_specs, out_specs=out_specs, check_vma=False)
```
